32 devices in a mesh: rep: 1, dp: 32 (over x, y, z, core).
Axes of the slice: x: 2, y: 2, z: 4, core: 2. Of those that a mesh axis runs over, the one named last changes fastest.
Arguments:
- x: bfloat16 [32, 2048, 512], P(('rep', 'dp'))
- dy: bfloat16 [32, 2048, 512], P(('rep', 'dp'))
- wq: bfloat16 [2, 512, 512], P(None, 'dp')
- wk: bfloat16 [2, 512, 512], P(None, 'dp')
- wv: bfloat16 [2, 512, 512], P(None, 'dp')
- wo: bfloat16 [2, 512, 512], P(None, 'dp')
- w_gate: bfloat16 [2, 512, 2048], P(None, 'dp')
- w_up: bfloat16 [2, 512, 2048], P(None, 'dp')
- w_down: bfloat16 [2, 2048, 512], P(None, 'dp')
- m_wq: float32 [2, 512, 512], P(None, 'dp')
- m_wk: float32 [2, 512, 512], P(None, 'dp')
- m_wv: float32 [2, 512, 512], P(None, 'dp')
- m_wo: float32 [2, 512, 512], P(None, 'dp')
- m_w_gate: float32 [2, 512, 2048], P(None, 'dp')
- m_w_up: float32 [2, 512, 2048], P(None, 'dp')
- m_w_down: float32 [2, 2048, 512], P(None, 'dp')
- v_wq: float32 [2, 512, 512], P(None, 'dp')
- v_wk: float32 [2, 512, 512], P(None, 'dp')
- v_wv: float32 [2, 512, 512], P(None, 'dp')
- v_wo: float32 [2, 512, 512], P(None, 'dp')
- v_w_gate: float32 [2, 512, 2048], P(None, 'dp')
- v_w_up: float32 [2, 512, 2048], P(None, 'dp')
- v_w_down: float32 [2, 2048, 512], P(None, 'dp')
Outputs:
- output 1: bfloat16 [2, 512, 512], P('rep', 'dp')
- output 2: bfloat16 [2, 512, 512], P('rep', 'dp')
- output 3: bfloat16 [2, 512, 512], P('rep', 'dp')
- output 4: bfloat16 [2, 512, 512], P('rep', 'dp')
- output 5: bfloat16 [2, 512, 2048], P('rep', 'dp')
- output 6: bfloat16 [2, 512, 2048], P('rep', 'dp')
- output 7: bfloat16 [2, 2048, 512], P('rep', 'dp')
- output 8: float32 [2, 512, 512], P('rep', 'dp')
- output 9: float32 [2, 512, 512], P('rep', 'dp')
- output 10: float32 [2, 512, 512], P('rep', 'dp')
- output 11: float32 [2, 512, 512], P('rep', 'dp')
- output 12: float32 [2, 512, 2048], P('rep', 'dp')
- output 13: float32 [2, 512, 2048], P('rep', 'dp')
- output 14: float32 [2, 2048, 512], P('rep', 'dp')
- output 15: float32 [2, 512, 512], P('rep', 'dp')
- output 16: float32 [2, 512, 512], P('rep', 'dp')
- output 17: float32 [2, 512, 512], P('rep', 'dp')
- output 18: float32 [2, 512, 512], P('rep', 'dp')
- output 19: float32 [2, 512, 2048], P('rep', 'dp')
- output 20: float32 [2, 512, 2048], P('rep', 'dp')
- output 21: float32 [2, 2048, 512], P('rep', 'dp')
All inputs are finite; a program needn't handle non-finite values.
Results may differ from the reference program's by a relative error of at most 0.0288.
Values are sent between devices in bfloat16 or wider.
A program may use at most 2 GiB of HBM per device.

```python
import jax
import jax.numpy as jnp
from jax import lax

SEQUENCES = 32
TOKENS = 2048
D = 512
HEADS = 4
KV_HEADS = 4
HEAD = 128
FF = 2048
LAYERS = 2
THETA = 10000
NAMES = ("wq", "wk", "wv", "wo", "w_gate", "w_up", "w_down")
SHAPES = {
    "wq": (LAYERS, D, HEADS * HEAD),
    "wk": (LAYERS, D, KV_HEADS * HEAD),
    "wv": (LAYERS, D, KV_HEADS * HEAD),
    "wo": (LAYERS, HEADS * HEAD, D),
    "w_gate": (LAYERS, D, FF),
    "w_up": (LAYERS, D, FF),
    "w_down": (LAYERS, FF, D),
}


def bump(key, n, height):
    away = (jnp.arange(n, dtype=jnp.int32) - jax.random.randint(key, (), 0, n, jnp.int32)) % n
    return jnp.where(away < n // 8, height, 1.0)


def together(key, own, strength):
    shared = jax.random.normal(key, own.shape[1:], jnp.float32)
    return (own + strength * shared) * lax.rsqrt(1 + strength * strength)


def setup_inputs(seed: int = 0, part: int = 0) -> dict:
    kx, kdy, ka, kb, kz, kf, kh, kl, *keys = jax.random.split(jax.random.key(seed), 8 + 3 * len(NAMES))
    kx, kdy, ka, kb = (jax.random.fold_in(k, part) for k in (kx, kdy, ka, kb))
    kw, km, kv = (keys[i::3] for i in range(3))
    shape = (SEQUENCES, TOKENS, D)
    much_x, much_dy = jax.random.uniform(kz, (2,), jnp.float32, 0.0, 1.0)
    loud = 2.0 ** jax.random.uniform(jax.random.fold_in(kz, 1), (), jnp.float32, -1.0, 2.0)
    layers = 2.0 ** jax.random.uniform(kl, (LAYERS, 1, 1), jnp.float32, -1.0, 1.0)
    times = {"wq": 1.0, "wk": 1.0, "wv": 2.0, "wo": layers, "w_gate": 1.0, "w_up": bump(kh, FF, 4.0), "w_down": layers}
    x = together(ka, jax.random.normal(kx, shape, jnp.float32), much_x) * bump(kf, D, 4.0)
    dy = together(kb, jax.random.normal(kdy, shape, jnp.float32), much_dy)
    drawn = {"x": x.astype(jnp.bfloat16), "dy": (loud * dy * (SEQUENCES * TOKENS) ** -0.5).astype(jnp.bfloat16)}
    for key, name in zip(kw, NAMES, strict=True):
        drawn[name] = (jax.random.normal(key, SHAPES[name], jnp.float32) * SHAPES[name][1] ** -0.5 * times[name]).astype(jnp.bfloat16)
    for key, name in zip(km, NAMES, strict=True):
        drawn[f"m_{name}"] = 0.1 * jax.random.normal(key, SHAPES[name], jnp.float32)
    for key, name in zip(kv, NAMES, strict=True):
        drawn[f"v_{name}"] = jax.random.uniform(key, SHAPES[name], jnp.float32, 0.02, 0.06)
    return drawn


def matmul(a, w):
    return jnp.dot(a, w, preferred_element_type=jnp.float32).astype(jnp.bfloat16)


def normed(h):
    wide = h.astype(jnp.float32)
    scale = lax.rsqrt(jnp.mean(wide**2, -1, keepdims=True) + 1e-6)
    return (wide * scale).astype(jnp.bfloat16)


def turned(t, theta):
    half = t.shape[-1] // 2
    angle = jnp.arange(t.shape[0], dtype=jnp.float32)[:, None] * theta ** (-jnp.arange(half, dtype=jnp.float32) / half)
    cos, sin = jnp.cos(angle)[:, None], jnp.sin(angle)[:, None]
    a, b = t[..., :half].astype(jnp.float32), t[..., half:].astype(jnp.float32)
    return jnp.concatenate([a * cos - b * sin, b * cos + a * sin], -1).astype(jnp.bfloat16)


def seen_by(q, k, v):
    tokens, kv = q.shape[0], k.shape[1]
    q = q.reshape(tokens, kv, -1, q.shape[-1])
    scores = jnp.einsum("tgsd,ugd->gstu", q.astype(jnp.float32), k.astype(jnp.float32)) * q.shape[-1] ** -0.5
    place = jnp.arange(tokens)
    weights = jax.nn.softmax(jnp.where(place[:, None] >= place, scores, -jnp.inf), -1).astype(jnp.bfloat16)
    return jnp.einsum("gstu,ugd->tgsd", weights.astype(jnp.float32), v.astype(jnp.float32)).astype(jnp.bfloat16).reshape(tokens, -1)


def layer(h, w):
    a = normed(h)
    q, k = (turned(matmul(a, w[name]).reshape(h.shape[0], -1, HEAD), THETA) for name in ("wq", "wk"))
    h = h + matmul(seen_by(q, k, matmul(a, w["wv"]).reshape(h.shape[0], -1, HEAD)), w["wo"])
    b = normed(h)
    gate = jnp.dot(b, w["w_gate"], preferred_element_type=jnp.float32)
    up = jnp.dot(b, w["w_up"], preferred_element_type=jnp.float32)
    return h + matmul((jax.nn.silu(gate) * up).astype(jnp.bfloat16), w["w_down"])


def adamw(w, m, v, g):
    m = 0.9 * m + 0.1 * g
    v = 0.95 * v + 0.05 * g * g
    step = m * lax.rsqrt(v + 1e-8) + 0.1 * w
    return (w - 0.02 * step).astype(jnp.bfloat16), m, v


def clipped(gradients, sum_of_squares, count):
    factor = jnp.minimum(1.0, 0.5 * lax.rsqrt(sum_of_squares / count + 1e-30))
    return [g * factor for g in gradients]


def stack(weights, h):
    return lax.scan(lambda h, w: (layer(h, w), None), h, weights)[0]


def reference(x, dy, wq, wk, wv, wo, w_gate, w_up, w_down, m_wq, m_wk, m_wv, m_wo, m_w_gate, m_w_up, m_w_down, v_wq, v_wk, v_wv, v_wo, v_w_gate, v_w_up, v_w_down):
    weights = dict(zip(NAMES, (wq, wk, wv, wo, w_gate, w_up, w_down), strict=True))

    def take(so_far, sequence):
        h, by_y = sequence
        _, back = jax.vjp(stack, weights, h)
        by_weights, by_h = back(by_y)
        return jax.tree.map(lambda total, term: total + term.astype(jnp.float32), so_far, by_weights), by_h

    none_yet = {name: jnp.zeros(w.shape, jnp.float32) for name, w in weights.items()}
    by_weights, by_x = lax.scan(take, none_yet, (x, dy))
    gradients = [by_weights[name].astype(jnp.bfloat16).astype(jnp.float32) for name in NAMES]
    gradients = clipped(gradients, sum(jnp.sum(g * g) for g in gradients), sum(g.size for g in gradients))
    first = (m_wq, m_wk, m_wv, m_wo, m_w_gate, m_w_up, m_w_down)
    second = (v_wq, v_wk, v_wv, v_wo, v_w_gate, v_w_up, v_w_down)
    new = [adamw(weights[name].astype(jnp.float32), m, v, g) for name, m, v, g in zip(NAMES, first, second, gradients, strict=True)]
    return tuple(one[which] for which in range(3) for one in new)
```

```python
import functools

import jax
import jax.numpy as jnp
import numpy as np
from jax import lax
from jax.experimental import pallas as pl
from jax.experimental.pallas import tpu as pltpu
from jax.sharding import PartitionSpec as P

BF, F32 = jnp.bfloat16, jnp.float32
MESH = pl.DeviceIdType.MESH
ANY = pl.BlockSpec(memory_space=pl.ANY)
IN_VMEM = pl.BlockSpec(memory_space=pltpu.VMEM)
VMEM = 58 * 2**20
T, D, HEADS, HEAD, FF = 2048, 512, 4, 128, 2048
BLOCK = 512
STEPS = T // BLOCK
UNITS, ROWS = 16, 16
NAMES = ("wq", "wk", "wv", "wo", "w_gate", "w_up", "w_down")
NEG = -1e30
HIDDEN = 2 * NEG
LOG2E = 1.4426950408889634
SCALE = HEAD**-0.5


def _dot(a, b, ca=1, cb=0):
    return lax.dot_general(a, b, (((ca,), (cb,)), ((), ())), preferred_element_type=F32)


def _square(w):
    return w.reshape(D, D)


def _blocks(w):
    return w.astype(BF).reshape(D // ROWS, ROWS, D)


def _normed(h):
    wide = h.astype(F32)
    scale = lax.rsqrt(jnp.mean(wide * wide, -1, keepdims=True) + 1e-6)
    return wide, scale, (wide * scale).astype(BF)


def _norm_back(wide, scale, ct):
    return scale * (ct - wide * (scale * scale * jnp.mean(ct * wide, -1, keepdims=True)))


def _turned(t, cos, sin):
    parts = [t[:, n : n + HEAD] for n in range(0, D, HEAD)]
    return jnp.concatenate([p * cos + pltpu.roll(p, HEAD // 2, 1) * sin for p in parts], 1).astype(BF)


def _head(n):
    return pl.ds(n * HEAD, HEAD)


def _call(body, name, out, scratch=(), grid=(STEPS,), ins=(), outs=(), flops=0, **more):
    return pl.pallas_call(
        body, name=name, grid=grid, in_specs=list(ins), out_specs=list(outs), out_shape=list(out), scratch_shapes=list(scratch),
        compiler_params=pltpu.CompilerParams(dimension_semantics=("arbitrary",) * len(grid), vmem_limit_bytes=VMEM, **more),
        cost_estimate=pl.CostEstimate(flops=flops, transcendentals=0, bytes_accessed=0),
    )


def _rows(width=D):
    return pl.BlockSpec((BLOCK, width), lambda i: (i, 0))


def _whole(*shape):
    return pl.BlockSpec(shape, lambda i: (0,) * len(shape))


def _units(layer, kind):
    return pl.BlockSpec((D // ROWS, 4, ROWS, D), lambda i: (0, layer * 4 + kind, 0, 0), pipeline_mode=pl.Buffered(1))


def _like(*shape, dtype=BF):
    return jax.ShapeDtypeStruct(shape, dtype)


def _qkv(h_ref, w_ref, cos_ref, sin_ref, q_ref, k_ref, v_ref):
    a = _normed(h_ref[...])[2]
    for i, out in enumerate((q_ref, k_ref, v_ref)):
        t = _dot(a, _square(w_ref[:, i])).astype(BF)
        out[...] = t if i == 2 else _turned(t.astype(F32), cos_ref[...], sin_ref[...])


def qkv(h, w, layer, cos, sin):
    return _call(_qkv, "qkv", [_like(T, D)] * 3, ins=[_rows(), _units(layer, 0), _rows(HEAD), _rows(HEAD)], outs=[_rows()] * 3,
                 flops=6 * T * D * D)(h, w, cos, sin)


def _flash(q_ref, k_ref, v_ref, o_ref, lse_ref, top_s, mix_s, vt_s):
    iq = pl.program_id(0)
    e = SCALE * LOG2E

    @pl.when(iq == 0)
    def _():
        for j in range(STEPS):
            vt_s[:, j * BLOCK : (j + 1) * BLOCK] = v_ref[j * BLOCK : (j + 1) * BLOCK, :].T

    top_s[...] = jnp.full_like(top_s, NEG)
    mix_s[...] = jnp.zeros_like(mix_s)
    ones = jnp.ones((8, BLOCK), BF)

    def block(j, masked):
        here = pl.ds(pl.multiple_of(j * BLOCK, BLOCK), BLOCK)
        scores = [_dot(k_ref[here, _head(n)], q_ref[:, _head(n)], 1, 1) for n in range(HEADS)]
        if masked:
            ok = lax.broadcasted_iota(jnp.int32, (BLOCK, BLOCK), 1) >= lax.broadcasted_iota(jnp.int32, (BLOCK, BLOCK), 0)
        weights, keeps = [], []
        for n, s in enumerate(scores):
            if masked:
                s = jnp.where(ok, s, HIDDEN)
            old = top_s[n : n + 1, :]
            top = jnp.maximum(old, s.max(axis=0, keepdims=True))
            top_s[n : n + 1, :] = top
            weights.append(jnp.exp2((s - top) * e).astype(BF))
            keeps.append(jnp.exp2((old - top) * e))
        for n in range(HEADS):
            values = jnp.concatenate([vt_s[_head(n), here], ones], axis=0)
            mix_s[n] = mix_s[n] * keeps[n] + _dot(values, weights[n])

    lax.fori_loop(0, iq, lambda j, _: block(j, False), None)
    block(iq, True)
    for n in range(HEADS):
        total = mix_s[n, HEAD : HEAD + 1, :]
        o_ref[:, _head(n)] = (mix_s[n, :HEAD, :] * (1 / total)).T.astype(BF)
        lse_ref[n : n + 1, :] = top_s[n : n + 1, :] * SCALE + jnp.log(total)


def flash(q, k, v):
    return _call(_flash, "flash", [_like(T, D), _like(HEADS, T, dtype=F32)], ins=[_rows(), _whole(T, D), _whole(T, D)],
                 outs=[_rows(), pl.BlockSpec((HEADS, BLOCK), lambda i: (0, i))],
                 scratch=[pltpu.VMEM((HEADS, BLOCK), F32), pltpu.VMEM((HEADS, HEAD + 8, BLOCK), F32), pltpu.VMEM((D, T), BF)],
                 flops=4 * T * T * D)(q, k, v)


def _ffn(h_ref, o_ref, wo_ref, gate_ref, up_ref, down_ref, mid_ref, out_ref):
    mid = h_ref[...] + _dot(o_ref[...], _square(wo_ref[:, 3])).astype(BF)
    mid_ref[...] = mid
    b = _normed(mid)[2]
    total = None
    for j in range(FF // BLOCK):
        gate, up = _dot(b, _square(gate_ref[:, j])), _dot(b, _square(up_ref[:, j]))
        hid = (gate * jax.nn.sigmoid(gate) * up).astype(BF)
        more = _dot(hid, _square(down_ref[8 * j : 8 * j + 8]))
        total = more if j == 0 else total + more
    out_ref[...] = mid + total.astype(BF)


def ffn(h, o, w, layer):
    return _call(_ffn, "ffn", [_like(T, D)] * 2, ins=[_rows(), _rows()] + [_units(layer, kind) for kind in range(4)], outs=[_rows()] * 2,
                 flops=26 * T * D * D)(h, o, w, w, w, w)


def _ffn_back(dh_ref, mid_ref, gate_ref, up_ref, down_ref, dmid_ref, dgate_ref, dup_ref, ddown_ref, b_s, bt_s, dht_s, db_s, dg_s, du_s, hid_s):
    j = pl.program_id(0)

    @pl.when(j == 0)
    def _():
        for i in range(STEPS):
            here = pl.ds(i * BLOCK, BLOCK)
            b = _normed(mid_ref[here, :])[2]
            b_s[here, :] = b
            bt_s[:, here] = b.T
            dht_s[:, here] = dh_ref[here, :].T
            db_s[here, :] = jnp.zeros((BLOCK, D), F32)

    gate_w, up_w, down_w = _square(gate_ref[:, 0]), _square(up_ref[:, 0]), _square(down_ref[...])

    def rows(i, _):
        here = pl.ds(pl.multiple_of(i * BLOCK, BLOCK), BLOCK)
        b = b_s[here, :]
        gate, up = _dot(b, gate_w), _dot(b, up_w)
        dhid = _dot(dh_ref[here, :], down_w, 1, 1).astype(BF).astype(F32)
        half = jax.nn.sigmoid(gate)
        silu = gate * half
        hid_s[here, :] = (silu * up).astype(BF)
        du = (dhid * silu).astype(BF)
        dg = (dhid * up * (half + silu * (1.0 - half))).astype(BF)
        dg_s[here, :] = dg
        du_s[here, :] = du
        db_s[here, :] += _dot(dg, gate_w, 1, 1) + _dot(du, up_w, 1, 1)

    lax.fori_loop(0, STEPS, rows, None)
    dgate_ref[:, 0] = _blocks(_dot(bt_s[...], dg_s[...]))
    dup_ref[:, 0] = _blocks(_dot(bt_s[...], du_s[...]))
    ddown_ref[...] = _dot(dht_s[...], hid_s[...]).astype(BF).T.reshape(8, 4, ROWS, D)

    @pl.when(j == pl.num_programs(0) - 1)
    def _():
        for i in range(STEPS):
            here = pl.ds(i * BLOCK, BLOCK)
            wide, scale, _ = _normed(mid_ref[here, :])
            dmid_ref[here, :] = dh_ref[here, :] + _norm_back(wide, scale, db_s[here, :].astype(BF).astype(F32)).astype(BF)


def ffn_back(dh, mid, w, layer):
    n = D // ROWS
    one = lambda kind: pl.BlockSpec((n, 1, ROWS, D), lambda j: (0, layer * UNITS + 4 * kind + j, 0, 0))
    some = pl.BlockSpec((n // 4, 4, ROWS, D), lambda j: (j, layer * 4 + 3, 0, 0))
    big = lambda dtype=BF: pltpu.VMEM((T, D), dtype)
    return _call(_ffn_back, "ffn_back", [_like(T, D)] + [_like(n, 4, ROWS, D)] * 3,
                 ins=[_whole(T, D), _whole(T, D), one(1), one(2), some],
                 outs=[_whole(T, D)] + [pl.BlockSpec((n, 1, ROWS, D), lambda j: (0, j, 0, 0))] * 2 + [pl.BlockSpec((n // 4, 4, ROWS, D), lambda j: (j, 0, 0, 0))],
                 scratch=[big(), pltpu.VMEM((D, T), BF), pltpu.VMEM((D, T), BF), big(F32), big(), big(), big()],
                 flops=64 * T * D * D)(dh, mid, w, w, w)


def _out_back(dmid_ref, o_ref, wo_ref, do_ref, delta_ref, dwo_ref, dwo_s):
    i = pl.program_id(0)
    dmid, o = dmid_ref[...], o_ref[...]
    do = _dot(dmid, _square(wo_ref[:, 3]), 1, 1).astype(BF)
    do_ref[...] = do
    pick = (lax.broadcasted_iota(jnp.int32, (8, D), 1) // HEAD == lax.broadcasted_iota(jnp.int32, (8, D), 0)).astype(F32)
    both = do.astype(F32) * o.astype(F32)
    delta_ref[...] = lax.dot_general(pick, both, (((1,), (1,)), ((), ())), precision=lax.Precision.HIGHEST, preferred_element_type=F32)[:HEADS]
    dwo = _dot(o, dmid, 0, 0)

    @pl.when(i == 0)
    def _():
        dwo_s[...] = dwo

    @pl.when(i > 0)
    def _():
        dwo_s[...] += dwo

    dwo_ref[:, 0] = _blocks(dwo_s[...])


def out_back(dmid, o, w, layer):
    n = D // ROWS
    return _call(_out_back, "out_back", [_like(T, D), _like(HEADS, T, dtype=F32), _like(n, 1, ROWS, D)], ins=[_rows(), _rows(), _units(layer, 0)],
                 outs=[_rows(), pl.BlockSpec((HEADS, BLOCK), lambda i: (0, i)), _whole(n, 1, ROWS, D)],
                 scratch=[pltpu.VMEM((D, D), F32)], flops=4 * T * D * D)(dmid, o, w)


def _flash_back(q_ref, k_ref, v_ref, do_ref, lse_ref, delta_ref, dq_ref, dk_ref, dv_ref, dq_s, dk_s, dv_s, kt_s):
    iq = pl.program_id(0)
    e = SCALE * LOG2E

    @pl.when(iq == 0)
    def _():
        for j in range(STEPS):
            here = pl.ds(j * BLOCK, BLOCK)
            kt_s[:, here] = k_ref[here, :].T
            dk_s[here, :] = jnp.zeros((BLOCK, D), F32)
            dv_s[here, :] = jnp.zeros((BLOCK, D), F32)

    dq_s[...] = jnp.zeros_like(dq_s)
    lses = [lse_ref[n : n + 1, :] * LOG2E for n in range(HEADS)]

    def block(j, masked):
        here = pl.ds(pl.multiple_of(j * BLOCK, BLOCK), BLOCK)
        scores = [_dot(k_ref[here, _head(n)], q_ref[:, _head(n)], 1, 1) for n in range(HEADS)]
        dps = [_dot(v_ref[here, _head(n)], do_ref[:, _head(n)], 1, 1) for n in range(HEADS)]
        if masked:
            ok = lax.broadcasted_iota(jnp.int32, (BLOCK, BLOCK), 1) >= lax.broadcasted_iota(jnp.int32, (BLOCK, BLOCK), 0)
        for n in range(HEADS):
            p = jnp.exp2(scores[n] * e - lses[n])
            if masked:
                p = jnp.where(ok, p, 0.0)
            ds = (p * (dps[n] - delta_ref[n : n + 1, :])).astype(BF)
            dv_s[here, _head(n)] += _dot(p.astype(BF), do_ref[:, _head(n)])
            dk_s[here, _head(n)] += _dot(ds, q_ref[:, _head(n)])
            dq_s[_head(n), :] += _dot(kt_s[_head(n), here], ds)

    lax.fori_loop(0, iq, lambda j, _: block(j, False), None)
    block(iq, True)
    dq_ref[...] = (dq_s[...] * SCALE).T.astype(BF)

    @pl.when(iq == STEPS - 1)
    def _():
        for j in range(STEPS):
            here = pl.ds(j * BLOCK, BLOCK)
            dk_ref[here, :] = (dk_s[here, :] * SCALE).astype(BF)
            dv_ref[here, :] = dv_s[here, :].astype(BF)


def flash_back(q, k, v, do, lse, delta):
    row = pl.BlockSpec((HEADS, BLOCK), lambda i: (0, i))
    return _call(_flash_back, "flash_back", [_like(T, D)] * 3, ins=[_rows(), _whole(T, D), _whole(T, D), _rows(), row, row],
                 outs=[_rows(), _whole(T, D), _whole(T, D)],
                 scratch=[pltpu.VMEM((D, BLOCK), F32), pltpu.VMEM((T, D), F32), pltpu.VMEM((T, D), F32), pltpu.VMEM((D, T), BF)],
                 flops=10 * T * T * D)(q, k, v, do, lse, delta)


def _qkv_back(first, h_ref, dq_ref, dk_ref, dv_ref, dmid_ref, w_ref, cos_ref, sin_ref, *refs):
    dh_ref, (dw_ref, dw_s) = (None, refs) if first else (refs[0], refs[1:])
    i = pl.program_id(0)
    wide, scale, a = _normed(h_ref[...])
    at = a.T
    da = None
    for n, ref in enumerate((dq_ref, dk_ref, dv_ref)):
        t = ref[...] if n == 2 else _turned(ref[...].astype(F32), cos_ref[...], -sin_ref[...])
        more = _dot(at, t)

        @pl.when(i == 0)
        def _():
            dw_s[n] = more

        @pl.when(i > 0)
        def _():
            dw_s[n] += more

        dw_ref[:, n] = _blocks(dw_s[n])
        if not first:
            back = _dot(t, _square(w_ref[:, n]), 1, 1).astype(BF)
            da = back if n == 0 else da + back
    if not first:
        dh_ref[...] = dmid_ref[...] + _norm_back(wide, scale, da.astype(F32)).astype(BF)


def qkv_back(h, dq, dk, dv, dmid, w, layer, cos, sin):
    n, first = D // ROWS, layer == 0
    return _call(functools.partial(_qkv_back, first), "qkv_back", [_like(T, D)] * (not first) + [_like(n, 3, ROWS, D)],
                 ins=[_rows()] * 5 + [_units(layer, 0), _rows(HEAD), _rows(HEAD)], outs=[_rows()] * (not first) + [_whole(n, 3, ROWS, D)],
                 scratch=[pltpu.VMEM((3, D, D), F32)], flops=(6 if first else 12) * T * D * D)(h, dq, dk, dv, dmid, w, cos, sin)


def tables():
    angle = np.arange(T)[:, None] * 10000.0 ** (-np.arange(HEAD // 2) / (HEAD // 2))
    cos, sin = np.cos(angle), np.sin(angle)
    return jnp.asarray(np.concatenate([cos, cos], 1), F32), jnp.asarray(np.concatenate([-sin, sin], 1), F32)


def place():
    me = lax.axis_index("dp")
    return me // 16, (me // 8) % 2, (me // 2) % 4, me % 2


def at(x, y, z, c):
    return {"dp": ((x * 2 + y) * 4 + z) * 2 + c}


def peers(x, y, z, c):
    return [at(x, y, (z + n) % 4, c) for n in (1, 2, 3)] + [at(1 - x, y, z, c), at(x, 1 - y, z, c), at(x, y, z, 1 - c)]


def meet(others):
    barrier = pltpu.get_barrier_semaphore()
    for other in others:
        pl.semaphore_signal(barrier, inc=1, device_id=other, device_id_type=MESH)
    pl.semaphore_wait(barrier, len(others))


def remote(src, dst, send, recv, to):
    return pltpu.make_async_remote_copy(src_ref=src, dst_ref=dst, send_sem=send, recv_sem=recv, device_id=to, device_id_type=MESH)


def split(span, n):
    a, b = span
    m = (a + b + n % 2) // 2
    return pl.ds(a, b - a), pl.ds(a, m - a), pl.ds(m, b - m)


def shard_pieces(refs, layer):
    wq, wk, wv, wo, gate, up, down = refs
    found = [(n, w.at[layer]) for n, w in enumerate((wq, wk, wv, wo))]
    for j in range(4):
        found.append((4 + j, gate.at[layer, :, pl.ds(j * D, D)]))
        found.append((8 + j, up.at[layer, :, pl.ds(j * D, D)]))
        found.append((12 + j, down.at[layer, pl.ds(j * ROWS, ROWS), :]))
    return [(unit + layer * UNITS, piece) for unit, piece in found]


def _gather(cuts, *refs):
    shards, (g, mine, local_sem, own_sem, send_sem, recv_sem) = refs[:7], refs[7:]
    x, y, z, c = place()
    loads = [pltpu.make_async_copy(piece, mine.at[unit], local_sem.at[unit]) for layer in range(2) for unit, piece in shard_pieces(shards, layer)]
    for load in loads:
        load.start()
    meet(peers(x, y, z, c))
    for load in loads:
        load.wait()
    spans = list(zip(cuts[:-1], cuts[1:]))
    own = pltpu.make_async_copy(mine, g.at[x, y, z, c], own_sem)
    own.start()

    def copies(n, step, arriving):
        u, lo, hi = split(spans[n], n)
        xx, yy, cc = (1 - x, 1 - y, 1 - c) if arriving else (x, y, c)
        if step == 0:
            here = [(z + 4 - k) % 4 if arriving else z for k in (1, 2, 3)]
            todo = [(mine.at[u], g.at[x, y, zz, c, u], at(x, y, (z + k) % 4, c)) for k, zz in zip((1, 2, 3), here)]
        elif step == 1:
            todo = [(g.at[xx, y, :, c, lo],) * 2 + (at(1 - x, y, z, c),), (g.at[x, yy, :, c, hi],) * 2 + (at(x, 1 - y, z, c),)]
        elif step == 2:
            todo = [(g.at[:, yy, :, c, lo],) * 2 + (at(x, 1 - y, z, c),), (g.at[xx, :, :, c, hi],) * 2 + (at(1 - x, y, z, c),)]
        else:
            todo = [(g.at[:, :, :, cc, u],) * 2 + (at(x, y, z, 1 - c),)]
        return [remote(s, d, send_sem.at[n, step, i], recv_sem.at[n, step, i], to) for i, (s, d, to) in enumerate(todo) if 0 not in d.shape]

    for n in range(len(spans)):
        for copy in copies(n, 0, False):
            copy.start()
    own.wait()
    for tick in range(len(spans) + 3):
        for step in (3, 2, 1, 0):
            n = tick - step
            if 0 <= n < len(spans):
                for copy in copies(n, step, True):
                    copy.wait_recv()
                if step < 3:
                    for copy in copies(n, step + 1, False):
                        copy.start()
    for n in range(len(spans)):
        for step in range(4):
            for copy in copies(n, step, False):
                copy.wait_send()


def gather(weights, cuts=(0, 3, 9, 16, 19, 25, 32)):
    n = len(cuts) - 1
    return pl.pallas_call(
        functools.partial(_gather, cuts),
        out_shape=jax.ShapeDtypeStruct((2, 2, 4, 2, 2 * UNITS, ROWS, D), BF),
        in_specs=[ANY] * 7,
        out_specs=ANY,
        scratch_shapes=[pltpu.VMEM((2 * UNITS, ROWS, D), BF), pltpu.SemaphoreType.DMA((2 * UNITS,)), pltpu.SemaphoreType.DMA,
                        pltpu.SemaphoreType.DMA((n, 4, 3)), pltpu.SemaphoreType.DMA((n, 4, 3))],
        compiler_params=pltpu.CompilerParams(collective_id=0, has_side_effects=True),
        name="gather",
    )(*weights)


def _add_into(total, more):
    lead = total.shape[:-2]

    def one(i, _):
        where, left = [], i
        for n in reversed(lead):
            where.append(left % n)
            left = left // n
        where = tuple(reversed(where))
        total[where] = (total[where].astype(F32) + more[where].astype(F32)).astype(BF)

    lax.fori_loop(0, int(np.prod(lead)), one, None)


def _scatter(spans, *refs):
    count = 1 + max(span[0] for span in spans)
    ds, (g, squares, s, r1, r2, r3, r4, sq, sq_all, local_sem, send_sem, recv_sem, sq_send, sq_recv) = refs[:count], refs[count:]
    x, y, z, c = place()

    def own(n, core):
        which, first, a, b = spans[n]
        return ds[which].at[:, :, :, core, pl.ds(first, b - a)]

    loads = [pltpu.make_async_copy(own(n, c), s.at[:, :, :, split(spans[n][2:], n)[0]], local_sem.at[n]) for n in range(len(spans))]

    def copies(n, step):
        u, lo, hi = split(spans[n][2:], n)
        if step == 0:
            todo = [(own(n, 1 - c), r1.at[:, :, :, u], at(x, y, z, 1 - c))]
        elif step == 1:
            todo = [(s.at[1 - x, :, :, lo], r2.at[:, :, lo], at(1 - x, y, z, c)), (s.at[:, 1 - y, :, hi], r2.at[:, :, hi], at(x, 1 - y, z, c))]
        elif step == 2:
            todo = [(s.at[x, 1 - y, :, lo], r3.at[:, lo], at(x, 1 - y, z, c)), (s.at[1 - x, y, :, hi], r3.at[:, hi], at(1 - x, y, z, c))]
        else:
            todo = [(s.at[x, y, (z + k) % 4, u], r4.at[k - 1, u], at(x, y, (z + k) % 4, c)) for k in (1, 2, 3)]
        return [remote(a, b, send_sem.at[n, step, i], recv_sem.at[n, step, i], to) for i, (a, b, to) in enumerate(todo) if 0 not in a.shape]

    def add(n, step):
        u, lo, hi = split(spans[n][2:], n)
        if step == 0:
            _add_into(s.at[:, :, :, u], r1.at[:, :, :, u])
        elif step == 1:
            _add_into(s.at[x, :, :, lo], r2.at[:, :, lo])
            _add_into(s.at[:, y, :, hi], r2.at[:, :, hi])
        elif step == 2:
            _add_into(s.at[x, y, :, u], r3.at[:, u])
        else:
            a, b = spans[n][2:]

            def one(i, total):
                i = a + i
                out = s[x, y, z, i].astype(F32) + r4[0, i].astype(F32) + r4[1, i].astype(F32) + r4[2, i].astype(F32)
                g[i] = out.astype(BF)
                out = out.astype(BF).astype(F32)
                return total + (out * out).reshape(ROWS // 8, 8, D // 128, 128).sum((0, 2))

            sq[...] += lax.fori_loop(0, b - a, one, jnp.zeros((8, 128), F32))

    sq[...] = jnp.zeros_like(sq)
    for load in loads:
        load.start()
    everyone = [{"dp": (lax.axis_index("dp") + k) % 32} for k in range(1, 32)]
    meet(everyone)
    for n in range(len(spans)):
        for copy in copies(n, 0):
            copy.start()
    for tick in range(len(spans) + 3):
        for step in (3, 2, 1, 0):
            n = tick - step
            if 0 <= n < len(spans):
                if step == 0:
                    loads[n].wait()
                for copy in copies(n, step):
                    copy.wait_recv()
                add(n, step)
                if step < 3:
                    for copy in copies(n, step + 1):
                        copy.start()
    spread = [remote(sq, sq_all.at[k + 1], sq_send.at[k], sq_recv.at[k], to) for k, to in enumerate(everyone)]
    for copy in spread:
        copy.start()
    for copy in spread:
        copy.wait_recv()
    sq_all[0] = sq[...]
    squares[...] = jnp.full((8, 128), jnp.sum(sq_all[...]))
    for copy in spread:
        copy.wait_send()
    for n in range(len(spans)):
        for step in range(4):
            for copy in copies(n, step):
                copy.wait_send()


def scatter(parts, most=4):
    spans = []
    for which, (d, unit) in enumerate(parts):
        spans += [(which, a, unit + a, unit + min(a + most, d.shape[1])) for a in range(0, d.shape[1], most)]
    n, u = len(spans), 2 * UNITS
    buffers = [pltpu.VMEM((*lead, u, ROWS, D), BF) for lead in ((2, 2, 4), (2, 2, 4), (2, 4), (4,), (3,))]
    sems = [pltpu.SemaphoreType.DMA(shape) for shape in ((n,), (n, 4, 3), (n, 4, 3), (31,), (31,))]
    return pl.pallas_call(
        functools.partial(_scatter, spans),
        out_shape=[_like(u, ROWS, D), _like(8, 128, dtype=F32)],
        in_specs=[ANY] * len(parts),
        out_specs=[IN_VMEM, IN_VMEM],
        scratch_shapes=[*buffers, pltpu.VMEM((8, 128), F32), pltpu.VMEM((32, 8, 128), F32), *sems],
        compiler_params=pltpu.CompilerParams(collective_id=1, has_side_effects=True, vmem_limit_bytes=VMEM),
        name="scatter",
    )(*[d.reshape(2, 2, 4, 2, *d.shape[1:]) for d, _ in parts])


def _adamw(squares, g, *refs):
    w, m, v, new_w, new_m, new_v = (refs[i : i + 7] for i in range(0, 42, 7))
    count = 2 * UNITS * ROWS * D * 32
    factor = jnp.minimum(1.0, 0.5 * lax.rsqrt(squares[0:1, 0:1] / count + 1e-30))
    for layer in range(2):
        for i in range(7):
            for unit, piece in _pieces(i):
                where = (layer, *piece)
                one = g[layer * UNITS + unit].astype(F32) * factor
                mm = 0.9 * m[i][where] + 0.1 * one
                vv = 0.95 * v[i][where] + 0.05 * one * one
                old = w[i][where].astype(F32)
                new_w[i][where] = (old - 0.02 * (mm * lax.rsqrt(vv + 1e-8) + 0.1 * old)).astype(BF)
                new_m[i][where] = mm
                new_v[i][where] = vv


def _pieces(i):
    every = slice(None)
    if i < 4:
        return [(i, (every, every))]
    if i < 6:
        return [(4 * (i - 3) + j, (every, pl.ds(j * D, D))) for j in range(4)]
    return [(12 + j, (pl.ds(j * ROWS, ROWS), every)) for j in range(4)]


def adamw_all(weights, m, v, g, squares):
    return pl.pallas_call(
        _adamw,
        out_shape=[_like(*w.shape) for w in weights] + [_like(*w.shape, dtype=F32) for w in weights] * 2,
        in_specs=[IN_VMEM] * 23,
        out_specs=[IN_VMEM] * 21,
        compiler_params=pltpu.CompilerParams(vmem_limit_bytes=VMEM),
        name="adamw_all",
    )(squares, g, *weights, *m, *v)


def solution(mesh):
    def step(x, dy, *arrays):
        weights, m, v = (arrays[i : i + 7] for i in (0, 7, 14))
        cos, sin = tables()
        w = gather(weights).reshape(32, 2 * UNITS, ROWS, D)
        h, kept, parts = x[0], [], []
        for layer in range(2):
            q, k, vv = qkv(h, w, layer, cos, sin)
            o, lse = flash(q, k, vv)
            mid, out = ffn(h, o, w, layer)
            kept.append((h, q, k, vv, o, lse, mid))
            h = out
        dh = dy[0]
        for layer in (1, 0):
            h, q, k, vv, o, lse, mid = kept[layer]
            first = layer * UNITS
            dmid, *by_ffn = ffn_back(dh, mid, w, layer)
            do, delta, by_o = out_back(dmid, o, w, layer)
            dq, dk, dv = flash_back(q, k, vv, do, lse, delta)
            *dh, by_qkv = qkv_back(h, dq, dk, dv, dmid, w, layer, cos, sin)
            dh = dh[0] if dh else None
            parts += [(d, first + 4 * (n + 1)) for n, d in enumerate(by_ffn)] + [(by_o, first + 3), (by_qkv, first)]
        g, squares = scatter(parts)
        return tuple(adamw_all(weights, m, v, g, squares))

    states, cut = P(("rep", "dp"), None, None), P(None, "dp", None)
    return jax.shard_map(
        step,
        mesh=mesh,
        in_specs=(states, states) + (cut,) * 21,
        out_specs=(P("rep", "dp", None),) * 21,
        check_vma=False,
    )
```

```python
import functools

import jax
import jax.numpy as jnp
import numpy as np
from jax import lax
from jax.experimental import pallas as pl
from jax.experimental.pallas import tpu as pltpu
from jax.sharding import PartitionSpec as P

BF, F32 = jnp.bfloat16, jnp.float32
MESH = pl.DeviceIdType.MESH
ANY = pl.BlockSpec(memory_space=pl.ANY)
IN_VMEM = pl.BlockSpec(memory_space=pltpu.VMEM)
VMEM = 58 * 2**20
T, D, HEADS, HEAD, FF = 2048, 512, 4, 128, 2048
BLOCK = 512
STEPS = T // BLOCK
LAG, MOST, LAST = 2, 2, 1
UNITS, ROWS = 16, 16
NEG = -1e30
HIDDEN = 2 * NEG
LOG2E = 1.4426950408889634
SCALE = HEAD**-0.5


def _dot(a, b, ca=1, cb=0):
    return lax.dot_general(a, b, (((ca,), (cb,)), ((), ())), preferred_element_type=F32)


def _dot_t(a, b):
    return _dot(a, b, 1, 1)


def _square(w):
    return w.reshape(D, D)


def _blocks(w):
    return w.astype(BF).reshape(D // ROWS, ROWS, D)


def _normed(h):
    wide = h.astype(F32)
    scale = lax.rsqrt(jnp.mean(wide * wide, -1, keepdims=True) + 1e-6)
    return wide, scale, (wide * scale).astype(BF)


def _norm_back(wide, scale, ct):
    return scale * (ct - wide * (scale * scale * jnp.mean(ct * wide, -1, keepdims=True)))


def _turned(t, cos, sin):
    parts = [t[:, n : n + HEAD] for n in range(0, D, HEAD)]
    return jnp.concatenate([p * cos + pltpu.roll(p, HEAD // 2, 1) * sin for p in parts], 1).astype(BF)


def _head(n):
    return pl.ds(n * HEAD, HEAD)


def _call(body, name, out, scratch=(), ins=(), outs=(), flops=0, parts=(), slots=()):
    out, outs, ins, scratch, more, own = list(out), list(outs), list(ins), list(scratch), {}, body
    if parts:
        number, *parts = parts
        spans, units = sum_spans(parts, MOST)
        buffers = sum_buffers(units, len(spans))
        n_in, n_out = len(ins), len(out)
        ins += [ANY] * len(parts)
        out += [_like(units, ROWS, D)]
        outs += [_whole(units, ROWS, D)]
        parts = [d.reshape(2, 2, 4, 2, *d.shape[1:]) for d in parts]
        more = dict(collective_id=number, has_side_effects=True)

        def own(*refs):
            refs = list(refs)
            given, refs = refs[:n_in], refs[n_in:]
            ds, refs = refs[: len(parts)], refs[len(parts) :]
            made, total, kept = refs[:n_out], refs[n_out], refs[n_out + 1 :]
            traffic = Sums(LAG, slots, spans, ds, total, *kept[len(scratch) :])
            body(*given, *made, *kept[: len(scratch)], traffic)

    run = pl.pallas_call(
        own, name=name, grid=(STEPS,), in_specs=ins, out_specs=outs, out_shape=out, scratch_shapes=scratch + (buffers if parts else []),
        compiler_params=pltpu.CompilerParams(dimension_semantics=("arbitrary",), vmem_limit_bytes=VMEM, **more),
        cost_estimate=pl.CostEstimate(flops=flops, transcendentals=0, bytes_accessed=0),
    )
    return lambda *given: run(*given, *parts)


def _rows(width=D):
    return pl.BlockSpec((BLOCK, width), lambda i: (i, 0))


def _whole(*shape):
    return pl.BlockSpec(shape, lambda i: (0,) * len(shape), pipeline_mode=pl.Buffered(1))


def _units(layer, kind):
    return pl.BlockSpec((D // ROWS, 4, ROWS, D), lambda i: (0, layer * 4 + kind, 0, 0), pipeline_mode=pl.Buffered(1))


def _like(*shape, dtype=BF):
    return jax.ShapeDtypeStruct(shape, dtype)


def _qkv(h_ref, w_ref, cos_ref, sin_ref, q_ref, k_ref, v_ref):
    a = _normed(h_ref[...])[2]
    for i, out in enumerate((q_ref, k_ref, v_ref)):
        t = _dot(a, _square(w_ref[:, i])).astype(BF)
        out[...] = t if i == 2 else _turned(t.astype(F32), cos_ref[...], sin_ref[...])


def qkv(h, w, layer, cos, sin):
    return _call(_qkv, "qkv", [_like(T, D)] * 3, ins=[_rows(), _units(layer, 0), _rows(HEAD), _rows(HEAD)], outs=[_rows()] * 3,
                 flops=6 * T * D * D)(h, w, cos, sin)


def _flash(q_ref, k_ref, v_ref, o_ref, lse_ref, top_s, mix_s, vt_s):
    iq = pl.program_id(0)
    e = SCALE * LOG2E

    @pl.when(iq == 0)
    def _():
        for j in range(STEPS):
            vt_s[:, j * BLOCK : (j + 1) * BLOCK] = v_ref[j * BLOCK : (j + 1) * BLOCK, :].T

    top_s[...] = jnp.full_like(top_s, NEG)
    mix_s[...] = jnp.zeros_like(mix_s)
    ones = jnp.ones((8, BLOCK), BF)

    def block(j, masked):
        here = pl.ds(pl.multiple_of(j * BLOCK, BLOCK), BLOCK)
        scores = [_dot_t(k_ref[here, _head(n)], q_ref[:, _head(n)]) for n in range(HEADS)]
        if masked:
            ok = lax.broadcasted_iota(jnp.int32, (BLOCK, BLOCK), 1) >= lax.broadcasted_iota(jnp.int32, (BLOCK, BLOCK), 0)
        weights, keeps = [], []
        for n, s in enumerate(scores):
            if masked:
                s = jnp.where(ok, s, HIDDEN)
            old = top_s[n : n + 1, :]
            top = jnp.maximum(old, s.max(axis=0, keepdims=True))
            top_s[n : n + 1, :] = top
            weights.append(jnp.exp2((s - top) * e).astype(BF))
            keeps.append(jnp.exp2((old - top) * e))
        for n in range(HEADS):
            values = jnp.concatenate([vt_s[_head(n), here], ones], axis=0)
            mix_s[n] = mix_s[n] * keeps[n] + _dot(values, weights[n])

    lax.fori_loop(0, iq, lambda j, _: block(j, False), None)
    block(iq, True)
    for n in range(HEADS):
        total = mix_s[n, HEAD : HEAD + 1, :]
        o_ref[:, _head(n)] = (mix_s[n, :HEAD, :] * (1 / total)).T.astype(BF)
        lse_ref[n : n + 1, :] = top_s[n : n + 1, :] * SCALE + jnp.log(total)


def flash(q, k, v):
    return _call(_flash, "flash", [_like(T, D), _like(HEADS, T, dtype=F32)], ins=[_rows(), _whole(T, D), _whole(T, D)],
                 outs=[_rows(), pl.BlockSpec((HEADS, BLOCK), lambda i: (0, i))],
                 scratch=[pltpu.VMEM((HEADS, BLOCK), F32), pltpu.VMEM((HEADS, HEAD + 8, BLOCK), F32), pltpu.VMEM((D, T), BF)],
                 flops=4 * T * T * D)(q, k, v)


def _ffn(h_ref, o_ref, wo_ref, gate_ref, up_ref, down_ref, mid_ref, out_ref):
    mid = h_ref[...] + _dot(o_ref[...], _square(wo_ref[:, 3])).astype(BF)
    mid_ref[...] = mid
    b = _normed(mid)[2]
    total = None
    for j in range(FF // BLOCK):
        gate, up = _dot(b, _square(gate_ref[:, j])), _dot(b, _square(up_ref[:, j]))
        hid = (gate * jax.nn.sigmoid(gate) * up).astype(BF)
        more = _dot(hid, _square(down_ref[8 * j : 8 * j + 8]))
        total = more if j == 0 else total + more
    out_ref[...] = mid + total.astype(BF)


def ffn(h, o, w, layer):
    return _call(_ffn, "ffn", [_like(T, D)] * 2, ins=[_rows(), _rows()] + [_units(layer, kind) for kind in range(4)], outs=[_rows()] * 2,
                 flops=26 * T * D * D)(h, o, w, w, w, w)


def _ffn_back(dh_ref, mid_ref, gate_ref, up_ref, down_ref, dmid_ref, dgate_ref, dup_ref, ddown_ref, b_s, bt_s, dht_s, db_s, dg_s, du_s, hid_s, traffic=None):
    j = pl.program_id(0)

    @pl.when(j == 0)
    def _():
        for i in range(STEPS):
            here = pl.ds(i * BLOCK, BLOCK)
            b = _normed(mid_ref[here, :])[2]
            b_s[here, :] = b
            bt_s[:, here] = b.T
            dht_s[:, here] = dh_ref[here, :].T
            db_s[here, :] = jnp.zeros((BLOCK, D), F32)

    gate_w, up_w, down_w = _square(gate_ref[:, 0]), _square(up_ref[:, 0]), _square(down_ref[...])

    def rows(i, _):
        if traffic:
            traffic.tick(j, i)
        here = pl.ds(pl.multiple_of(i * BLOCK, BLOCK), BLOCK)
        b = b_s[here, :]
        gate, up = _dot(b, gate_w), _dot(b, up_w)
        dhid = _dot_t(dh_ref[here, :], down_w).astype(BF).astype(F32)
        half = jax.nn.sigmoid(gate)
        silu = gate * half
        hid_s[here, :] = (silu * up).astype(BF)
        du = (dhid * silu).astype(BF)
        dg = (dhid * up * (half + silu * (1.0 - half))).astype(BF)
        dg_s[here, :] = dg
        du_s[here, :] = du
        db_s[here, :] += _dot_t(dg, gate_w) + _dot_t(du, up_w)

    lax.fori_loop(0, STEPS, rows, None)
    dgate_ref[:, 0] = _blocks(_dot(bt_s[...], dg_s[...]))
    dup_ref[:, 0] = _blocks(_dot(bt_s[...], du_s[...]))
    ddown_ref[...] = _dot(dht_s[...], hid_s[...]).astype(BF).T.reshape(8, 4, ROWS, D)

    @pl.when(j == pl.num_programs(0) - 1)
    def _():
        for i in range(STEPS):
            here = pl.ds(i * BLOCK, BLOCK)
            wide, scale, _ = _normed(mid_ref[here, :])
            dmid_ref[here, :] = dh_ref[here, :] + _norm_back(wide, scale, db_s[here, :].astype(BF).astype(F32)).astype(BF)
        if traffic:
            traffic.finish()


def ffn_back(dh, mid, w, layer, parts=()):
    n = D // ROWS
    one = lambda kind: pl.BlockSpec((n, 1, ROWS, D), lambda j: (0, layer * UNITS + 4 * kind + j, 0, 0))
    some = pl.BlockSpec((n // 4, 4, ROWS, D), lambda j: (j, layer * 4 + 3, 0, 0))
    big = lambda dtype=BF: pltpu.VMEM((T, D), dtype)
    return _call(_ffn_back, "ffn_back", [_like(T, D)] + [_like(n, 4, ROWS, D)] * 3,
                 ins=[_whole(T, D), _whole(T, D), one(1), one(2), some],
                 outs=[_whole(T, D)] + [pl.BlockSpec((n, 1, ROWS, D), lambda j: (0, j, 0, 0))] * 2 + [pl.BlockSpec((n // 4, 4, ROWS, D), lambda j: (j, 0, 0, 0))],
                 scratch=[big(), pltpu.VMEM((D, T), BF), pltpu.VMEM((D, T), BF), big(F32), big(), big(), big()],
                 flops=64 * T * D * D, parts=parts, slots=[(i, j) for i in range(STEPS) for j in range(STEPS)])(dh, mid, w, w, w)


def _attn_back(first, h_ref, q_ref, k_ref, v_ref, o_ref, lse_ref, dmid_ref, w_ref, cos_ref, sin_ref, *refs):
    step = pl.program_id(0)
    iq = STEPS - 1 - step
    dh_ref, refs = (None, refs) if first else (refs[0], refs[1:])
    dw_ref, do_s, delta_s, dq_s, dk_s, dv_s, kt_s, dw_s = refs[:8]
    traffic = refs[8] if len(refs) > 8 else None
    e = SCALE * LOG2E

    @pl.when(step == 0)
    def _():
        for j in range(STEPS):
            here = pl.ds(j * BLOCK, BLOCK)
            kt_s[:, here] = k_ref[here, :].T
            dk_s[here, :] = jnp.zeros((BLOCK, D), F32)
            dv_s[here, :] = jnp.zeros((BLOCK, D), F32)
        dw_s[...] = jnp.zeros_like(dw_s)

    dmid, o = dmid_ref[...], o_ref[...]
    do = _dot_t(dmid, _square(w_ref[:, 3])).astype(BF)
    do_s[...] = do
    pick = (lax.broadcasted_iota(jnp.int32, (8, D), 1) // HEAD == lax.broadcasted_iota(jnp.int32, (8, D), 0)).astype(F32)
    both = do.astype(F32) * o.astype(F32)
    delta_s[...] = lax.dot_general(pick, both, (((1,), (1,)), ((), ())), precision=lax.Precision.HIGHEST, preferred_element_type=F32)
    dw_s[3] += _dot(o.T, dmid)
    dq_s[...] = jnp.zeros_like(dq_s)

    def block(j, masked):
        if traffic:
            traffic.tick(iq, j)
        here = pl.ds(pl.multiple_of(j * BLOCK, BLOCK), BLOCK)
        scores = [_dot_t(k_ref[here, _head(n)], q_ref[:, _head(n)]) for n in range(HEADS)]
        dps = [_dot_t(v_ref[here, _head(n)], do_s[:, _head(n)]) for n in range(HEADS)]
        if masked:
            ok = lax.broadcasted_iota(jnp.int32, (BLOCK, BLOCK), 1) >= lax.broadcasted_iota(jnp.int32, (BLOCK, BLOCK), 0)
        for n in range(HEADS):
            p = jnp.exp2(scores[n] * e - lse_ref[n : n + 1, :] * LOG2E)
            if masked:
                p = jnp.where(ok, p, 0.0)
            ds = (p * (dps[n] - delta_s[n : n + 1, :])).astype(BF)
            dv_s[here, _head(n)] += _dot(p.astype(BF), do_s[:, _head(n)])
            dk_s[here, _head(n)] += _dot(ds, q_ref[:, _head(n)])
            dq_s[_head(n), :] += _dot(kt_s[_head(n), here], ds)

    lax.fori_loop(0, iq, lambda j, _: block(j, False), None)
    block(iq, True)
    if traffic:
        traffic.tick(iq, STEPS)
    here = pl.ds(pl.multiple_of(iq * BLOCK, BLOCK), BLOCK)
    wide, scale, a = _normed(h_ref[...])
    at = a.T
    dq = (dq_s[...] * SCALE).T.astype(BF)
    dk = (dk_s[here, :] * SCALE).astype(BF)
    da = None
    for n, t in enumerate((dq, dk, dv_s[here, :].astype(BF))):
        if n < 2:
            t = _turned(t.astype(F32), cos_ref[...], -sin_ref[...])
        dw_s[n] += _dot(at, t)
        if not first:
            back = _dot_t(t, _square(w_ref[:, n])).astype(BF)
            da = back if n == 0 else da + back
    if not first:
        dh_ref[...] = dmid + _norm_back(wide, scale, da.astype(F32)).astype(BF)

    @pl.when(step == STEPS - 1)
    def _():
        for n in range(4):
            dw_ref[:, n] = _blocks(dw_s[n])
        if traffic:
            traffic.finish()


def attn_back(h, q, k, v, o, lse, dmid, w, layer, cos, sin, parts=()):
    n, first = D // ROWS, layer == 0
    down = lambda width=D: pl.BlockSpec((BLOCK, width), lambda i: (STEPS - 1 - i, 0))
    every = _whole(T, D)
    big = pltpu.VMEM((T, D), F32)
    return _call(functools.partial(_attn_back, first), "attn_back", [_like(T, D)] * (not first) + [_like(n, 4, ROWS, D)],
                 ins=[down(), down(), every, every, down(), pl.BlockSpec((HEADS, BLOCK), lambda i: (0, STEPS - 1 - i)), down(), _units(layer, 0), down(HEAD), down(HEAD)],
                 outs=[down()] * (not first) + [_whole(n, 4, ROWS, D)],
                 scratch=[pltpu.VMEM((BLOCK, D), BF), pltpu.VMEM((8, BLOCK), F32), pltpu.VMEM((D, BLOCK), F32), big, big, pltpu.VMEM((D, T), BF), pltpu.VMEM((4, D, D), F32)],
                 flops=14 * T * T * D, parts=parts, slots=[(i, j) for i in reversed(range(STEPS)) for j in (*range(i + 1), STEPS)])(h, q, k, v, o, lse, dmid, w, cos, sin)


def tables():
    angle = np.arange(T)[:, None] * 10000.0 ** (-np.arange(HEAD // 2) / (HEAD // 2))
    cos, sin = np.cos(angle), np.sin(angle)
    return jnp.asarray(np.concatenate([cos, cos], 1), F32), jnp.asarray(np.concatenate([-sin, sin], 1), F32)


def place():
    me = lax.axis_index("dp")
    return me // 16, (me // 8) % 2, (me // 2) % 4, me % 2


def at(x, y, z, c):
    return {"dp": ((x * 2 + y) * 4 + z) * 2 + c}


def peers(x, y, z, c):
    return [at(x, y, (z + n) % 4, c) for n in (1, 2, 3)] + [at(1 - x, y, z, c), at(x, 1 - y, z, c), at(x, y, z, 1 - c)]


def meet(others):
    barrier = pltpu.get_barrier_semaphore()
    for other in others:
        pl.semaphore_signal(barrier, inc=1, device_id=other, device_id_type=MESH)
    pl.semaphore_wait(barrier, len(others))


def remote(src, dst, send, recv, to):
    return pltpu.make_async_remote_copy(src_ref=src, dst_ref=dst, send_sem=send, recv_sem=recv, device_id=to, device_id_type=MESH)


def halves(span, n):
    a, b = span
    m = (a + b + n % 2) // 2
    return [(first, pl.ds(lo, hi - lo)) for first, lo, hi in ((True, a, m), (False, m, b)) if hi > lo]


def stretch(span):
    return pl.ds(span[0], span[1] - span[0])


def shard_pieces(refs, layer):
    wq, wk, wv, wo, gate, up, down = refs
    found = [(n, w.at[layer]) for n, w in enumerate((wq, wk, wv, wo))]
    for j in range(4):
        found.append((4 + j, gate.at[layer, :, pl.ds(j * D, D)]))
        found.append((8 + j, up.at[layer, :, pl.ds(j * D, D)]))
        found.append((12 + j, down.at[layer, pl.ds(j * ROWS, ROWS), :]))
    return [(unit + layer * UNITS, piece) for unit, piece in found]


def _gather(cuts, *refs):
    shards, (g, mine, local_sem, own_sem, send_sem, recv_sem) = refs[:7], refs[7:]
    x, y, z, c = place()
    loads = [pltpu.make_async_copy(piece, mine.at[unit], local_sem.at[unit]) for layer in range(2) for unit, piece in shard_pieces(shards, layer)]
    for load in loads:
        load.start()
    meet(peers(x, y, z, c))
    for load in loads:
        load.wait()
    spans = list(zip(cuts[:-1], cuts[1:]))
    own = pltpu.make_async_copy(mine, g.at[x, y, z, c], own_sem)
    own.start()

    def copies(n, step, arriving):
        u = stretch(spans[n])
        xx, yy, cc = (1 - x, 1 - y, 1 - c) if arriving else (x, y, c)
        by_x, by_y = at(1 - x, y, z, c), at(x, 1 - y, z, c)
        if step == 0:
            here = [(z + 4 - k) % 4 if arriving else z for k in (1, 2, 3)]
            todo = [(mine.at[u], g.at[x, y, zz, c, u], at(x, y, (z + k) % 4, c)) for k, zz in zip((1, 2, 3), here)]
        elif step == 1:
            todo = [(g.at[xx, y, :, c, u],) * 2 + (by_x,) if first else (g.at[x, yy, :, c, u],) * 2 + (by_y,) for first, u in halves(spans[n], n)]
        elif step == 2:
            todo = [(g.at[:, yy, :, c, u],) * 2 + (by_y,) if first else (g.at[xx, :, :, c, u],) * 2 + (by_x,) for first, u in halves(spans[n], n)]
        else:
            todo = [(g.at[:, :, :, cc, u],) * 2 + (at(x, y, z, 1 - c),)]
        return [remote(s, d, send_sem.at[n, step, i], recv_sem.at[n, step, i], to) for i, (s, d, to) in enumerate(todo)]

    for n in range(len(spans)):
        for copy in copies(n, 0, False):
            copy.start()
    own.wait()
    for tick in range(len(spans) + 3):
        for step in (3, 2, 1, 0):
            n = tick - step
            if 0 <= n < len(spans):
                for copy in copies(n, step, True):
                    copy.wait_recv()
                if step < 3:
                    for copy in copies(n, step + 1, False):
                        copy.start()
    for n in range(len(spans)):
        for step in range(4):
            for copy in copies(n, step, False):
                copy.wait_send()


def gather(weights, cuts=(0, 3, 9, 16, 19, 25, 32)):
    n = len(cuts) - 1
    return pl.pallas_call(
        functools.partial(_gather, cuts),
        out_shape=jax.ShapeDtypeStruct((2, 2, 4, 2, 2 * UNITS, ROWS, D), BF),
        in_specs=[ANY] * 7,
        out_specs=ANY,
        scratch_shapes=[pltpu.VMEM((2 * UNITS, ROWS, D), BF), pltpu.SemaphoreType.DMA((2 * UNITS,)), pltpu.SemaphoreType.DMA,
                        pltpu.SemaphoreType.DMA((n, 4, 3)), pltpu.SemaphoreType.DMA((n, 4, 3))],
        compiler_params=pltpu.CompilerParams(collective_id=0, has_side_effects=True),
        name="gather",
    )(*weights)


def _add_into(total, more):
    lead = total.shape[:-3]

    def one(i, _):
        where = []
        for n in reversed(lead):
            where = [i % n] + where
            i = i // n
        where = tuple(where)
        total[where] = (total[where].astype(F32) + more[where].astype(F32)).astype(BF)

    lax.fori_loop(0, int(np.prod(lead)), one, None)


def sum_spans(parts, most):
    spans, units = [], 0
    for which, d in enumerate(parts):
        n = d.shape[1]
        spans += [(which, a, units + a, units + min(a + most, n)) for a in range(0, n, most)]
        units += n
    return spans, units


def sum_buffers(units, n):
    return [pltpu.VMEM((*lead, units, ROWS, D), BF) for lead in ((2, 2, 4), (2, 2, 4), (2, 4), (4,), (3,))] + [
        pltpu.SemaphoreType.DMA(shape) for shape in ((n,), (n, 4, 3), (n, 4, 3))]


class Sums:
    def __init__(self, lag, slots, spans, ds, g, *buffers):
        self.lag, self.slots, self.spans, self.ds, self.g = lag, slots, spans, ds, g
        self.s, self.r1, self.r2, self.r3, self.r4, self.local_sem, self.send_sem, self.recv_sem = buffers
        self.place = place()

    def own(self, n, core):
        which, first, a, b = self.spans[n]
        return self.ds[which].at[:, :, :, core, pl.ds(first, b - a)]

    def load(self, n):
        return pltpu.make_async_copy(self.own(n, self.place[3]), self.s.at[:, :, :, stretch(self.spans[n][2:])], self.local_sem.at[n])

    def copies(self, n, step):
        (x, y, z, c), s, span = self.place, self.s, self.spans[n][2:]
        u, by_x, by_y = stretch(span), at(1 - x, y, z, c), at(x, 1 - y, z, c)
        if step == 0:
            todo = [(self.own(n, 1 - c), self.r1.at[:, :, :, u], at(x, y, z, 1 - c))]
        elif step == 1:
            todo = [(s.at[1 - x, :, :, u] if first else s.at[:, 1 - y, :, u], self.r2.at[:, :, u], by_x if first else by_y) for first, u in halves(span, n)]
        elif step == 2:
            todo = [(s.at[x, 1 - y, :, u] if first else s.at[1 - x, y, :, u], self.r3.at[:, u], by_y if first else by_x) for first, u in halves(span, n)]
        else:
            todo = [(s.at[x, y, (z + k) % 4, u], self.r4.at[k - 1, u], at(x, y, (z + k) % 4, c)) for k in (1, 2, 3)]
        return [remote(a, b, self.send_sem.at[n, step, i], self.recv_sem.at[n, step, i], to) for i, (a, b, to) in enumerate(todo)]

    def add(self, n, step):
        (x, y, z, c), s, span = self.place, self.s, self.spans[n][2:]
        u = stretch(span)
        if step == 0:
            _add_into(s.at[:, :, :, u], self.r1.at[:, :, :, u])
        elif step == 1:
            for first, u in halves(span, n):
                _add_into(s.at[x, :, :, u] if first else s.at[:, y, :, u], self.r2.at[:, :, u])
        elif step == 2:
            _add_into(s.at[x, y, :, u], self.r3.at[:, u])
        else:
            out = s[x, y, z, u].astype(F32)
            for k in range(3):
                out = out + self.r4[k, u].astype(F32)
            self.g[u] = out.astype(BF)

    def begin(self, others=None):
        for n in range(len(self.spans)):
            self.load(n).start()
        meet(others or peers(*self.place))
        for n in range(len(self.spans)):
            self.start(n, 0)

    def start(self, n, step):
        for copy in self.copies(n, step):
            copy.start()

    def turns(self):
        found = [self.begin]
        for tick in range(len(self.spans) + 3 * self.lag):
            now = [(tick - self.lag * step, step) for step in range(4) if 0 <= tick - self.lag * step < len(self.spans)]

            def turn(now=now):
                for n, step in now:
                    if step == 0:
                        self.load(n).wait()
                    for copy in self.copies(n, step):
                        copy.wait_recv()
                    self.add(n, step)
                for n, step in now:
                    if step < 3:
                        self.start(n, step + 1)

            found.append(turn)
        return found

    def tick(self, i, j):
        turns = self.turns()
        for n, turn in enumerate(turns):
            a, b = self.slots[n * len(self.slots) // len(turns)]
            pl.when((i == a) & (j == b))(turn)

    def finish(self):
        for n in range(len(self.spans)):
            for step in range(4):
                for copy in self.copies(n, step):
                    copy.wait_send()


def _last_sums(spans, d, *refs):
    *done, g, squares, sq, sq_all, sq_send, sq_recv = refs[: -len(sum_buffers(1, 1))]
    traffic = Sums(1, (), spans, [d], g, *refs[-len(sum_buffers(1, 1)) :])
    me = lax.axis_index("dp")
    everyone = [{"dp": (me + k) % 32} for k in range(1, 32)]
    begin, *turns = traffic.turns()
    begin(everyone)
    sq[...] = jnp.zeros_like(sq)

    def squared(ref):
        def one(i, total):
            wide = ref[i].astype(F32)
            return total + (wide * wide).reshape(ROWS // 8, 8, D // HEAD, HEAD).sum((0, 2))

        sq[...] += lax.fori_loop(0, ref.shape[0], one, jnp.zeros((8, HEAD), F32))

    for ref in done:
        squared(ref)
    for turn in turns:
        turn()
    squared(g)
    spread = [remote(sq, sq_all.at[k + 1], sq_send.at[k], sq_recv.at[k], to) for k, to in enumerate(everyone)]
    for copy in spread:
        copy.start()
    for copy in spread:
        copy.wait_recv()
    sq_all[0] = sq[...]
    squares[...] = jnp.full((8, HEAD), jnp.sum(sq_all[...]))
    for copy in spread:
        copy.wait_send()
    traffic.finish()


def last_sums(d, done):
    spans, units = sum_spans([d], LAST)
    return pl.pallas_call(
        functools.partial(_last_sums, spans),
        out_shape=[_like(units, ROWS, D), _like(8, HEAD, dtype=F32)],
        in_specs=[ANY] + [IN_VMEM] * len(done),
        out_specs=[IN_VMEM, IN_VMEM],
        scratch_shapes=[pltpu.VMEM((8, HEAD), F32), pltpu.VMEM((32, 8, HEAD), F32), pltpu.SemaphoreType.DMA((31,)), pltpu.SemaphoreType.DMA((31,)),
                        *sum_buffers(units, len(spans))],
        compiler_params=pltpu.CompilerParams(collective_id=1, has_side_effects=True, vmem_limit_bytes=VMEM),
        name="last_sums",
    )(d.reshape(2, 2, 4, 2, *d.shape[1:]), *done)


def _adamw(squares, *refs):
    g, (w, m, v, new_w, new_m, new_v) = refs[:4], (refs[i : i + 7] for i in range(4, 46, 7))
    count = 2 * UNITS * ROWS * D * 32
    factor = jnp.minimum(1.0, 0.5 * lax.rsqrt(squares[0:1, 0:1] / count + 1e-30))
    for layer in range(2):
        for i in range(7):
            for unit, piece in _pieces(i):
                where = (layer, *piece)
                sums, unit = (g[2 * layer], unit) if i < 4 else (g[2 * layer + 1], unit - 4)
                one = sums[unit].astype(F32) * factor
                mm = 0.9 * m[i][where] + 0.1 * one
                vv = 0.95 * v[i][where] + 0.05 * one * one
                old = w[i][where].astype(F32)
                new_w[i][where] = (old - 0.02 * (mm * lax.rsqrt(vv + 1e-8) + 0.1 * old)).astype(BF)
                new_m[i][where] = mm
                new_v[i][where] = vv


def _pieces(i):
    every = slice(None)
    if i < 4:
        return [(i, (every, every))]
    if i < 6:
        return [(4 * (i - 3) + j, (every, pl.ds(j * D, D))) for j in range(4)]
    return [(12 + j, (pl.ds(j * ROWS, ROWS), every)) for j in range(4)]


def adamw_all(weights, m, v, sums, squares):
    return pl.pallas_call(
        _adamw,
        out_shape=[_like(*w.shape) for w in weights] + [_like(*w.shape, dtype=F32) for w in weights] * 2,
        in_specs=[IN_VMEM] * 26,
        out_specs=[IN_VMEM] * 21,
        compiler_params=pltpu.CompilerParams(vmem_limit_bytes=VMEM),
        name="adamw_all",
    )(squares, *sums, *weights, *m, *v)


def solution(mesh):
    def step(x, dy, *arrays):
        weights, m, v = (arrays[i : i + 7] for i in (0, 7, 14))
        cos, sin = tables()
        w = gather(weights).reshape(32, 2 * UNITS, ROWS, D)
        h, kept = x[0], []
        for layer in range(2):
            q, k, vv = qkv(h, w, layer, cos, sin)
            o, lse = flash(q, k, vv)
            mid, out = ffn(h, o, w, layer)
            kept.append(((h, q, k, vv, o, lse), mid))
            h = out
        saved, mid = kept[1]
        dmid, *by_ffn = ffn_back(dy[0], mid, w, 1)
        dh, by_attn, ffn_sum_1 = attn_back(*saved, dmid, w, 1, cos, sin, (2, *by_ffn))
        saved, mid = kept[0]
        dmid, *by_ffn, attn_sum_1 = ffn_back(dh, mid, w, 0, (3, by_attn))
        by_attn, ffn_sum_0 = attn_back(*saved, dmid, w, 0, cos, sin, (4, *by_ffn))
        attn_sum_0, squares = last_sums(by_attn, (ffn_sum_0, attn_sum_1, ffn_sum_1))
        return tuple(adamw_all(weights, m, v, (attn_sum_0, ffn_sum_0, attn_sum_1, ffn_sum_1), squares))

    states, cut = P(("rep", "dp"), None, None), P(None, "dp", None)
    return jax.shard_map(
        step,
        mesh=mesh,
        in_specs=(states, states) + (cut,) * 21,
        out_specs=(P("rep", "dp", None),) * 21,
        check_vma=False,
    )
```

```python
import functools

import jax
import jax.numpy as jnp
import numpy as np
from jax import lax
from jax.experimental import pallas as pl
from jax.experimental.pallas import tpu as pltpu
from jax.sharding import PartitionSpec as P

BF, F32 = jnp.bfloat16, jnp.float32
MESH = pl.DeviceIdType.MESH
ANY = pl.BlockSpec(memory_space=pl.ANY)
IN_VMEM = pl.BlockSpec(memory_space=pltpu.VMEM)
VMEM = 58 * 2**20
T, D, HEADS, HEAD, FF = 2048, 512, 4, 128, 2048
BLOCK = 512
STEPS = T // BLOCK
LAG, MOST, LAST, SPAN, FIRST = 2, 2, 2, 2, 2
UNITS, ROWS = 16, 16
NEG = -1e30
HIDDEN = 2 * NEG
LOG2E = 1.4426950408889634
SCALE = HEAD**-0.5


def _dot(a, b, ca=1, cb=0):
    return lax.dot_general(a, b, (((ca,), (cb,)), ((), ())), preferred_element_type=F32)


def _dot_t(a, b):
    return _dot(a, b, 1, 1)


def _square(w):
    return w.reshape(D, D)


def _blocks(w):
    return w.astype(BF).reshape(D // ROWS, ROWS, D)


def _normed(h):
    wide = h.astype(F32)
    scale = lax.rsqrt(jnp.mean(wide * wide, -1, keepdims=True) + 1e-6)
    return wide, scale, (wide * scale).astype(BF)


def _norm_back(wide, scale, ct):
    return scale * (ct - wide * (scale * scale * jnp.mean(ct * wide, -1, keepdims=True)))


def _turned(t, cos, sin):
    parts = [t[:, n : n + HEAD] for n in range(0, D, HEAD)]
    return jnp.concatenate([p * cos + pltpu.roll(p, HEAD // 2, 1) * sin for p in parts], 1).astype(BF)


def _head(n):
    return pl.ds(n * HEAD, HEAD)


def _call(body, name, out, scratch=(), ins=(), outs=(), flops=0, parts=(), slots=()):
    out, outs, ins, scratch, more, own = list(out), list(outs), list(ins), list(scratch), {}, body
    if parts:
        number, *parts = parts
        spans, units = sum_spans(parts, MOST)
        buffers = sum_buffers(units, len(spans))
        n_in, n_out = len(ins), len(out)
        ins += [ANY] * len(parts)
        out += [_like(units, ROWS, D)]
        outs += [_whole(units, ROWS, D)]
        parts = [d.reshape(2, 2, 4, 2, *d.shape[1:]) for d in parts]
        more = dict(collective_id=number, has_side_effects=True)

        def own(*refs):
            refs = list(refs)
            given, refs = refs[:n_in], refs[n_in:]
            ds, refs = refs[: len(parts)], refs[len(parts) :]
            made, total, kept = refs[:n_out], refs[n_out], refs[n_out + 1 :]
            traffic = Sums(LAG, slots, spans, ds, total, *kept[len(scratch) :])
            body(*given, *made, *kept[: len(scratch)], traffic)

    run = pl.pallas_call(
        own, name=name, grid=(STEPS,), in_specs=ins, out_specs=outs, out_shape=out, scratch_shapes=scratch + (buffers if parts else []),
        compiler_params=pltpu.CompilerParams(dimension_semantics=("arbitrary",), vmem_limit_bytes=VMEM, **more),
        cost_estimate=pl.CostEstimate(flops=flops, transcendentals=0, bytes_accessed=0),
    )
    return lambda *given: run(*given, *parts)


def _rows(width=D):
    return pl.BlockSpec((BLOCK, width), lambda i: (i, 0))


def _whole(*shape):
    return pl.BlockSpec(shape, lambda i: (0,) * len(shape), pipeline_mode=pl.Buffered(1))


def _of(layer, *shape):
    return pl.BlockSpec((None, *shape), lambda i: (layer, *(0,) * len(shape)), pipeline_mode=pl.Buffered(1))


def _units(layer, kind):
    return pl.BlockSpec((D // ROWS, 4, ROWS, D), lambda i: (0, layer * 4 + kind, 0, 0), pipeline_mode=pl.Buffered(1))


def _like(*shape, dtype=BF):
    return jax.ShapeDtypeStruct(shape, dtype)


def _ffn_back(dh_ref, mid_ref, gate_ref, up_ref, down_ref, dmid_ref, dgate_ref, dup_ref, ddown_ref, b_s, bt_s, dht_s, db_s, dg_s, du_s, hid_s, traffic=None):
    j = pl.program_id(0)

    @pl.when(j == 0)
    def _():
        for i in range(STEPS):
            here = pl.ds(i * BLOCK, BLOCK)
            b = _normed(mid_ref[here, :])[2]
            b_s[here, :] = b
            bt_s[:, here] = b.T
            dht_s[:, here] = dh_ref[here, :].T
            db_s[here, :] = jnp.zeros((BLOCK, D), F32)

    gate_w, up_w, down_w = _square(gate_ref[:, 0]), _square(up_ref[:, 0]), _square(down_ref[...])

    def rows(i, _):
        if traffic:
            traffic.tick(j, i)
        here = pl.ds(pl.multiple_of(i * BLOCK, BLOCK), BLOCK)
        b = b_s[here, :]
        gate, up = _dot(b, gate_w), _dot(b, up_w)
        dhid = _dot_t(dh_ref[here, :], down_w).astype(BF).astype(F32)
        half = jax.nn.sigmoid(gate)
        silu = gate * half
        hid_s[here, :] = (silu * up).astype(BF)
        du = (dhid * silu).astype(BF)
        dg = (dhid * up * (half + silu * (1.0 - half))).astype(BF)
        dg_s[here, :] = dg
        du_s[here, :] = du
        db_s[here, :] += _dot_t(dg, gate_w) + _dot_t(du, up_w)

    lax.fori_loop(0, STEPS, rows, None)
    dgate_ref[:, 0] = _blocks(_dot(bt_s[...], dg_s[...]))
    dup_ref[:, 0] = _blocks(_dot(bt_s[...], du_s[...]))
    ddown_ref[...] = _dot(dht_s[...], hid_s[...]).astype(BF).T.reshape(8, 4, ROWS, D)

    @pl.when(j == pl.num_programs(0) - 1)
    def _():
        for i in range(STEPS):
            here = pl.ds(i * BLOCK, BLOCK)
            wide, scale, _ = _normed(mid_ref[here, :])
            dmid_ref[here, :] = dh_ref[here, :] + _norm_back(wide, scale, db_s[here, :].astype(BF).astype(F32)).astype(BF)
        if traffic:
            traffic.finish()


def ffn_back(dh, mid, w, layer, parts=()):
    n = D // ROWS
    one = lambda kind: pl.BlockSpec((n, 1, ROWS, D), lambda j: (0, layer * UNITS + 4 * kind + j, 0, 0))
    some = pl.BlockSpec((n // 4, 4, ROWS, D), lambda j: (j, layer * 4 + 3, 0, 0))
    big = lambda dtype=BF: pltpu.VMEM((T, D), dtype)
    return _call(_ffn_back, "ffn_back", [_like(T, D)] + [_like(n, 4, ROWS, D)] * 3,
                 ins=[_whole(T, D), _of(layer, T, D), one(1), one(2), some],
                 outs=[_whole(T, D)] + [pl.BlockSpec((n, 1, ROWS, D), lambda j: (0, j, 0, 0))] * 2 + [pl.BlockSpec((n // 4, 4, ROWS, D), lambda j: (j, 0, 0, 0))],
                 scratch=[big(), pltpu.VMEM((D, T), BF), pltpu.VMEM((D, T), BF), big(F32), big(), big(), big()],
                 flops=64 * T * D * D, parts=parts, slots=[(i, j) for i in range(STEPS) for j in range(STEPS)])(dh, mid, w, w, w)


def _attn_back(first, h_ref, q_ref, k_ref, v_ref, o_ref, lse_ref, dmid_ref, w_ref, cos_ref, sin_ref, *refs):
    step = pl.program_id(0)
    iq = STEPS - 1 - step
    dh_ref, refs = (None, refs) if first else (refs[0], refs[1:])
    dw_ref, do_s, delta_s, dq_s, dk_s, dv_s, kt_s, dw_s = refs[:8]
    traffic = refs[8] if len(refs) > 8 else None
    e = SCALE * LOG2E

    @pl.when(step == 0)
    def _():
        for j in range(STEPS):
            here = pl.ds(j * BLOCK, BLOCK)
            kt_s[:, here] = k_ref[here, :].T
            dk_s[here, :] = jnp.zeros((BLOCK, D), F32)
            dv_s[here, :] = jnp.zeros((BLOCK, D), F32)
        dw_s[...] = jnp.zeros_like(dw_s)

    dmid, o = dmid_ref[...], o_ref[...]
    do = _dot_t(dmid, _square(w_ref[:, 3])).astype(BF)
    do_s[...] = do
    pick = (lax.broadcasted_iota(jnp.int32, (8, D), 1) // HEAD == lax.broadcasted_iota(jnp.int32, (8, D), 0)).astype(F32)
    both = do.astype(F32) * o.astype(F32)
    delta_s[...] = lax.dot_general(pick, both, (((1,), (1,)), ((), ())), precision=lax.Precision.HIGHEST, preferred_element_type=F32)
    dw_s[3] += _dot(o.T, dmid)
    dq_s[...] = jnp.zeros_like(dq_s)

    def block(j, masked):
        if traffic:
            traffic.tick(iq, DIAGONAL if masked else j)
        here = pl.ds(pl.multiple_of(j * BLOCK, BLOCK), BLOCK)
        scores = [_dot_t(k_ref[here, _head(n)], q_ref[:, _head(n)]) for n in range(HEADS)]
        dps = [_dot_t(v_ref[here, _head(n)], do_s[:, _head(n)]) for n in range(HEADS)]
        if masked:
            ok = lax.broadcasted_iota(jnp.int32, (BLOCK, BLOCK), 1) >= lax.broadcasted_iota(jnp.int32, (BLOCK, BLOCK), 0)
        for n in range(HEADS):
            p = jnp.exp2(scores[n] * e - lse_ref[n : n + 1, :] * LOG2E)
            if masked:
                p = jnp.where(ok, p, 0.0)
            ds = (p * (dps[n] - delta_s[n : n + 1, :])).astype(BF)
            dv_s[here, _head(n)] += _dot(p.astype(BF), do_s[:, _head(n)])
            dk_s[here, _head(n)] += _dot(ds, q_ref[:, _head(n)])
            dq_s[_head(n), :] += _dot(kt_s[_head(n), here], ds)

    lax.fori_loop(0, iq, lambda j, _: block(j, False), None)
    block(iq, True)
    if traffic:
        traffic.tick(iq, AFTER)
    here = pl.ds(pl.multiple_of(iq * BLOCK, BLOCK), BLOCK)
    wide, scale, a = _normed(h_ref[...])
    at = a.T
    dq = (dq_s[...] * SCALE).T.astype(BF)
    dk = (dk_s[here, :] * SCALE).astype(BF)
    da = None
    for n, t in enumerate((dq, dk, dv_s[here, :].astype(BF))):
        if n < 2:
            t = _turned(t.astype(F32), cos_ref[...], -sin_ref[...])
        dw_s[n] += _dot(at, t)
        if not first:
            back = _dot_t(t, _square(w_ref[:, n])).astype(BF)
            da = back if n == 0 else da + back
    if not first:
        dh_ref[...] = dmid + _norm_back(wide, scale, da.astype(F32)).astype(BF)

    @pl.when(step == STEPS - 1)
    def _():
        for n in range(4):
            dw_ref[:, n] = _blocks(dw_s[n])
        if traffic:
            traffic.finish()


def attn_back(h, q, k, v, o, lse, dmid, w, layer, cos, sin, parts=()):
    n, first = D // ROWS, layer == 0
    down = lambda width=D: pl.BlockSpec((BLOCK, width), lambda i: (STEPS - 1 - i, 0))
    ours = pl.BlockSpec((None, BLOCK, D), lambda i: (layer, STEPS - 1 - i, 0))
    every = _of(layer, T, D)
    big = pltpu.VMEM((T, D), F32)
    return _call(functools.partial(_attn_back, first), "attn_back", [_like(T, D)] * (not first) + [_like(n, 4, ROWS, D)],
                 ins=[down(), ours, every, every, ours, pl.BlockSpec((None, HEADS, BLOCK), lambda i: (layer, 0, STEPS - 1 - i)), down(), _units(layer, 0), down(HEAD), down(HEAD)],
                 outs=[down()] * (not first) + [_whole(n, 4, ROWS, D)],
                 scratch=[pltpu.VMEM((BLOCK, D), BF), pltpu.VMEM((8, BLOCK), F32), pltpu.VMEM((D, BLOCK), F32), big, big, pltpu.VMEM((D, T), BF), pltpu.VMEM((4, D, D), F32)],
                 flops=14 * T * T * D, parts=parts, slots=attention_slots([(i, i) for i in reversed(range(STEPS))]))(h, q, k, v, o, lse, dmid, w, cos, sin)


def tables():
    angle = np.arange(T)[:, None] * 10000.0 ** (-np.arange(HEAD // 2) / (HEAD // 2))
    cos, sin = np.cos(angle), np.sin(angle)
    return jnp.asarray(np.concatenate([cos, cos], 1), F32), jnp.asarray(np.concatenate([-sin, sin], 1), F32)


def place():
    me = lax.axis_index("dp")
    return me // 16, (me // 8) % 2, (me // 2) % 4, me % 2


def at(x, y, z, c):
    return {"dp": ((x * 2 + y) * 4 + z) * 2 + c}


def peers(x, y, z, c):
    return [at(x, y, (z + n) % 4, c) for n in (1, 2, 3)] + [at(1 - x, y, z, c), at(x, 1 - y, z, c), at(x, y, z, 1 - c)]


def meet(others):
    barrier = pltpu.get_barrier_semaphore()
    for other in others:
        pl.semaphore_signal(barrier, inc=1, device_id=other, device_id_type=MESH)
    pl.semaphore_wait(barrier, len(others))


def remote(src, dst, send, recv, to):
    return pltpu.make_async_remote_copy(src_ref=src, dst_ref=dst, send_sem=send, recv_sem=recv, device_id=to, device_id_type=MESH)


def halves(span, n):
    a, b = span
    m = (a + b + n % 2) // 2
    return [(first, pl.ds(lo, hi - lo)) for first, lo, hi in ((True, a, m), (False, m, b)) if hi > lo]


def stretch(span):
    return pl.ds(span[0], span[1] - span[0])


def shard_pieces(refs, layer):
    wq, wk, wv, wo, gate, up, down = refs
    found = [(n, w.at[layer]) for n, w in enumerate((wq, wk, wv, wo))]
    for j in range(4):
        found.append((4 + j, gate.at[layer, :, pl.ds(j * D, D)]))
        found.append((8 + j, up.at[layer, :, pl.ds(j * D, D)]))
        found.append((12 + j, down.at[layer, pl.ds(j * ROWS, ROWS), :]))
    return [(unit + layer * UNITS, piece) for unit, piece in found]


class Fetch:
    def __init__(self, spans, shards, g, kept, own_sem, kept_sem, send_sem, recv_sem):
        self.spans, self.shards, self.g, self.kept = spans, shards, g, kept
        self.own_sem, self.kept_sem, self.send_sem, self.recv_sem = own_sem, kept_sem, send_sem, recv_sem
        self.place = place()

    def loads(self):
        pieces = [piece for layer in range(2) for piece in shard_pieces(self.shards, layer)]
        return [pltpu.make_async_copy(piece, self.g.at[(*self.place, unit)], self.own_sem.at[unit]) for unit, piece in pieces]

    def keep(self, n):
        u = stretch(self.spans[n])
        return pltpu.make_async_copy(self.g.at[:, :, :, :, u], self.kept.at[:, :, :, :, u], self.kept_sem.at[n])

    def copies(self, n, step, arriving=False):
        (x, y, z, c), g, span = self.place, self.g, self.spans[n]
        u, by_x, by_y = stretch(span), at(1 - x, y, z, c), at(x, 1 - y, z, c)
        xx, yy, cc = (1 - x, 1 - y, 1 - c) if arriving else (x, y, c)
        if step == 0:
            todo = [(g.at[x, y, (z + 4 - k) % 4 if arriving else z, c, u], at(x, y, (z + k) % 4, c)) for k in (1, 2, 3)]
        elif step == 1:
            todo = [(g.at[xx, y, :, c, u], by_x) if first else (g.at[x, yy, :, c, u], by_y) for first, u in halves(span, n)]
        elif step == 2:
            todo = [(g.at[:, yy, :, c, u], by_y) if first else (g.at[xx, :, :, c, u], by_x) for first, u in halves(span, n)]
        else:
            todo = [(g.at[:, :, :, cc, u], at(x, y, z, 1 - c))]
        return [remote(piece, piece, self.send_sem.at[n, step, i], self.recv_sem.at[n, step, i], to) for i, (piece, to) in enumerate(todo)]

    def start(self, n, step):
        for copy in self.copies(n, step):
            copy.start()

    def begin(self):
        for load in self.loads():
            load.start()
        meet(peers(*self.place))
        for load in self.loads():
            load.wait()
        for n in range(len(self.spans)):
            self.start(n, 0)

    def turns(self, first, last, lag):
        found = []
        for tick in range(last - first + 3 * lag):
            now = [(first + tick - lag * step, step) for step in (3, 2, 1, 0) if 0 <= tick - lag * step < last - first]

            def turn(now=now):
                for n, step in now:
                    for copy in self.copies(n, step, True):
                        copy.wait_recv()
                    if step < 3:
                        self.start(n, step + 1)
                    else:
                        self.keep(n).start()

            found.append(turn)
        return found

    def finish(self):
        for n in range(len(self.spans)):
            self.keep(n).wait()
            for step in range(4):
                for copy in self.copies(n, step):
                    copy.wait_send()


DIAGONAL, AFTER = "diagonal", "after"


def run_at(slots, turns, i, j):
    for n, turn in enumerate(turns):
        a, b = slots[n * len(slots) // len(turns)]
        if isinstance(b, str) or isinstance(j, str):
            if b == j:
                pl.when(i == a)(turn)
        else:
            pl.when(i * UNITS + j == a * UNITS + b)(turn)


def attention_slots(steps):
    return [(s, j) for s, n in steps for j in (*range(n), DIAGONAL, AFTER)]


def _add_into(total, more):
    lead = total.shape[:-3]

    def one(i, _):
        where = []
        for n in reversed(lead):
            where = [i % n] + where
            i = i // n
        where = tuple(where)
        total[where] = (total[where].astype(F32) + more[where].astype(F32)).astype(BF)

    lax.fori_loop(0, int(np.prod(lead)), one, None)


def sum_spans(parts, most):
    spans, units = [], 0
    for which, d in enumerate(parts):
        n = d.shape[1]
        spans += [(which, a, units + a, units + min(a + most, n)) for a in range(0, n, most)]
        units += n
    return spans, units


def sum_buffers(units, n):
    return [pltpu.VMEM((*lead, units, ROWS, D), BF) for lead in ((2, 2, 4), (2, 2, 4), (2, 4), (4,), (3,))] + [
        pltpu.SemaphoreType.DMA(shape) for shape in ((n,), (n, 4, 3), (n, 4, 3))]


class Sums:
    def __init__(self, lag, slots, spans, ds, g, *buffers):
        self.lag, self.slots, self.spans, self.ds, self.g = lag, slots, spans, ds, g
        self.s, self.r1, self.r2, self.r3, self.r4, self.local_sem, self.send_sem, self.recv_sem = buffers
        self.place = place()

    def own(self, n, core):
        which, first, a, b = self.spans[n]
        return self.ds[which].at[:, :, :, core, pl.ds(first, b - a)]

    def load(self, n):
        return pltpu.make_async_copy(self.own(n, self.place[3]), self.s.at[:, :, :, stretch(self.spans[n][2:])], self.local_sem.at[n])

    def copies(self, n, step):
        (x, y, z, c), s, span = self.place, self.s, self.spans[n][2:]
        u, by_x, by_y = stretch(span), at(1 - x, y, z, c), at(x, 1 - y, z, c)
        if step == 0:
            todo = [(self.own(n, 1 - c), self.r1.at[:, :, :, u], at(x, y, z, 1 - c))]
        elif step == 1:
            todo = [(s.at[1 - x, :, :, u] if first else s.at[:, 1 - y, :, u], self.r2.at[:, :, u], by_x if first else by_y) for first, u in halves(span, n)]
        elif step == 2:
            todo = [(s.at[x, 1 - y, :, u] if first else s.at[1 - x, y, :, u], self.r3.at[:, u], by_y if first else by_x) for first, u in halves(span, n)]
        else:
            todo = [(s.at[x, y, (z + k) % 4, u], self.r4.at[k - 1, u], at(x, y, (z + k) % 4, c)) for k in (1, 2, 3)]
        return [remote(a, b, self.send_sem.at[n, step, i], self.recv_sem.at[n, step, i], to) for i, (a, b, to) in enumerate(todo)]

    def add(self, n, step):
        (x, y, z, c), s, span = self.place, self.s, self.spans[n][2:]
        u = stretch(span)
        if step == 0:
            _add_into(s.at[:, :, :, u], self.r1.at[:, :, :, u])
        elif step == 1:
            for first, u in halves(span, n):
                _add_into(s.at[x, :, :, u] if first else s.at[:, y, :, u], self.r2.at[:, :, u])
        elif step == 2:
            _add_into(s.at[x, y, :, u], self.r3.at[:, u])
        else:
            out = s[x, y, z, u].astype(F32)
            for k in range(3):
                out = out + self.r4[k, u].astype(F32)
            self.g[u] = out.astype(BF)

    def begin(self, others=None):
        for n in range(len(self.spans)):
            self.load(n).start()
        meet(others or peers(*self.place))
        for n in range(len(self.spans)):
            self.start(n, 0)

    def start(self, n, step):
        for copy in self.copies(n, step):
            copy.start()

    def turns(self):
        found = [self.begin]
        for tick in range(len(self.spans) + 3 * self.lag):
            now = [(tick - self.lag * step, step) for step in range(4) if 0 <= tick - self.lag * step < len(self.spans)]

            def turn(now=now):
                for n, step in now:
                    if step == 0:
                        self.load(n).wait()
                    for copy in self.copies(n, step):
                        copy.wait_recv()
                    self.add(n, step)
                for n, step in now:
                    if step < 3:
                        self.start(n, step + 1)

            found.append(turn)
        return found

    def tick(self, i, j):
        run_at(self.slots, self.turns(), i, j)

    def finish(self):
        for n in range(len(self.spans)):
            for step in range(4):
                for copy in self.copies(n, step):
                    copy.wait_send()


def _last_sums(spans, d, *refs):
    *done, g, squares, sq, sq_all, sq_send, sq_recv = refs[: -len(sum_buffers(1, 1))]
    traffic = Sums(1, (), spans, [d], g, *refs[-len(sum_buffers(1, 1)) :])
    me = lax.axis_index("dp")
    everyone = [{"dp": (me + k) % 32} for k in range(1, 32)]
    begin, *turns = traffic.turns()
    begin(everyone)
    sq[...] = jnp.zeros_like(sq)

    def squared(ref):
        def one(i, total):
            wide = ref[i].astype(F32)
            return total + (wide * wide).reshape(ROWS // 8, 8, D // HEAD, HEAD).sum((0, 2))

        sq[...] += lax.fori_loop(0, ref.shape[0], one, jnp.zeros((8, HEAD), F32))

    for ref in done:
        squared(ref)
    for turn in turns:
        turn()
    squared(g)
    spread = [remote(sq, sq_all.at[k + 1], sq_send.at[k], sq_recv.at[k], to) for k, to in enumerate(everyone)]
    for copy in spread:
        copy.start()
    for copy in spread:
        copy.wait_recv()
    sq_all[0] = sq[...]
    squares[...] = jnp.full((8, HEAD), jnp.sum(sq_all[...]))
    for copy in spread:
        copy.wait_send()
    traffic.finish()


def last_sums(d, done):
    spans, units = sum_spans([d], LAST)
    return pl.pallas_call(
        functools.partial(_last_sums, spans),
        out_shape=[_like(units, ROWS, D), _like(8, HEAD, dtype=F32)],
        in_specs=[ANY] + [IN_VMEM] * len(done),
        out_specs=[IN_VMEM, IN_VMEM],
        scratch_shapes=[pltpu.VMEM((8, HEAD), F32), pltpu.VMEM((32, 8, HEAD), F32), pltpu.SemaphoreType.DMA((31,)), pltpu.SemaphoreType.DMA((31,)),
                        *sum_buffers(units, len(spans))],
        compiler_params=pltpu.CompilerParams(collective_id=1, has_side_effects=True, vmem_limit_bytes=VMEM),
        name="last_sums",
    )(d.reshape(2, 2, 4, 2, *d.shape[1:]), *done)


def _adamw(squares, *refs):
    g, (w, m, v, new_w, new_m, new_v) = refs[:4], (refs[i : i + 7] for i in range(4, 46, 7))
    count = 2 * UNITS * ROWS * D * 32
    factor = jnp.minimum(1.0, 0.5 * lax.rsqrt(squares[0:1, 0:1] / count + 1e-30))
    for layer in range(2):
        for i in range(7):
            for unit, piece in _pieces(i):
                where = (layer, *piece)
                sums, unit = (g[2 * layer], unit) if i < 4 else (g[2 * layer + 1], unit - 4)
                one = sums[unit].astype(F32) * factor
                mm = 0.9 * m[i][where] + 0.1 * one
                vv = 0.95 * v[i][where] + 0.05 * one * one
                old = w[i][where].astype(F32)
                new_w[i][where] = (old - 0.02 * (mm * lax.rsqrt(vv + 1e-8) + 0.1 * old)).astype(BF)
                new_m[i][where] = mm
                new_v[i][where] = vv


def _pieces(i):
    every = slice(None)
    if i < 4:
        return [(i, (every, every))]
    if i < 6:
        return [(4 * (i - 3) + j, (every, pl.ds(j * D, D))) for j in range(4)]
    return [(12 + j, (pl.ds(j * ROWS, ROWS), every)) for j in range(4)]


def adamw_all(weights, m, v, sums, squares):
    return pl.pallas_call(
        _adamw,
        out_shape=[_like(*w.shape) for w in weights] + [_like(*w.shape, dtype=F32) for w in weights] * 2,
        in_specs=[IN_VMEM] * 26,
        out_specs=[IN_VMEM] * 21,
        compiler_params=pltpu.CompilerParams(vmem_limit_bytes=VMEM),
        name="adamw_all",
    )(squares, *sums, *weights, *m, *v)


def _forward(spans, x_ref, cos_ref, sin_ref, *refs):
    shards, (kept, q_ref, k_ref, v_ref, o_ref, lse_ref, mid_ref, h1_ref), refs = refs[:7], refs[7:15], refs[15:]
    g, h_s, k_s, vt_s, top_s, mix_s, *sems = refs
    fetch = Fetch(spans, shards, g, kept, *sems)
    s = pl.program_id(0)
    layer, i = s // (2 * STEPS), s % STEPS
    here = pl.ds(pl.multiple_of(i * BLOCK, BLOCK), BLOCK)
    unit = layer * UNITS
    phase = s // STEPS
    early = attention_slots([(n, n) for n in range(STEPS)])
    late = [(n, f"part {j}") for n in range(STEPS, 2 * STEPS) for j in range(STEPS)] + attention_slots([(n + 2 * STEPS, n) for n in range(STEPS)])
    cut = FIRST + (UNITS - 4) // SPAN

    def tick(j):
        run_at(early, fetch.turns(FIRST, cut, LAG), s, j)
        run_at(late, fetch.turns(cut, len(spans), LAG), s, j)

    def weight(n):
        return g[:, :, :, :, unit + n].reshape(D, D)

    @pl.when(s == 0)
    def _():
        fetch.begin()
        for turn in fetch.turns(0, FIRST, 1):
            turn()

    @pl.when(phase == 0)
    def _():
        h_s[here, :] = x_ref[here, :]

    @pl.when(phase != 1)
    def _():
        a = _normed(h_s[here, :])[2]
        for n, out in enumerate((q_ref, k_ref, v_ref)):
            t = _dot(a, weight(n)).astype(BF)
            t = t if n == 2 else _turned(t.astype(F32), cos_ref[...], sin_ref[...])
            out[...] = t
            if n == 1:
                k_s[here, :] = t
            if n == 2:
                vt_s[:, here] = t.T
        top_s[...] = jnp.full_like(top_s, NEG)
        mix_s[...] = jnp.zeros_like(mix_s)
        ones = jnp.ones((8, BLOCK), BF)
        e = SCALE * LOG2E

        def block(j, masked):
            tick(DIAGONAL if masked else j)
            keys = pl.ds(pl.multiple_of(j * BLOCK, BLOCK), BLOCK)
            scores = [_dot_t(k_s[keys, _head(n)], q_ref[:, _head(n)]) for n in range(HEADS)]
            if masked:
                ok = lax.broadcasted_iota(jnp.int32, (BLOCK, BLOCK), 1) >= lax.broadcasted_iota(jnp.int32, (BLOCK, BLOCK), 0)
            weights, keeps = [], []
            for n, x in enumerate(scores):
                if masked:
                    x = jnp.where(ok, x, HIDDEN)
                old = top_s[n : n + 1, :]
                top = jnp.maximum(old, x.max(axis=0, keepdims=True))
                top_s[n : n + 1, :] = top
                weights.append(jnp.exp2((x - top) * e).astype(BF))
                keeps.append(jnp.exp2((old - top) * e))
            for n in range(HEADS):
                values = jnp.concatenate([vt_s[_head(n), keys], ones], axis=0)
                mix_s[n] = mix_s[n] * keeps[n] + _dot(values, weights[n])

        lax.fori_loop(0, i, lambda j, _: block(j, False), None)
        block(i, True)
        tick(AFTER)
        for n in range(HEADS):
            total = mix_s[n, HEAD : HEAD + 1, :]
            o_ref[:, _head(n)] = (mix_s[n, :HEAD, :] * (1 / total)).T.astype(BF)
            lse_ref[n : n + 1, :] = top_s[n : n + 1, :] * SCALE + jnp.log(total)
        mid = h_s[here, :] + _dot(o_ref[...], weight(3)).astype(BF)
        mid_ref[...] = mid
        h_s[here, :] = mid

    @pl.when(phase == 1)
    def _():
        mid = h_s[here, :]
        b = _normed(mid)[2]
        total = None
        for j in range(FF // BLOCK):
            tick(f"part {j}")
            gate, up = _dot(b, weight(4 + j)), _dot(b, weight(8 + j))
            hid = (gate * jax.nn.sigmoid(gate) * up).astype(BF)
            more = _dot(hid, g[j // 2, j % 2, :, :, 12:UNITS].reshape(D, D))
            total = more if j == 0 else total + more
        out = mid + total.astype(BF)
        h1_ref[...] = out
        h_s[here, :] = out

    @pl.when(s == pl.num_programs(0) - 1)
    def _():
        fetch.finish()


def forward(x, weights, cos, sin):
    spans = [(n * 4 // FIRST, (n + 1) * 4 // FIRST) for n in range(FIRST)] + [(n, n + SPAN) for n in range(4, 2 * UNITS, SPAN)]
    n = len(spans)

    def rows(width=D):
        return pl.BlockSpec((BLOCK, width), lambda s: (s % STEPS, 0))

    def place_of(s):
        t = s % (2 * STEPS)
        return s // (2 * STEPS), t - t // STEPS * (t - STEPS + 1)

    both = pl.BlockSpec((None, BLOCK, D), lambda s: (*place_of(s), 0))
    stats = pl.BlockSpec((None, HEADS, BLOCK), lambda s: (place_of(s)[0], 0, place_of(s)[1]))
    ffn_rows = pl.BlockSpec((BLOCK, D), lambda s: (s // STEPS % 2 * (s - STEPS) + s // STEPS // 2 * (STEPS - 1), 0))
    gathered = (2, 2, 4, 2, 2 * UNITS, ROWS, D)
    w, *rest = pl.pallas_call(
        functools.partial(_forward, spans),
        name="forward",
        grid=(3 * STEPS,),
        in_specs=[_whole(T, D), rows(HEAD), rows(HEAD)] + [ANY] * 7,
        out_specs=[ANY] + [both] * 4 + [stats, both, ffn_rows],
        out_shape=[_like(*gathered)] + [_like(2, T, D)] * 4 + [_like(2, HEADS, T, dtype=F32), _like(2, T, D), _like(T, D)],
        scratch_shapes=[pltpu.VMEM(gathered, BF), pltpu.VMEM((T, D), BF), pltpu.VMEM((T, D), BF), pltpu.VMEM((D, T), BF), pltpu.VMEM((HEADS, BLOCK), F32),
                        pltpu.VMEM((HEADS, HEAD + 8, BLOCK), F32)] + [pltpu.SemaphoreType.DMA(shape) for shape in ((2 * UNITS,), (n,), (n, 4, 3), (n, 4, 3))],
        compiler_params=pltpu.CompilerParams(dimension_semantics=("arbitrary",), vmem_limit_bytes=VMEM, collective_id=0, has_side_effects=True),
        cost_estimate=pl.CostEstimate(flops=50 * T * D * D, transcendentals=0, bytes_accessed=0),
    )(x, cos, sin, *weights)
    return w.reshape(D // ROWS, 2 * UNITS, ROWS, D), *rest


def solution(mesh):
    def step(x, dy, *arrays):
        weights, m, v = (arrays[i : i + 7] for i in (0, 7, 14))
        cos, sin = tables()
        w, q, k, vv, o, lse, mid, h1 = forward(x[0], weights, cos, sin)
        saved = (q, k, vv, o, lse)
        dmid, *by_ffn = ffn_back(dy[0], mid, w, 1)
        dh, by_attn, ffn_sum_1 = attn_back(h1, *saved, dmid, w, 1, cos, sin, (2, *by_ffn))
        dmid, *by_ffn, attn_sum_1 = ffn_back(dh, mid, w, 0, (3, by_attn))
        by_attn, ffn_sum_0 = attn_back(x[0], *saved, dmid, w, 0, cos, sin, (4, *by_ffn))
        attn_sum_0, squares = last_sums(by_attn, (ffn_sum_0, attn_sum_1, ffn_sum_1))
        return tuple(adamw_all(weights, m, v, (attn_sum_0, ffn_sum_0, attn_sum_1, ffn_sum_1), squares))

    states, cut = P(("rep", "dp"), None, None), P(None, "dp", None)
    return jax.shard_map(
        step,
        mesh=mesh,
        in_specs=(states, states) + (cut,) * 21,
        out_specs=(P("rep", "dp", None),) * 21,
        check_vma=False,
    )
```

```python
import functools

import jax
import jax.numpy as jnp
import numpy as np
from jax import lax
from jax.experimental import pallas as pl
from jax.experimental.pallas import tpu as pltpu
from jax.sharding import PartitionSpec as P

BF, F32 = jnp.bfloat16, jnp.float32
MESH = pl.DeviceIdType.MESH
ANY = pl.BlockSpec(memory_space=pl.ANY)
IN_VMEM = pl.BlockSpec(memory_space=pltpu.VMEM)
VMEM = 58 * 2**20
T, D, HEADS, HEAD, FF = 2048, 512, 4, 128, 2048
BLOCK = 512
STEPS = T // BLOCK
LAG, MOST, LAST, SPAN, FIRST, DELAY, AHEAD = 2, 2, 2, 2, 1, 2, 4
UNITS, ROWS = 16, 16
NEG = -1e30
HIDDEN = 2 * NEG
LOG2E = 1.4426950408889634
SCALE = HEAD**-0.5


def _dot(a, b, ca=1, cb=0):
    return lax.dot_general(a, b, (((ca,), (cb,)), ((), ())), preferred_element_type=F32)


def _dot_t(a, b):
    return _dot(a, b, 1, 1)


def _square(w):
    return w.reshape(D, D)


def _blocks(w):
    return w.astype(BF).reshape(D // ROWS, ROWS, D)


def _normed(h):
    wide = h.astype(F32)
    scale = lax.rsqrt(jnp.mean(wide * wide, -1, keepdims=True) + 1e-6)
    return wide, scale, (wide * scale).astype(BF)


def _norm_back(wide, scale, ct):
    return scale * (ct - wide * (scale * scale * jnp.mean(ct * wide, -1, keepdims=True)))


def _turned(t, cos, sin):
    parts = [t[:, n : n + HEAD] for n in range(0, D, HEAD)]
    return jnp.concatenate([p * cos + pltpu.roll(p, HEAD // 2, 1) * sin for p in parts], 1).astype(BF)


def _head(n):
    return pl.ds(n * HEAD, HEAD)


def _call(body, name, out, scratch=(), ins=(), outs=(), flops=0, parts=(), slots=(), lag=LAG):
    out, outs, ins, scratch, more, own = list(out), list(outs), list(ins), list(scratch), {}, body
    if parts:
        number, *parts = parts
        spans, units = sum_spans(parts, MOST)
        buffers = sum_buffers(units, len(spans))
        n_in, n_out = len(ins), len(out)
        ins += [ANY] * len(parts)
        out += [_like(units, ROWS, D)]
        outs += [_whole(units, ROWS, D)]
        parts = [d.reshape(2, 2, 4, 2, *d.shape[1:]) for d in parts]
        more = dict(collective_id=number, has_side_effects=True)

        def own(*refs):
            refs = list(refs)
            given, refs = refs[:n_in], refs[n_in:]
            ds, refs = refs[: len(parts)], refs[len(parts) :]
            made, total, kept = refs[:n_out], refs[n_out], refs[n_out + 1 :]
            traffic = Sums(lag, slots, spans, ds, total, *kept[len(scratch) :])
            body(*given, *made, *kept[: len(scratch)], traffic)

    run = pl.pallas_call(
        own, name=name, grid=(STEPS,), in_specs=ins, out_specs=outs, out_shape=out, scratch_shapes=scratch + (buffers if parts else []),
        compiler_params=pltpu.CompilerParams(dimension_semantics=("arbitrary",), vmem_limit_bytes=VMEM, **more),
        cost_estimate=pl.CostEstimate(flops=flops, transcendentals=0, bytes_accessed=0),
    )
    return lambda *given: run(*given, *parts)


def _rows(width=D):
    return pl.BlockSpec((BLOCK, width), lambda i: (i, 0))


def _whole(*shape):
    return pl.BlockSpec(shape, lambda i: (0,) * len(shape), pipeline_mode=pl.Buffered(1))


def _of(layer, *shape):
    return pl.BlockSpec((None, *shape), lambda i: (layer, *(0,) * len(shape)), pipeline_mode=pl.Buffered(1))


def _units(layer, kind):
    return pl.BlockSpec((D // ROWS, 4, ROWS, D), lambda i: (0, layer * 4 + kind, 0, 0), pipeline_mode=pl.Buffered(1))


def _like(*shape, dtype=BF):
    return jax.ShapeDtypeStruct(shape, dtype)


def _ffn_back(dh_ref, mid_ref, gate_ref, up_ref, down_ref, dmid_ref, dgate_ref, dup_ref, ddown_ref, b_s, bt_s, dht_s, db_s, dg_s, du_s, hid_s, traffic=None):
    j = pl.program_id(0)

    @pl.when(j == 0)
    def _():
        for i in range(STEPS):
            here = pl.ds(i * BLOCK, BLOCK)
            b = _normed(mid_ref[here, :])[2]
            b_s[here, :] = b
            bt_s[:, here] = b.T
            dht_s[:, here] = dh_ref[here, :].T
            db_s[here, :] = jnp.zeros((BLOCK, D), F32)

    gate_w, up_w, down_w = _square(gate_ref[:, 0]), _square(up_ref[:, 0]), _square(down_ref[...])

    def rows(i, _):
        here = pl.ds(pl.multiple_of(i * BLOCK, BLOCK), BLOCK)
        b = b_s[here, :]
        gate, up = _dot(b, gate_w), _dot(b, up_w)
        dhid = _dot_t(dh_ref[here, :], down_w).astype(BF).astype(F32)
        half = 0.5 * jnp.tanh(0.5 * gate) + 0.5
        silu = gate * half
        hid_s[here, :] = (silu * up).astype(BF)
        du = (dhid * silu).astype(BF)
        dg = (dhid * up * (half + silu * (1.0 - half))).astype(BF)
        dg_s[here, :] = dg
        du_s[here, :] = du
        db_s[here, :] += _dot_t(dg, gate_w) + _dot_t(du, up_w)

    if traffic:
        traffic.tick(j, BEFORE)
    lax.fori_loop(0, STEPS, rows, None, unroll=True)
    if traffic:
        traffic.tick(j, AFTER)
    dgate_ref[:, 0] = _blocks(_dot(bt_s[...], dg_s[...]))
    dup_ref[:, 0] = _blocks(_dot(bt_s[...], du_s[...]))
    ddown_ref[...] = _dot(dht_s[...], hid_s[...]).astype(BF).T.reshape(8, 4, ROWS, D)

    @pl.when(j == pl.num_programs(0) - 1)
    def _():
        for i in range(STEPS):
            here = pl.ds(i * BLOCK, BLOCK)
            wide, scale, _ = _normed(mid_ref[here, :])
            dmid_ref[here, :] = dh_ref[here, :] + _norm_back(wide, scale, db_s[here, :].astype(BF).astype(F32)).astype(BF)
        if traffic:
            traffic.finish()


def ffn_back(dh, mid, w, layer, parts=()):
    n = D // ROWS
    one = lambda kind: pl.BlockSpec((n, 1, ROWS, D), lambda j: (0, layer * UNITS + 4 * kind + j, 0, 0))
    some = pl.BlockSpec((n // 4, 4, ROWS, D), lambda j: (j, layer * 4 + 3, 0, 0))
    big = lambda dtype=BF: pltpu.VMEM((T, D), dtype)
    return _call(_ffn_back, "ffn_back", [_like(T, D)] + [_like(n, 4, ROWS, D)] * 3,
                 ins=[_whole(T, D), _of(layer, T, D), one(1), one(2), some],
                 outs=[_whole(T, D)] + [pl.BlockSpec((n, 1, ROWS, D), lambda j: (0, j, 0, 0))] * 2 + [pl.BlockSpec((n // 4, 4, ROWS, D), lambda j: (j, 0, 0, 0))],
                 scratch=[big(), pltpu.VMEM((D, T), BF), pltpu.VMEM((D, T), BF), big(F32), big(), big(), big()],
                 flops=64 * T * D * D, parts=parts, lag=1, slots=[(j, place) for j in range(STEPS) for place in (BEFORE, AFTER)])(dh, mid, w, w, w)


def _attn_back(first, h_ref, q_ref, k_ref, v_ref, o_ref, lse_ref, dmid_ref, w_ref, cos_ref, sin_ref, *refs):
    step = pl.program_id(0)
    iq = STEPS - 1 - step
    dh_ref, refs = (None, refs) if first else (refs[0], refs[1:])
    dw_ref, do_s, delta_s, dq_s, dk_s, dv_s, kt_s, dw_s = refs[:8]
    traffic = refs[8] if len(refs) > 8 else None
    e = SCALE * LOG2E

    @pl.when(step == 0)
    def _():
        for j in range(STEPS):
            here = pl.ds(j * BLOCK, BLOCK)
            kt_s[:, here] = k_ref[here, :].T
            dk_s[here, :] = jnp.zeros((BLOCK, D), F32)
            dv_s[here, :] = jnp.zeros((BLOCK, D), F32)
        dw_s[...] = jnp.zeros_like(dw_s)

    dmid, o = dmid_ref[...], o_ref[...]
    do = _dot_t(dmid, _square(w_ref[:, 3])).astype(BF)
    do_s[...] = do
    pick = (lax.broadcasted_iota(jnp.int32, (8, D), 1) // HEAD == lax.broadcasted_iota(jnp.int32, (8, D), 0)).astype(F32)
    both = do.astype(F32) * o.astype(F32)
    delta_s[...] = lax.dot_general(pick, both, (((1,), (1,)), ((), ())), precision=lax.Precision.HIGHEST, preferred_element_type=F32)
    dw_s[3] += _dot(o.T, dmid)
    dq_s[...] = jnp.zeros_like(dq_s)

    def block(j, masked):
        if traffic:
            traffic.tick(iq, DIAGONAL if masked else j)
        here = pl.ds(pl.multiple_of(j * BLOCK, BLOCK), BLOCK)
        scores = [_dot_t(k_ref[here, _head(n)], q_ref[:, _head(n)]) for n in range(HEADS)]
        dps = [_dot_t(v_ref[here, _head(n)], do_s[:, _head(n)]) for n in range(HEADS)]
        if masked:
            ok = lax.broadcasted_iota(jnp.int32, (BLOCK, BLOCK), 1) >= lax.broadcasted_iota(jnp.int32, (BLOCK, BLOCK), 0)
        for n in range(HEADS):
            p = jnp.exp2(scores[n] * e - lse_ref[n : n + 1, :] * LOG2E)
            if masked:
                p = jnp.where(ok, p, 0.0)
            ds = (p * (dps[n] - delta_s[n : n + 1, :])).astype(BF)
            dv_s[here, _head(n)] += _dot(p.astype(BF), do_s[:, _head(n)])
            dk_s[here, _head(n)] += _dot(ds, q_ref[:, _head(n)])
            dq_s[_head(n), :] += _dot(kt_s[_head(n), here], ds)

    lax.fori_loop(0, iq, lambda j, _: block(j, False), None)
    block(iq, True)
    if traffic:
        traffic.tick(iq, AFTER)
    here = pl.ds(pl.multiple_of(iq * BLOCK, BLOCK), BLOCK)
    wide, scale, a = _normed(h_ref[...])
    at = a.T
    dq = (dq_s[...] * SCALE).T.astype(BF)
    dk = (dk_s[here, :] * SCALE).astype(BF)
    da = None
    for n, t in enumerate((dq, dk, dv_s[here, :].astype(BF))):
        if n < 2:
            t = _turned(t.astype(F32), cos_ref[...], -sin_ref[...])
        dw_s[n] += _dot(at, t)
        if not first:
            back = _dot_t(t, _square(w_ref[:, n])).astype(BF)
            da = back if n == 0 else da + back
    if not first:
        dh_ref[...] = dmid + _norm_back(wide, scale, da.astype(F32)).astype(BF)

    @pl.when(step == STEPS - 1)
    def _():
        for n in range(4):
            dw_ref[:, n] = _blocks(dw_s[n])
        if traffic:
            traffic.finish()


def attn_back(h, q, k, v, o, lse, dmid, w, layer, cos, sin, parts=()):
    n, first = D // ROWS, layer == 0
    down = lambda width=D: pl.BlockSpec((BLOCK, width), lambda i: (STEPS - 1 - i, 0))
    ours = pl.BlockSpec((None, BLOCK, D), lambda i: (layer, STEPS - 1 - i, 0))
    every = _of(layer, T, D)
    big = pltpu.VMEM((T, D), F32)
    return _call(functools.partial(_attn_back, first), "attn_back", [_like(T, D)] * (not first) + [_like(n, 4, ROWS, D)],
                 ins=[down(), ours, every, every, ours, pl.BlockSpec((None, HEADS, BLOCK), lambda i: (layer, 0, STEPS - 1 - i)), down(), _units(layer, 0), down(HEAD), down(HEAD)],
                 outs=[down()] * (not first) + [_whole(n, 4, ROWS, D)],
                 scratch=[pltpu.VMEM((BLOCK, D), BF), pltpu.VMEM((8, BLOCK), F32), pltpu.VMEM((D, BLOCK), F32), big, big, pltpu.VMEM((D, T), BF), pltpu.VMEM((4, D, D), F32)],
                 flops=14 * T * T * D, parts=parts, slots=attention_slots([(i, i) for i in reversed(range(STEPS))]))(h, q, k, v, o, lse, dmid, w, cos, sin)


def tables():
    angle = np.arange(T)[:, None] * 10000.0 ** (-np.arange(HEAD // 2) / (HEAD // 2))
    cos, sin = np.cos(angle), np.sin(angle)
    return jnp.asarray(np.concatenate([cos, cos], 1), F32), jnp.asarray(np.concatenate([-sin, sin], 1), F32)


def place():
    me = lax.axis_index("dp")
    return me // 16, (me // 8) % 2, (me // 2) % 4, me % 2


def at(x, y, z, c):
    return {"dp": ((x * 2 + y) * 4 + z) * 2 + c}


def peers(x, y, z, c):
    return [at(x, y, (z + n) % 4, c) for n in (1, 2, 3)] + [at(1 - x, y, z, c), at(x, 1 - y, z, c), at(x, y, z, 1 - c)]


def greet(others):
    for other in others:
        pl.semaphore_signal(pltpu.get_barrier_semaphore(), inc=1, device_id=other, device_id_type=MESH)


def wait_for(others):
    pl.semaphore_wait(pltpu.get_barrier_semaphore(), len(others))


def remote(src, dst, send, recv, to):
    return pltpu.make_async_remote_copy(src_ref=src, dst_ref=dst, send_sem=send, recv_sem=recv, device_id=to, device_id_type=MESH)


def halves(span, n):
    a, b = span
    m = (a + b + n % 2) // 2
    return [(first, pl.ds(lo, hi - lo)) for first, lo, hi in ((True, a, m), (False, m, b)) if hi > lo]


def stretch(span):
    return pl.ds(span[0], span[1] - span[0])


def shard_pieces(refs, layer):
    wq, wk, wv, wo, gate, up, down = refs
    found = [(n, w.at[layer]) for n, w in enumerate((wq, wk, wv, wo))]
    for j in range(4):
        found.append((4 + j, gate.at[layer, :, pl.ds(j * D, D)]))
        found.append((8 + j, up.at[layer, :, pl.ds(j * D, D)]))
        found.append((12 + j, down.at[layer, pl.ds(j * ROWS, ROWS), :]))
    return [(unit + layer * UNITS, piece) for unit, piece in found]


class Fetch:
    def __init__(self, spans, shards, g, kept, own_sem, kept_sem, send_sem, recv_sem):
        self.spans, self.shards, self.g, self.kept = spans, shards, g, kept
        self.own_sem, self.kept_sem, self.send_sem, self.recv_sem = own_sem, kept_sem, send_sem, recv_sem
        self.place = place()

    def loads(self):
        pieces = [piece for layer in range(2) for piece in shard_pieces(self.shards, layer)]
        return [pltpu.make_async_copy(piece, self.g.at[(*self.place, unit)], self.own_sem.at[unit]) for unit, piece in pieces]

    def keep(self, n):
        u = stretch(self.spans[n])
        return pltpu.make_async_copy(self.g.at[:, :, :, :, u], self.kept.at[:, :, :, :, u], self.kept_sem.at[n])

    def copies(self, n, step, arriving=False):
        (x, y, z, c), g, span = self.place, self.g, self.spans[n]
        u, by_x, by_y = stretch(span), at(1 - x, y, z, c), at(x, 1 - y, z, c)
        xx, yy, cc = (1 - x, 1 - y, 1 - c) if arriving else (x, y, c)
        if step == 0:
            todo = [(g.at[x, y, (z + 4 - k) % 4 if arriving else z, c, u], at(x, y, (z + k) % 4, c)) for k in (1, 2, 3)]
        elif step == 1:
            todo = [(g.at[xx, y, :, c, u], by_x) if first else (g.at[x, yy, :, c, u], by_y) for first, u in halves(span, n)]
        elif step == 2:
            todo = [(g.at[:, yy, :, c, u], by_y) if first else (g.at[xx, :, :, c, u], by_x) for first, u in halves(span, n)]
        else:
            todo = [(g.at[:, :, :, cc, u], at(x, y, z, 1 - c))]
        return [remote(piece, piece, self.send_sem.at[n, step, i], self.recv_sem.at[n, step, i], to) for i, (piece, to) in enumerate(todo)]

    def start(self, n, step):
        for copy in self.copies(n, step):
            copy.start()

    def begin(self):
        for load in self.loads():
            load.start()
        greet(peers(*self.place))
        wait_for(peers(*self.place))
        for load in self.loads():
            load.wait()
    def turns(self):
        found = {}
        for step in (3, 2, 1, 0, -1):
            for n, (a, _) in enumerate(self.spans):
                turn = n + DELAY * (a >= UNITS) + (-AHEAD if step < 0 else step if n < FIRST else LAG * step)
                found.setdefault(max(turn, 0) - (turn < 0), []).append((n, step))

        def turn(now):
            for n, step in now:
                for copy in self.copies(n, step, True) if step >= 0 else ():
                    copy.wait_recv()
                if step < 3:
                    self.start(n, step + 1)
                else:
                    self.keep(n).start()

        done, named = 0, []
        for n in sorted(found):
            named.append((functools.partial(turn, found[n]), done))
            done = max([done] + [self.spans[m][1] for m, step in found[n] if step == 3])
        return named

    def finish(self):
        for n in range(len(self.spans)):
            self.keep(n).wait()
            for step in range(4):
                for copy in self.copies(n, step):
                    copy.wait_send()


BEFORE, DIAGONAL, AFTER = "before", "diagonal", "after"


def run_at(slots, turns, i, j):
    for n, turn in enumerate(turns):
        a, b = slots[n * len(slots) // len(turns)]
        if isinstance(b, str) or isinstance(j, str):
            if b == j:
                pl.when(i == a)(turn)
        else:
            pl.when(i * UNITS + j == a * UNITS + b)(turn)


def attention_slots(steps):
    return [(s, j) for s, n in steps for j in (*range(n), DIAGONAL, AFTER)]


def _add_into(total, more):
    lead = total.shape[:-4]

    def one(i, _):
        where = []
        for n in reversed(lead):
            where = [i % n] + where
            i = i // n
        where = tuple(where)
        total[where] = (total[where].astype(F32) + more[where].astype(F32)).astype(BF)

    lax.fori_loop(0, int(np.prod(lead, dtype=int)), one, None)


def sum_spans(parts, most):
    spans, units = [], 0
    for which, d in enumerate(parts):
        n = d.shape[1]
        spans += [(which, a, units + a, units + min(a + most, n)) for a in range(0, n, most)]
        units += n
    return spans, units


def sum_buffers(units, n):
    return [pltpu.VMEM((*lead, units, ROWS, D), BF) for lead in ((2, 2, 4), (2, 2, 4), (2, 4), (4,), (3,))] + [
        pltpu.SemaphoreType.DMA(shape) for shape in ((n,), (n, 4, 3), (n, 4, 3))]


class Sums:
    def __init__(self, lag, slots, spans, ds, g, *buffers):
        self.lag, self.slots, self.spans, self.ds, self.g = lag, slots, spans, ds, g
        self.s, self.r1, self.r2, self.r3, self.r4, self.local_sem, self.send_sem, self.recv_sem = buffers
        self.place = place()

    def own(self, n, core):
        which, first, a, b = self.spans[n]
        return self.ds[which].at[:, :, :, core, pl.ds(first, b - a)]

    def load(self, n):
        return pltpu.make_async_copy(self.own(n, self.place[3]), self.s.at[:, :, :, stretch(self.spans[n][2:])], self.local_sem.at[n])

    def copies(self, n, step):
        (x, y, z, c), s, span = self.place, self.s, self.spans[n][2:]
        u, by_x, by_y = stretch(span), at(1 - x, y, z, c), at(x, 1 - y, z, c)
        if step == 0:
            todo = [(self.own(n, 1 - c), self.r1.at[:, :, :, u], at(x, y, z, 1 - c))]
        elif step == 1:
            todo = [(s.at[1 - x, :, :, u] if first else s.at[:, 1 - y, :, u], self.r2.at[:, :, u], by_x if first else by_y) for first, u in halves(span, n)]
        elif step == 2:
            todo = [(s.at[x, 1 - y, :, u] if first else s.at[1 - x, y, :, u], self.r3.at[:, u], by_y if first else by_x) for first, u in halves(span, n)]
        else:
            todo = [(s.at[x, y, (z + k) % 4, u], self.r4.at[k - 1, u], at(x, y, (z + k) % 4, c)) for k in (1, 2, 3)]
        return [remote(a, b, self.send_sem.at[n, step, i], self.recv_sem.at[n, step, i], to) for i, (a, b, to) in enumerate(todo)]

    def add(self, n, step):
        (x, y, z, c), s, span = self.place, self.s, self.spans[n][2:]
        u = stretch(span)
        if step == 0:
            _add_into(s.at[:, :, :, u], self.r1.at[:, :, :, u])
        elif step == 1:
            for first, u in halves(span, n):
                _add_into(s.at[x, :, :, u] if first else s.at[:, y, :, u], self.r2.at[:, :, u])
        elif step == 2:
            _add_into(s.at[x, y, :, u], self.r3.at[:, u])
        else:
            out = s[x, y, z, u].astype(F32)
            for k in range(3):
                out = out + self.r4[k, u].astype(F32)
            self.g[u] = out.astype(BF)

    def begin(self):
        for n in range(len(self.spans)):
            self.load(n).start()
        greet(peers(*self.place))

    def send(self):
        wait_for(peers(*self.place))
        for n in range(len(self.spans)):
            self.start(n, 0)

    def start(self, n, step):
        for copy in self.copies(n, step):
            copy.start()

    def turns(self):
        found = [self.begin, self.send]
        for tick in range(len(self.spans) + 3 * self.lag):
            now = [(tick - self.lag * step, step) for step in range(4) if 0 <= tick - self.lag * step < len(self.spans)]

            def turn(now=now):
                for n, step in now:
                    if step == 0:
                        self.load(n).wait()
                    for copy in self.copies(n, step):
                        copy.wait_recv()
                    self.add(n, step)
                    if step < 3:
                        self.start(n, step + 1)

            found.append(turn)
        return found

    def tick(self, i, j):
        run_at(self.slots, self.turns(), i, j)

    def finish(self):
        for n in range(len(self.spans)):
            for step in range(4):
                for copy in self.copies(n, step):
                    copy.wait_send()


def _last_sums(spans, d, *refs):
    *done, g, squares, sq, sq_all, sq_send, sq_recv = refs[: -len(sum_buffers(1, 1))]
    traffic = Sums(1, (), spans, [d], g, *refs[-len(sum_buffers(1, 1)) :])
    me = lax.axis_index("dp")
    everyone = [{"dp": (me + k) % 32} for k in range(1, 32)]
    greet(everyone)
    for n in range(len(spans)):
        traffic.load(n).start()
    wait_for(everyone)
    for n in range(len(spans)):
        traffic.start(n, 0)
    sq[...] = jnp.zeros_like(sq)

    def squared(ref):
        def one(i, total):
            wide = ref[i].astype(F32)
            return total + (wide * wide).reshape(ROWS // 8, 8, D // HEAD, HEAD).sum((0, 2))

        sq[...] += lax.fori_loop(0, ref.shape[0], one, jnp.zeros((8, HEAD), F32))

    for ref in done:
        squared(ref)
    for turn in traffic.turns()[2:]:
        turn()
    squared(g)
    spread = [remote(sq, sq_all.at[k + 1], sq_send.at[k], sq_recv.at[k], to) for k, to in enumerate(everyone)]
    for copy in spread:
        copy.start()
    for copy in spread:
        copy.wait_recv()
    sq_all[0] = sq[...]
    squares[...] = jnp.full((8, HEAD), jnp.sum(sq_all[...]))
    for copy in spread:
        copy.wait_send()
    traffic.finish()


def last_sums(d, done):
    spans, units = sum_spans([d], LAST)
    return pl.pallas_call(
        functools.partial(_last_sums, spans),
        out_shape=[_like(units, ROWS, D), _like(8, HEAD, dtype=F32)],
        in_specs=[ANY] + [IN_VMEM] * len(done),
        out_specs=[IN_VMEM, IN_VMEM],
        scratch_shapes=[pltpu.VMEM((8, HEAD), F32), pltpu.VMEM((32, 8, HEAD), F32), pltpu.SemaphoreType.DMA((31,)), pltpu.SemaphoreType.DMA((31,)),
                        *sum_buffers(units, len(spans))],
        compiler_params=pltpu.CompilerParams(collective_id=1, has_side_effects=True, vmem_limit_bytes=VMEM),
        name="last_sums",
    )(d.reshape(2, 2, 4, 2, *d.shape[1:]), *done)


def _adamw(squares, *refs):
    g, (w, m, v, new_w, new_m, new_v) = refs[:4], (refs[i : i + 7] for i in range(4, 46, 7))
    count = 2 * UNITS * ROWS * D * 32
    factor = jnp.minimum(1.0, 0.5 * lax.rsqrt(squares[0:1, 0:1] / count + 1e-30))
    for layer in range(2):
        for i in range(7):
            for unit, piece in _pieces(i):
                where = (layer, *piece)
                one = _sum_of(g, layer, unit).astype(F32) * factor
                mm = 0.9 * m[i][where] + 0.1 * one
                vv = 0.95 * v[i][where] + 0.05 * one * one
                old = w[i][where].astype(F32)
                new_w[i][where] = (old - 0.02 * (mm * lax.rsqrt(vv + 1e-8) + 0.1 * old)).astype(BF)
                new_m[i][where] = mm
                new_v[i][where] = vv


def _sum_of(sums, layer, unit):
    if layer == 0:
        return sums[0][unit] if unit < 4 else sums[1][unit - 4]
    return sums[3][unit + 4] if unit < 4 else sums[2][unit - 4] if unit < 12 else sums[3][unit - 12]


def _pieces(i):
    every = slice(None)
    if i < 4:
        return [(i, (every, every))]
    if i < 6:
        return [(4 * (i - 3) + j, (every, pl.ds(j * D, D))) for j in range(4)]
    return [(12 + j, (pl.ds(j * ROWS, ROWS), every)) for j in range(4)]


def adamw_all(weights, m, v, sums, squares):
    return pl.pallas_call(
        _adamw,
        out_shape=[_like(*w.shape) for w in weights] + [_like(*w.shape, dtype=F32) for w in weights] * 2,
        in_specs=[IN_VMEM] * 26,
        out_specs=[IN_VMEM] * 21,
        compiler_params=pltpu.CompilerParams(vmem_limit_bytes=VMEM),
        name="adamw_all",
    )(squares, *sums, *weights, *m, *v)


def _forward(spans, x_ref, cos_ref, sin_ref, *refs):
    shards, (kept, q_ref, k_ref, v_ref, o_ref, lse_ref, mid_ref, h1_ref), refs = refs[:7], refs[7:15], refs[15:]
    g, h_s, k_s, vt_s, top_s, mix_s, *sems = refs
    fetch = Fetch(spans, shards, g, kept, *sems)
    s = pl.program_id(0)
    layer, i = s // (2 * STEPS), s % STEPS
    here = pl.ds(pl.multiple_of(i * BLOCK, BLOCK), BLOCK)
    unit = layer * UNITS
    phase = s // STEPS
    turns = fetch.turns()
    ready = [turn for turn, unit in turns if unit < 4]
    early = [turn for turn, unit in turns if 4 <= unit < UNITS]
    middle = [turn for turn, unit in turns if UNITS <= unit < UNITS + 4]
    late = [turn for turn, unit in turns if unit >= UNITS + 4]

    def tick(j):
        run_at(attention_slots([(n, n) for n in range(STEPS)]), early, s, j)
        run_at([(n, f"part {j}") for n in range(STEPS, 2 * STEPS) for j in range(STEPS)], middle, s, j)
        run_at(attention_slots([(n + 2 * STEPS, n) for n in range(STEPS)]), late, s, j)

    def weight(n):
        return g[:, :, :, :, unit + n].reshape(D, D)

    @pl.when(s == 0)
    def _():
        fetch.begin()
        for turn in ready:
            turn()

    @pl.when(phase == 0)
    def _():
        h_s[here, :] = x_ref[here, :]

    @pl.when(phase != 1)
    def _():
        a = _normed(h_s[here, :])[2]
        for n, out in enumerate((q_ref, k_ref, v_ref)):
            t = _dot(a, weight(n)).astype(BF)
            t = t if n == 2 else _turned(t.astype(F32), cos_ref[...], sin_ref[...])
            out[...] = t
            if n == 1:
                k_s[here, :] = t
            if n == 2:
                vt_s[:, here] = t.T
        top_s[...] = jnp.full_like(top_s, NEG)
        mix_s[...] = jnp.zeros_like(mix_s)
        ones = jnp.ones((8, BLOCK), BF)
        e = SCALE * LOG2E

        def block(j, masked):
            tick(DIAGONAL if masked else j)
            keys = pl.ds(pl.multiple_of(j * BLOCK, BLOCK), BLOCK)
            scores = [_dot_t(k_s[keys, _head(n)], q_ref[:, _head(n)]) for n in range(HEADS)]
            if masked:
                ok = lax.broadcasted_iota(jnp.int32, (BLOCK, BLOCK), 1) >= lax.broadcasted_iota(jnp.int32, (BLOCK, BLOCK), 0)
            weights, keeps = [], []
            for n, x in enumerate(scores):
                if masked:
                    x = jnp.where(ok, x, HIDDEN)
                old = top_s[n : n + 1, :]
                top = jnp.maximum(old, x.max(axis=0, keepdims=True))
                top_s[n : n + 1, :] = top
                weights.append(jnp.exp2((x - top) * e).astype(BF))
                keeps.append(jnp.exp2((old - top) * e))
            for n in range(HEADS):
                values = jnp.concatenate([vt_s[_head(n), keys], ones], axis=0)
                mix_s[n] = mix_s[n] * keeps[n] + _dot(values, weights[n])

        lax.fori_loop(0, i, lambda j, _: block(j, False), None)
        block(i, True)
        tick(AFTER)
        for n in range(HEADS):
            total = mix_s[n, HEAD : HEAD + 1, :]
            o_ref[:, _head(n)] = (mix_s[n, :HEAD, :] * (1 / total)).T.astype(BF)
            lse_ref[n : n + 1, :] = top_s[n : n + 1, :] * SCALE + jnp.log(total)
        mid = h_s[here, :] + _dot(o_ref[...], weight(3)).astype(BF)
        mid_ref[...] = mid
        h_s[here, :] = mid

    @pl.when(phase == 1)
    def _():
        mid = h_s[here, :]
        b = _normed(mid)[2]
        total = None
        for j in range(FF // BLOCK):
            tick(f"part {j}")
            gate, up = _dot(b, weight(4 + j)), _dot(b, weight(8 + j))
            hid = (gate * (0.5 * jnp.tanh(0.5 * gate) + 0.5) * up).astype(BF)
            more = _dot(hid, g[j // 2, j % 2, :, :, 12:UNITS].reshape(D, D))
            total = more if j == 0 else total + more
        out = mid + total.astype(BF)
        h1_ref[...] = out
        h_s[here, :] = out

    @pl.when(s == pl.num_programs(0) - 1)
    def _():
        fetch.finish()


def forward(x, weights, cos, sin):
    spans = [(n * 4 // FIRST, (n + 1) * 4 // FIRST) for n in range(FIRST)] + [(n, n + SPAN) for n in range(4, 2 * UNITS, SPAN)]
    n = len(spans)

    def rows(width=D):
        return pl.BlockSpec((BLOCK, width), lambda s: (s % STEPS, 0))

    def place_of(s):
        t = s % (2 * STEPS)
        return s // (2 * STEPS), t - t // STEPS * (t - STEPS + 1)

    both = pl.BlockSpec((None, BLOCK, D), lambda s: (*place_of(s), 0))
    stats = pl.BlockSpec((None, HEADS, BLOCK), lambda s: (place_of(s)[0], 0, place_of(s)[1]))
    ffn_rows = pl.BlockSpec((BLOCK, D), lambda s: (s // STEPS % 2 * (s - STEPS) + s // STEPS // 2 * (STEPS - 1), 0))
    gathered = (2, 2, 4, 2, 2 * UNITS, ROWS, D)
    w, *rest = pl.pallas_call(
        functools.partial(_forward, spans),
        name="forward",
        grid=(3 * STEPS,),
        in_specs=[_whole(T, D), rows(HEAD), rows(HEAD)] + [ANY] * 7,
        out_specs=[ANY] + [both] * 4 + [stats, both, ffn_rows],
        out_shape=[_like(*gathered)] + [_like(2, T, D)] * 4 + [_like(2, HEADS, T, dtype=F32), _like(2, T, D), _like(T, D)],
        scratch_shapes=[pltpu.VMEM(gathered, BF), pltpu.VMEM((T, D), BF), pltpu.VMEM((T, D), BF), pltpu.VMEM((D, T), BF), pltpu.VMEM((HEADS, BLOCK), F32),
                        pltpu.VMEM((HEADS, HEAD + 8, BLOCK), F32)] + [pltpu.SemaphoreType.DMA(shape) for shape in ((2 * UNITS,), (n,), (n, 4, 3), (n, 4, 3))],
        compiler_params=pltpu.CompilerParams(dimension_semantics=("arbitrary",), vmem_limit_bytes=VMEM, collective_id=0, has_side_effects=True),
        cost_estimate=pl.CostEstimate(flops=50 * T * D * D, transcendentals=0, bytes_accessed=0),
    )(x, cos, sin, *weights)
    return w.reshape(D // ROWS, 2 * UNITS, ROWS, D), *rest


def solution(mesh):
    def step(x, dy, *arrays):
        weights, m, v = (arrays[i : i + 7] for i in (0, 7, 14))
        cos, sin = tables()
        w, q, k, vv, o, lse, mid, h1 = forward(x[0], weights, cos, sin)
        saved = (q, k, vv, o, lse)
        dmid, gate_1, up_1, down_1 = ffn_back(dy[0], mid, w, 1)
        dh, attn_1, some_1 = attn_back(h1, *saved, dmid, w, 1, cos, sin, (2, gate_1, up_1))
        dmid, *ffn_0, rest_1 = ffn_back(dh, mid, w, 0, (3, down_1, attn_1))
        attn_0, ffn_0 = attn_back(x[0], *saved, dmid, w, 0, cos, sin, (4, *ffn_0))
        attn_0, squares = last_sums(attn_0, (ffn_0, some_1, rest_1))
        return tuple(adamw_all(weights, m, v, (attn_0, ffn_0, some_1, rest_1), squares))

    states, cut = P(("rep", "dp"), None, None), P(None, "dp", None)
    return jax.shard_map(
        step,
        mesh=mesh,
        in_specs=(states, states) + (cut,) * 21,
        out_specs=(P("rep", "dp", None),) * 21,
        check_vma=False,
    )
```

```python
import functools

import jax
import jax.numpy as jnp
import numpy as np
from jax import lax
from jax.experimental import pallas as pl
from jax.experimental.pallas import tpu as pltpu
from jax.sharding import PartitionSpec as P

BF, F32 = jnp.bfloat16, jnp.float32
MESH = pl.DeviceIdType.MESH
ANY = pl.BlockSpec(memory_space=pl.ANY)
IN_VMEM = pl.BlockSpec(memory_space=pltpu.VMEM)
VMEM = 58 * 2**20
T, D, HEADS, HEAD, FF = 2048, 512, 4, 128, 2048
BLOCK = 512
STEPS = T // BLOCK
LAG, MOST, LAST, SPAN, FIRST, DELAY, AHEAD = 2, 2, 2, 2, 1, 2, 4
FINE = 64
PARTS = 3
UNITS, ROWS = 16, 16
NEG = -1e30
HIDDEN = 2 * NEG
LOG2E = 1.4426950408889634
SCALE = HEAD**-0.5


def _dot(a, b, ca=1, cb=0):
    return lax.dot_general(a, b, (((ca,), (cb,)), ((), ())), preferred_element_type=F32)


def _dot_t(a, b):
    return _dot(a, b, 1, 1)


def _square(w):
    return w.reshape(D, D)


def _blocks(w):
    return w.astype(BF).reshape(D // ROWS, ROWS, D)


def _normed(h):
    wide = h.astype(F32)
    scale = lax.rsqrt(jnp.mean(wide * wide, -1, keepdims=True) + 1e-6)
    return wide, scale, (wide * scale).astype(BF)


def _norm_back(wide, scale, ct):
    return scale * (ct - wide * (scale * scale * jnp.mean(ct * wide, -1, keepdims=True)))


def _turned(t, cos, sin):
    parts = [t[:, n : n + HEAD] for n in range(0, D, HEAD)]
    return jnp.concatenate([p * cos + pltpu.roll(p, HEAD // 2, 1) * sin for p in parts], 1).astype(BF)


def _head(n):
    return pl.ds(n * HEAD, HEAD)


def _call(body, name, out, scratch=(), ins=(), outs=(), flops=0, parts=(), slots=(), lag=LAG):
    out, outs, ins, scratch, more, own = list(out), list(outs), list(ins), list(scratch), {}, body
    if parts:
        number, *parts = parts
        spans, units = sum_spans(parts, MOST)
        buffers = sum_buffers(units, len(spans))
        n_in, n_out = len(ins), len(out)
        ins += [ANY] * len(parts)
        out += [_like(units, ROWS, D)]
        outs += [_whole(units, ROWS, D)]
        parts = [d.reshape(2, 2, 4, 2, *d.shape[1:]) for d in parts]
        more = dict(collective_id=number, has_side_effects=True)

        def own(*refs):
            refs = list(refs)
            given, refs = refs[:n_in], refs[n_in:]
            ds, refs = refs[: len(parts)], refs[len(parts) :]
            made, total, kept = refs[:n_out], refs[n_out], refs[n_out + 1 :]
            traffic = Sums(lag, slots, spans, ds, total, *kept[len(scratch) :])
            body(*given, *made, *kept[: len(scratch)], traffic)

    run = pl.pallas_call(
        own, name=name, grid=(STEPS,), in_specs=ins, out_specs=outs, out_shape=out, scratch_shapes=scratch + (buffers if parts else []),
        compiler_params=pltpu.CompilerParams(dimension_semantics=("arbitrary",), vmem_limit_bytes=VMEM, **more),
        cost_estimate=pl.CostEstimate(flops=flops, transcendentals=0, bytes_accessed=0),
    )
    return lambda *given: run(*given, *parts)


def _rows(width=D):
    return pl.BlockSpec((BLOCK, width), lambda i: (i, 0))


def _whole(*shape):
    return pl.BlockSpec(shape, lambda i: (0,) * len(shape), pipeline_mode=pl.Buffered(1))


def _of(layer, *shape):
    return pl.BlockSpec((None, *shape), lambda i: (layer, *(0,) * len(shape)), pipeline_mode=pl.Buffered(1))


def _angle_specs():
    return [_whole(2, n, HEAD) for n in (FINE, T // FINE)]


def _units(layer, kind):
    return pl.BlockSpec((D // ROWS, 4, ROWS, D), lambda i: (0, layer * 4 + kind, 0, 0), pipeline_mode=pl.Buffered(1))


def _like(*shape, dtype=BF):
    return jax.ShapeDtypeStruct(shape, dtype)


def _ffn_back(dh_ref, mid_ref, gate_ref, up_ref, down_ref, dmid_ref, dgate_ref, dup_ref, ddown_ref, b_s, bt_s, dht_s, db_s, dg_s, du_s, hid_s, traffic=None):
    j = pl.program_id(0)

    @pl.when(j == 0)
    def _():
        for i in range(STEPS):
            here = pl.ds(i * BLOCK, BLOCK)
            b = _normed(mid_ref[here, :])[2]
            b_s[here, :] = b
            bt_s[:, here] = b.T
            dht_s[:, here] = dh_ref[here, :].T
            db_s[here, :] = jnp.zeros((BLOCK, D), F32)

    gate_w, up_w, down_w = _square(gate_ref[:, 0]), _square(up_ref[:, 0]), _square(down_ref[...])

    def rows(i, _):
        here = pl.ds(pl.multiple_of(i * BLOCK, BLOCK), BLOCK)
        b = b_s[here, :]
        gate, up = _dot(b, gate_w), _dot(b, up_w)
        dhid = _dot_t(dh_ref[here, :], down_w).astype(BF).astype(F32)
        half = 0.5 * jnp.tanh(0.5 * gate) + 0.5
        silu = gate * half
        hid_s[here, :] = (silu * up).astype(BF)
        du = (dhid * silu).astype(BF)
        dg = (dhid * up * (half + silu * (1.0 - half))).astype(BF)
        dg_s[here, :] = dg
        du_s[here, :] = du
        db_s[here, :] += _dot_t(dg, gate_w) + _dot_t(du, up_w)

    if traffic:
        traffic.tick(j, BEFORE)
    lax.fori_loop(0, STEPS, rows, None, unroll=True)
    if traffic:
        traffic.tick(j, AFTER)
    dgate_ref[:, 0] = _blocks(_dot(bt_s[...], dg_s[...]))
    dup_ref[:, 0] = _blocks(_dot(bt_s[...], du_s[...]))
    ddown_ref[...] = _dot(dht_s[...], hid_s[...]).astype(BF).T.reshape(8, 4, ROWS, D)

    @pl.when(j == pl.num_programs(0) - 1)
    def _():
        for i in range(STEPS):
            here = pl.ds(i * BLOCK, BLOCK)
            wide, scale, _ = _normed(mid_ref[here, :])
            dmid_ref[here, :] = dh_ref[here, :] + _norm_back(wide, scale, db_s[here, :].astype(BF).astype(F32)).astype(BF)
        if traffic:
            traffic.finish()


def ffn_back(dh, mid, w, layer, parts=()):
    n = D // ROWS
    one = lambda kind: pl.BlockSpec((n, 1, ROWS, D), lambda j: (0, layer * UNITS + 4 * kind + j, 0, 0))
    some = pl.BlockSpec((n // 4, 4, ROWS, D), lambda j: (j, layer * 4 + 3, 0, 0))
    big = lambda dtype=BF: pltpu.VMEM((T, D), dtype)
    return _call(_ffn_back, "ffn_back", [_like(T, D)] + [_like(n, 4, ROWS, D)] * 3,
                 ins=[_whole(T, D), _of(layer, T, D), one(1), one(2), some],
                 outs=[_whole(T, D)] + [pl.BlockSpec((n, 1, ROWS, D), lambda j: (0, j, 0, 0))] * 2 + [pl.BlockSpec((n // 4, 4, ROWS, D), lambda j: (j, 0, 0, 0))],
                 scratch=[big(), pltpu.VMEM((D, T), BF), pltpu.VMEM((D, T), BF), big(F32), big(), big(), big()],
                 flops=64 * T * D * D, parts=parts, lag=1, slots=[(0, BEFORE)] + [(j, place) for j in range(1, STEPS) for place in (BEFORE, AFTER)])(dh, mid, w, w, w)


def _attn_back(first, h_ref, q_ref, k_ref, v_ref, o_ref, lse_ref, dmid_ref, w_ref, fine_ref, coarse_ref, *refs):
    step = pl.program_id(0)
    iq = STEPS - 1 - step
    dh_ref, refs = (None, refs) if first else (refs[0], refs[1:])
    dw_ref, do_s, dot_s, qt_s, cols_s, dq_s, dkt_s, dvt_s, dw_s, *traffic = refs
    traffic = traffic[0] if traffic else None
    e = SCALE * LOG2E

    @pl.when(step == 0)
    def _():
        dkt_s[...] = jnp.zeros_like(dkt_s)
        dvt_s[...] = jnp.zeros_like(dvt_s)
        dw_s[...] = jnp.zeros_like(dw_s)

    dmid, o = dmid_ref[...], o_ref[...]
    do = _dot_t(dmid, _square(w_ref[:, 3])).astype(BF)
    do_s[...], dot_s[...], qt_s[...] = do, do.T, q_ref[...].T
    pick = (lax.broadcasted_iota(jnp.int32, (8, D), 1) // HEAD == lax.broadcasted_iota(jnp.int32, (8, D), 0)).astype(F32)
    both = do.astype(F32) * o.astype(F32)
    delta = lax.dot_general(pick, both, (((1,), (1,)), ((), ())), precision=lax.Precision.HIGHEST, preferred_element_type=F32)
    parts = []
    for n in range(HEADS):
        for left in (lse_ref[n : n + 1, :] * (-1 / SCALE), -delta[n : n + 1, :]):
            for _ in range(PARTS):
                parts.append(left.astype(BF).astype(F32))
                left = left - parts[-1]
    parts.append(jnp.zeros((HEAD - len(parts), BLOCK), F32))
    cols_s[...] = jnp.concatenate(parts, 0).T.astype(BF)
    dw_s[3] += _dot(o.T, dmid)
    dq_s[...] = jnp.zeros_like(dq_s)

    def block(j, masked):
        if traffic:
            traffic.tick(iq, DIAGONAL if masked else j)
        here = pl.ds(pl.multiple_of(j * BLOCK, BLOCK), BLOCK)
        lane = lax.broadcasted_iota(jnp.int32, (BLOCK, HEAD), 1) // PARTS

        def beside(a, b, n):
            return _dot_t(jnp.concatenate([a, cols_s[...]], 1), jnp.concatenate([b, (lane == n).astype(F32).astype(BF)], 1))

        scores = [beside(q_ref[:, _head(n)], k_ref[here, _head(n)], 2 * n) for n in range(HEADS)]
        dps = [beside(do_s[:, _head(n)], v_ref[here, _head(n)], 2 * n + 1) for n in range(HEADS)]
        if masked:
            ok = lax.broadcasted_iota(jnp.int32, (BLOCK, BLOCK), 0) >= lax.broadcasted_iota(jnp.int32, (BLOCK, BLOCK), 1)
        for n in range(HEADS):
            p = jnp.exp2(scores[n] * e)
            if masked:
                p = jnp.where(ok, p, 0.0)
            ds = (p * dps[n]).astype(BF)
            dvt_s[_head(n), here] += _dot(dot_s[_head(n), :], p.astype(BF))
            dkt_s[_head(n), here] += _dot(qt_s[_head(n), :], ds)
            dq_s[:, _head(n)] += _dot(ds, k_ref[here, _head(n)])

    lax.fori_loop(0, iq, lambda j, _: block(j, False), None)
    block(iq, True)
    if traffic:
        traffic.tick(iq, AFTER)
    here = pl.ds(pl.multiple_of(iq * BLOCK, BLOCK), BLOCK)
    wide, scale, a = _normed(h_ref[...])
    cos, sin = _angles(fine_ref, coarse_ref, iq)
    at = a.T
    dq = (dq_s[...] * SCALE).astype(BF)
    dk = (dkt_s[:, here] * SCALE).T.astype(BF)
    da = None
    for n, t in enumerate((dq, dk, dvt_s[:, here].T.astype(BF))):
        if n < 2:
            t = _turned(t.astype(F32), cos, -sin)
        dw_s[n] += _dot(at, t)
        if not first:
            back = _dot_t(t, _square(w_ref[:, n])).astype(BF)
            da = back if n == 0 else da + back
    if not first:
        dh_ref[...] = dmid + _norm_back(wide, scale, da.astype(F32)).astype(BF)

    @pl.when(step == STEPS - 1)
    def _():
        for n in range(4):
            dw_ref[:, n] = _blocks(dw_s[n])
        if traffic:
            traffic.finish()


def attn_back(h, q, k, v, o, lse, dmid, w, layer, angles, parts=()):
    n, first = D // ROWS, layer == 0
    down = lambda width=D: pl.BlockSpec((BLOCK, width), lambda i: (STEPS - 1 - i, 0))
    ours = pl.BlockSpec((None, BLOCK, D), lambda i: (layer, STEPS - 1 - i, 0))
    every = _of(layer, T, D)
    flat, tall = (functools.partial(pltpu.VMEM, (D, size)) for size in (BLOCK, T))
    return _call(functools.partial(_attn_back, first), "attn_back", [_like(T, D)] * (not first) + [_like(n, 4, ROWS, D)],
                 ins=[down(), ours, every, every, ours, pl.BlockSpec((None, HEADS, BLOCK), lambda i: (layer, 0, STEPS - 1 - i)), down(), _units(layer, 0), *_angle_specs()],
                 outs=[down()] * (not first) + [_whole(n, 4, ROWS, D)],
                 scratch=[pltpu.VMEM((BLOCK, D), BF), flat(BF), flat(BF), pltpu.VMEM((BLOCK, HEAD), BF), pltpu.VMEM((BLOCK, D), F32), tall(F32), tall(F32), pltpu.VMEM((4, D, D), F32)],
                 flops=14 * T * T * D, parts=parts, slots=attention_slots([(i, i) for i in reversed(range(STEPS))]))(h, q, k, v, o, lse, dmid, w, *angles)


def angles_of():
    def table(places):
        angle = places[:, None] * 10000.0 ** (-np.arange(HEAD // 2) / (HEAD // 2))
        return jnp.asarray([np.concatenate([t, u], 1) for t, u in ((np.cos(angle),) * 2, (-np.sin(angle), np.sin(angle)))], F32)

    return table(np.arange(FINE)), table(np.arange(0, T, FINE))


def _angles(fine_ref, coarse_ref, i):
    some = pl.ds(pl.multiple_of(i * (BLOCK // FINE), BLOCK // FINE), BLOCK // FINE)
    (cos, sin), (cos_0, sin_0) = fine_ref[...], (coarse_ref[n, some, :][:, None] for n in range(2))
    return [t.reshape(BLOCK, HEAD) for t in (cos_0 * cos - sin_0 * sin, sin_0 * cos + cos_0 * sin)]


def place():
    me = lax.axis_index("dp")
    return me // 16, (me // 8) % 2, (me // 2) % 4, me % 2


def at(x, y, z, c):
    return {"dp": ((x * 2 + y) * 4 + z) * 2 + c}


def peers(x, y, z, c):
    return [at(x, y, (z + n) % 4, c) for n in (1, 2, 3)] + [at(1 - x, y, z, c), at(x, 1 - y, z, c), at(x, y, z, 1 - c)]


def greet(others):
    for other in others:
        pl.semaphore_signal(pltpu.get_barrier_semaphore(), inc=1, device_id=other, device_id_type=MESH)


def wait_for(others):
    pl.semaphore_wait(pltpu.get_barrier_semaphore(), len(others))


def remote(src, dst, send, recv, to):
    return pltpu.make_async_remote_copy(src_ref=src, dst_ref=dst, send_sem=send, recv_sem=recv, device_id=to, device_id_type=MESH)


def halves(span, n):
    a, b = span
    m = (a + b + n % 2) // 2
    return [(first, pl.ds(lo, hi - lo)) for first, lo, hi in ((True, a, m), (False, m, b)) if hi > lo]


def stretch(span):
    return pl.ds(span[0], span[1] - span[0])


def shard_pieces(refs, layer):
    wq, wk, wv, wo, gate, up, down = refs
    found = [(n, w.at[layer]) for n, w in enumerate((wq, wk, wv, wo))]
    for j in range(4):
        found.append((4 + j, gate.at[layer, :, pl.ds(j * D, D)]))
        found.append((8 + j, up.at[layer, :, pl.ds(j * D, D)]))
        found.append((12 + j, down.at[layer, pl.ds(j * ROWS, ROWS), :]))
    return [(unit + layer * UNITS, piece) for unit, piece in found]


class Fetch:
    def __init__(self, spans, shards, g, kept, own_sem, kept_sem, send_sem, recv_sem):
        self.spans, self.shards, self.g, self.kept = spans, shards, g, kept
        self.own_sem, self.kept_sem, self.send_sem, self.recv_sem = own_sem, kept_sem, send_sem, recv_sem
        self.place = place()

    def loads(self):
        pieces = [piece for layer in range(2) for piece in shard_pieces(self.shards, layer)]
        return [pltpu.make_async_copy(piece, self.g.at[(*self.place, unit)], self.own_sem.at[unit]) for unit, piece in pieces]

    def keep(self, n):
        u = stretch(self.spans[n])
        return pltpu.make_async_copy(self.g.at[:, :, :, :, u], self.kept.at[:, :, :, :, u], self.kept_sem.at[n])

    def copies(self, n, step, arriving=False):
        (x, y, z, c), g, span = self.place, self.g, self.spans[n]
        u, by_x, by_y = stretch(span), at(1 - x, y, z, c), at(x, 1 - y, z, c)
        xx, yy, cc = (1 - x, 1 - y, 1 - c) if arriving else (x, y, c)
        if step == 0:
            todo = [(g.at[x, y, (z + 4 - k) % 4 if arriving else z, c, u], at(x, y, (z + k) % 4, c)) for k in (1, 2, 3)]
        elif step == 1:
            todo = [(g.at[xx, y, :, c, u], by_x) if first else (g.at[x, yy, :, c, u], by_y) for first, u in halves(span, n)]
        elif step == 2:
            todo = [(g.at[:, yy, :, c, u], by_y) if first else (g.at[xx, :, :, c, u], by_x) for first, u in halves(span, n)]
        else:
            todo = [(g.at[:, :, :, cc, u], at(x, y, z, 1 - c))]
        return [remote(piece, piece, self.send_sem.at[n, step, i], self.recv_sem.at[n, step, i], to) for i, (piece, to) in enumerate(todo)]

    def start(self, n, step):
        for copy in self.copies(n, step):
            copy.start()

    def begin(self):
        for load in self.loads():
            load.start()
        greet(peers(*self.place))
        wait_for(peers(*self.place))
        for load in self.loads():
            load.wait()
    def turns(self):
        found = {}
        for step in (3, 2, 1, 0, -1):
            for n, (a, _) in enumerate(self.spans):
                turn = n + DELAY * (a >= UNITS) + (-AHEAD if step < 0 else step if n < FIRST else LAG * step)
                found.setdefault(max(turn, 0) - (turn < 0), []).append((n, step))

        def turn(now):
            for n, step in now:
                for copy in self.copies(n, step, True) if step >= 0 else ():
                    copy.wait_recv()
                if step < 3:
                    self.start(n, step + 1)
                else:
                    self.keep(n).start()

        done, named = 0, []
        for n in sorted(found):
            named.append((functools.partial(turn, found[n]), done))
            done = max([done] + [self.spans[m][1] for m, step in found[n] if step == 3])
        return named

    def finish(self):
        for n in range(len(self.spans)):
            self.keep(n).wait()
            for step in range(4):
                for copy in self.copies(n, step):
                    copy.wait_send()


BEFORE, DIAGONAL, AFTER = "before", "diagonal", "after"


def run_at(slots, turns, i, j):
    for n, turn in enumerate(turns):
        a, b = slots[n * len(slots) // len(turns)]
        if isinstance(b, str) or isinstance(j, str):
            if b == j:
                pl.when(i == a)(turn)
        else:
            pl.when(i * UNITS + j == a * UNITS + b)(turn)


def attention_slots(steps):
    return [(s, j) for s, n in steps for j in (*range(n), DIAGONAL, AFTER)]


def _add_into(total, more):
    lead = total.shape[:-4]

    def one(i, _):
        where = []
        for n in reversed(lead):
            where = [i % n] + where
            i = i // n
        where = tuple(where)
        total[where] = (total[where].astype(F32) + more[where].astype(F32)).astype(BF)

    lax.fori_loop(0, int(np.prod(lead, dtype=int)), one, None)


def sum_spans(parts, most):
    spans, units = [], 0
    for which, d in enumerate(parts):
        n = d.shape[1]
        spans += [(which, a, units + a, units + min(a + most, n)) for a in range(0, n, most)]
        units += n
    return spans, units


def sum_buffers(units, n):
    return [pltpu.VMEM((*lead, units, ROWS, D), BF) for lead in ((2, 2, 4), (2, 2, 4), (2, 4), (4,), (3,))] + [
        pltpu.SemaphoreType.DMA(shape) for shape in ((n,), (n, 4, 3), (n, 4, 3))]


class Sums:
    def __init__(self, lag, slots, spans, ds, g, *buffers):
        self.lag, self.slots, self.spans, self.ds, self.g = lag, slots, spans, ds, g
        self.s, self.r1, self.r2, self.r3, self.r4, self.local_sem, self.send_sem, self.recv_sem = buffers
        self.place = place()

    def own(self, n, core):
        which, first, a, b = self.spans[n]
        return self.ds[which].at[:, :, :, core, pl.ds(first, b - a)]

    def load(self, n):
        return pltpu.make_async_copy(self.own(n, self.place[3]), self.s.at[:, :, :, stretch(self.spans[n][2:])], self.local_sem.at[n])

    def copies(self, n, step):
        (x, y, z, c), s, span = self.place, self.s, self.spans[n][2:]
        u, by_x, by_y = stretch(span), at(1 - x, y, z, c), at(x, 1 - y, z, c)
        if step == 0:
            todo = [(self.own(n, 1 - c), self.r1.at[:, :, :, u], at(x, y, z, 1 - c))]
        elif step == 1:
            todo = [(s.at[1 - x, :, :, u] if first else s.at[:, 1 - y, :, u], self.r2.at[:, :, u], by_x if first else by_y) for first, u in halves(span, n)]
        elif step == 2:
            todo = [(s.at[x, 1 - y, :, u] if first else s.at[1 - x, y, :, u], self.r3.at[:, u], by_y if first else by_x) for first, u in halves(span, n)]
        else:
            todo = [(s.at[x, y, (z + k) % 4, u], self.r4.at[k - 1, u], at(x, y, (z + k) % 4, c)) for k in (1, 2, 3)]
        return [remote(a, b, self.send_sem.at[n, step, i], self.recv_sem.at[n, step, i], to) for i, (a, b, to) in enumerate(todo)]

    def add(self, n, step):
        (x, y, z, c), s, span = self.place, self.s, self.spans[n][2:]
        u = stretch(span)
        if step == 0:
            _add_into(s.at[:, :, :, u], self.r1.at[:, :, :, u])
        elif step == 1:
            for first, u in halves(span, n):
                _add_into(s.at[x, :, :, u] if first else s.at[:, y, :, u], self.r2.at[:, :, u])
        elif step == 2:
            _add_into(s.at[x, y, :, u], self.r3.at[:, u])
        else:
            out = s[x, y, z, u].astype(F32)
            for k in range(3):
                out = out + self.r4[k, u].astype(F32)
            self.g[u] = out.astype(BF)

    def begin(self):
        for n in range(len(self.spans)):
            self.load(n).start()
        greet(peers(*self.place))

    def send(self):
        wait_for(peers(*self.place))
        for n in range(len(self.spans)):
            self.start(n, 0)

    def start(self, n, step):
        for copy in self.copies(n, step):
            copy.start()

    def turns(self):
        found = [self.begin, self.send]
        for tick in range(len(self.spans) + 3 * self.lag):
            now = [(tick - self.lag * step, step) for step in range(4) if 0 <= tick - self.lag * step < len(self.spans)]

            def turn(now=now):
                for n, step in now:
                    if step == 0:
                        self.load(n).wait()
                    for copy in self.copies(n, step):
                        copy.wait_recv()
                    self.add(n, step)
                    if step < 3:
                        self.start(n, step + 1)

            found.append(turn)
        return found

    def tick(self, i, j):
        run_at(self.slots, self.turns(), i, j)

    def finish(self):
        for n in range(len(self.spans)):
            for step in range(4):
                for copy in self.copies(n, step):
                    copy.wait_send()


def _last_sums(spans, d, *refs):
    *done, g, squares, sq, sq_all, sq_send, sq_recv = refs[: -len(sum_buffers(1, 1))]
    traffic = Sums(1, (), spans, [d], g, *refs[-len(sum_buffers(1, 1)) :])
    me = lax.axis_index("dp")
    everyone = [{"dp": (me + k) % 32} for k in range(1, 32)]
    greet(everyone)
    for n in range(len(spans)):
        traffic.load(n).start()
    wait_for(everyone)
    for n in range(len(spans)):
        traffic.start(n, 0)
    sq[...] = jnp.zeros_like(sq)

    def squared(ref):
        def one(i, total):
            wide = ref[i].astype(F32)
            return total + (wide * wide).reshape(ROWS // 8, 8, D // HEAD, HEAD).sum((0, 2))

        sq[...] += lax.fori_loop(0, ref.shape[0], one, jnp.zeros((8, HEAD), F32))

    for ref in done:
        squared(ref)
    for turn in traffic.turns()[2:]:
        turn()
    squared(g)
    spread = [remote(sq, sq_all.at[k + 1], sq_send.at[k], sq_recv.at[k], to) for k, to in enumerate(everyone)]
    for copy in spread:
        copy.start()
    for copy in spread:
        copy.wait_recv()
    sq_all[0] = sq[...]
    squares[...] = jnp.full((8, HEAD), jnp.sum(sq_all[...]))
    for copy in spread:
        copy.wait_send()
    traffic.finish()


def last_sums(d, done):
    spans, units = sum_spans([d], LAST)
    return pl.pallas_call(
        functools.partial(_last_sums, spans),
        out_shape=[_like(units, ROWS, D), _like(8, HEAD, dtype=F32)],
        in_specs=[ANY] + [IN_VMEM] * len(done),
        out_specs=[IN_VMEM, IN_VMEM],
        scratch_shapes=[pltpu.VMEM((8, HEAD), F32), pltpu.VMEM((32, 8, HEAD), F32), pltpu.SemaphoreType.DMA((31,)), pltpu.SemaphoreType.DMA((31,)),
                        *sum_buffers(units, len(spans))],
        compiler_params=pltpu.CompilerParams(collective_id=1, has_side_effects=True, vmem_limit_bytes=VMEM),
        name="last_sums",
    )(d.reshape(2, 2, 4, 2, *d.shape[1:]), *done)


def _adamw(squares, *refs):
    g, (w, m, v, new_w, new_m, new_v) = refs[:4], (refs[i : i + 7] for i in range(4, 46, 7))
    count = 2 * UNITS * ROWS * D * 32
    factor = jnp.minimum(1.0, 0.5 * lax.rsqrt(squares[0:1, 0:1] / count + 1e-30))
    for layer in range(2):
        for i in range(7):
            for unit, piece in _pieces(i):
                where = (layer, *piece)
                sums, unit = (g[2 * layer], unit) if i < 4 else (g[2 * layer + 1], unit - 4)
                one = sums[unit].astype(F32) * factor
                mm = 0.9 * m[i][where] + 0.1 * one
                vv = 0.95 * v[i][where] + 0.05 * one * one
                old = w[i][where].astype(F32)
                new_w[i][where] = (old - 0.02 * (mm * lax.rsqrt(vv + 1e-8) + 0.1 * old)).astype(BF)
                new_m[i][where] = mm
                new_v[i][where] = vv


def _pieces(i):
    every = slice(None)
    if i < 4:
        return [(i, (every, every))]
    if i < 6:
        return [(4 * (i - 3) + j, (every, pl.ds(j * D, D))) for j in range(4)]
    return [(12 + j, (pl.ds(j * ROWS, ROWS), every)) for j in range(4)]


def adamw_all(weights, m, v, sums, squares):
    return pl.pallas_call(
        _adamw,
        out_shape=[_like(*w.shape) for w in weights] + [_like(*w.shape, dtype=F32) for w in weights] * 2,
        in_specs=[IN_VMEM] * 26,
        out_specs=[IN_VMEM] * 21,
        compiler_params=pltpu.CompilerParams(vmem_limit_bytes=VMEM),
        name="adamw_all",
    )(squares, *sums, *weights, *m, *v)


def _forward(spans, x_ref, fine_ref, coarse_ref, *refs):
    shards, (kept, q_ref, k_ref, v_ref, o_ref, lse_ref, mid_ref, h1_ref), refs = refs[:7], refs[7:15], refs[15:]
    g, h_s, k_s, vt_s, top_s, mix_s, *sems = refs
    fetch = Fetch(spans, shards, g, kept, *sems)
    s = pl.program_id(0)
    layer, i = s // (2 * STEPS), s % STEPS
    here = pl.ds(pl.multiple_of(i * BLOCK, BLOCK), BLOCK)
    unit = layer * UNITS
    phase = s // STEPS
    turns = fetch.turns()
    ready = [turn for turn, unit in turns if unit < 4]
    early = [turn for turn, unit in turns if 4 <= unit < UNITS]
    middle = [turn for turn, unit in turns if UNITS <= unit < UNITS + 4]
    late = [turn for turn, unit in turns if unit >= UNITS + 4]

    def tick(j):
        run_at(attention_slots([(n, n) for n in range(STEPS)]), early, s, j)
        run_at([(n, f"part {j}") for n in range(STEPS, 2 * STEPS) for j in range(STEPS)], middle, s, j)
        run_at(attention_slots([(n + 2 * STEPS, n) for n in range(STEPS)]), late, s, j)

    def weight(n):
        return g[:, :, :, :, unit + n].reshape(D, D)

    @pl.when(s == 0)
    def _():
        fetch.begin()
        for turn in ready:
            turn()

    @pl.when(phase == 0)
    def _():
        h_s[here, :] = x_ref[here, :]

    @pl.when(phase != 1)
    def _():
        a = _normed(h_s[here, :])[2]
        cos, sin = _angles(fine_ref, coarse_ref, i)
        for n, out in enumerate((q_ref, k_ref, v_ref)):
            t = _dot(a, weight(n)).astype(BF)
            t = t if n == 2 else _turned(t.astype(F32), cos, sin)
            out[...] = t
            if n == 1:
                k_s[here, :] = t
            if n == 2:
                vt_s[:, here] = t.T
        top_s[...] = jnp.full_like(top_s, NEG)
        mix_s[...] = jnp.zeros_like(mix_s)
        ones = jnp.ones((8, BLOCK), BF)
        e = SCALE * LOG2E

        def block(j, masked):
            tick(DIAGONAL if masked else j)
            keys = pl.ds(pl.multiple_of(j * BLOCK, BLOCK), BLOCK)
            scores = [_dot_t(k_s[keys, _head(n)], q_ref[:, _head(n)]) for n in range(HEADS)]
            if masked:
                ok = lax.broadcasted_iota(jnp.int32, (BLOCK, BLOCK), 1) >= lax.broadcasted_iota(jnp.int32, (BLOCK, BLOCK), 0)
            weights, keeps = [], []
            for n, x in enumerate(scores):
                if masked:
                    x = jnp.where(ok, x, HIDDEN)
                old = top_s[n : n + 1, :]
                top = jnp.maximum(old, x.max(axis=0, keepdims=True))
                top_s[n : n + 1, :] = top
                weights.append(jnp.exp2((x - top) * e).astype(BF))
                keeps.append(jnp.exp2((old - top) * e))
            for n in range(HEADS):
                values = jnp.concatenate([vt_s[_head(n), keys], ones], axis=0)
                mix_s[n] = mix_s[n] * keeps[n] + _dot(values, weights[n])

        lax.fori_loop(0, i, lambda j, _: block(j, False), None)
        block(i, True)
        tick(AFTER)
        for n in range(HEADS):
            total = mix_s[n, HEAD : HEAD + 1, :]
            o_ref[:, _head(n)] = (mix_s[n, :HEAD, :] * (1 / total)).T.astype(BF)
            lse_ref[n : n + 1, :] = top_s[n : n + 1, :] * SCALE + jnp.log(total)
        mid = h_s[here, :] + _dot(o_ref[...], weight(3)).astype(BF)
        mid_ref[...] = mid
        h_s[here, :] = mid

    @pl.when(phase == 1)
    def _():
        mid = h_s[here, :]
        b = _normed(mid)[2]
        total = None
        for j in range(FF // BLOCK):
            tick(f"part {j}")
            gate, up = _dot(b, weight(4 + j)), _dot(b, weight(8 + j))
            hid = (gate * (0.5 * jnp.tanh(0.5 * gate) + 0.5) * up).astype(BF)
            more = _dot(hid, g[j // 2, j % 2, :, :, 12:UNITS].reshape(D, D))
            total = more if j == 0 else total + more
        out = mid + total.astype(BF)
        h1_ref[...] = out
        h_s[here, :] = out

    @pl.when(s == pl.num_programs(0) - 1)
    def _():
        fetch.finish()


def forward(x, weights, angles):
    spans = [(n * 4 // FIRST, (n + 1) * 4 // FIRST) for n in range(FIRST)] + [(n, n + SPAN) for n in range(4, 2 * UNITS, SPAN)]
    n = len(spans)

    def place_of(s):
        t = s % (2 * STEPS)
        return s // (2 * STEPS), t - t // STEPS * (t - STEPS + 1)

    both = pl.BlockSpec((None, BLOCK, D), lambda s: (*place_of(s), 0))
    stats = pl.BlockSpec((None, HEADS, BLOCK), lambda s: (place_of(s)[0], 0, place_of(s)[1]))
    ffn_rows = pl.BlockSpec((BLOCK, D), lambda s: (s // STEPS % 2 * (s - STEPS) + s // STEPS // 2 * (STEPS - 1), 0))
    gathered = (2, 2, 4, 2, 2 * UNITS, ROWS, D)
    w, *rest = pl.pallas_call(
        functools.partial(_forward, spans),
        name="forward",
        grid=(3 * STEPS,),
        in_specs=[_whole(T, D), *_angle_specs()] + [ANY] * 7,
        out_specs=[ANY] + [both] * 4 + [stats, both, ffn_rows],
        out_shape=[_like(*gathered)] + [_like(2, T, D)] * 4 + [_like(2, HEADS, T, dtype=F32), _like(2, T, D), _like(T, D)],
        scratch_shapes=[pltpu.VMEM(gathered, BF), pltpu.VMEM((T, D), BF), pltpu.VMEM((T, D), BF), pltpu.VMEM((D, T), BF), pltpu.VMEM((HEADS, BLOCK), F32),
                        pltpu.VMEM((HEADS, HEAD + 8, BLOCK), F32)] + [pltpu.SemaphoreType.DMA(shape) for shape in ((2 * UNITS,), (n,), (n, 4, 3), (n, 4, 3))],
        compiler_params=pltpu.CompilerParams(dimension_semantics=("arbitrary",), vmem_limit_bytes=VMEM, collective_id=0, has_side_effects=True),
        cost_estimate=pl.CostEstimate(flops=50 * T * D * D, transcendentals=0, bytes_accessed=0),
    )(x, *angles, *weights)
    return w.reshape(D // ROWS, 2 * UNITS, ROWS, D), *rest


def solution(mesh):
    def step(x, dy, *arrays):
        weights, m, v = (arrays[i : i + 7] for i in (0, 7, 14))
        angles = angles_of()
        w, q, k, vv, o, lse, mid, h1 = forward(x[0], weights, angles)
        saved = (q, k, vv, o, lse)
        dmid, *ffn_1 = ffn_back(dy[0], mid, w, 1)
        dh, attn_1, ffn_1 = attn_back(h1, *saved, dmid, w, 1, angles, (2, *ffn_1))
        dmid, *ffn_0, attn_1 = ffn_back(dh, mid, w, 0, (3, attn_1))
        attn_0, ffn_0 = attn_back(x[0], *saved, dmid, w, 0, angles, (4, *ffn_0))
        attn_0, squares = last_sums(attn_0, (ffn_0, attn_1, ffn_1))
        return tuple(adamw_all(weights, m, v, (attn_0, ffn_0, attn_1, ffn_1), squares))

    states, cut = P(("rep", "dp"), None, None), P(None, "dp", None)
    return jax.shard_map(
        step,
        mesh=mesh,
        in_specs=(states, states) + (cut,) * 21,
        out_specs=(P("rep", "dp", None),) * 21,
        check_vma=False,
    )
```

```python
import functools

import jax
import jax.numpy as jnp
import numpy as np
from jax import lax
from jax.experimental import pallas as pl
from jax.experimental.pallas import tpu as pltpu
from jax.sharding import PartitionSpec as P

BF, F32 = jnp.bfloat16, jnp.float32
MESH = pl.DeviceIdType.MESH
ANY = pl.BlockSpec(memory_space=pl.ANY)
IN_VMEM = pl.BlockSpec(memory_space=pltpu.VMEM)
VMEM = 58 * 2**20
T, D, HEADS, HEAD, FF = 2048, 512, 4, 128, 2048
BLOCK = 512
STEPS = T // BLOCK
LAG, MOST, LAST, SPAN, FIRST, DELAY, AHEAD = 2, 2, 2, 2, 1, 2, 4
FINE = 64
PARTS = 3
UNITS, ROWS = 16, 16
NEG = -1e30
HIDDEN = 2 * NEG
LOG2E = 1.4426950408889634
SCALE = HEAD**-0.5


def _dot(a, b, ca=1, cb=0):
    return lax.dot_general(a, b, (((ca,), (cb,)), ((), ())), preferred_element_type=F32)


def _dot_t(a, b):
    return _dot(a, b, 1, 1)


def _square(w):
    return w.reshape(D, D)


def _blocks(w):
    return w.astype(BF).reshape(D // ROWS, ROWS, D)


def _normed(h):
    wide = h.astype(F32)
    scale = lax.rsqrt(jnp.mean(wide * wide, -1, keepdims=True) + 1e-6)
    return wide, scale, (wide * scale).astype(BF)


def _norm_back(wide, scale, ct):
    return scale * (ct - wide * (scale * scale * jnp.mean(ct * wide, -1, keepdims=True)))


def _turned(t, cos, sin):
    parts = [t[:, n : n + HEAD] for n in range(0, D, HEAD)]
    return jnp.concatenate([p * cos + pltpu.roll(p, HEAD // 2, 1) * sin for p in parts], 1).astype(BF)


def _head(n):
    return pl.ds(n * HEAD, HEAD)


def _call(body, name, out, scratch=(), ins=(), outs=(), flops=0, parts=(), slots=(), lag=LAG, flags=None):
    out, outs, ins, scratch, more, own = list(out), list(outs), list(ins), list(scratch), {}, body
    if parts:
        number, *parts = parts
        spans, units = sum_spans(parts, MOST)
        buffers = sum_buffers(units, len(spans))
        n_in, n_out = len(ins), len(out)
        ins += [ANY] * len(parts)
        out += [_like(units, ROWS, D)]
        outs += [_whole(units, ROWS, D)]
        parts = [d.reshape(2, 2, 4, 2, *d.shape[1:]) for d in parts]
        more = dict(collective_id=number, has_side_effects=True)

        def own(*refs):
            refs = list(refs)
            given, refs = refs[:n_in], refs[n_in:]
            ds, refs = refs[: len(parts)], refs[len(parts) :]
            made, total, kept = refs[:n_out], refs[n_out], refs[n_out + 1 :]
            traffic = Sums(lag, slots, spans, ds, total, *kept[len(scratch) :])
            body(*given, *made, *kept[: len(scratch)], traffic)

    run = pl.pallas_call(
        own, name=name, grid=(STEPS,), in_specs=ins, out_specs=outs, out_shape=out, scratch_shapes=scratch + (buffers if parts else []),
        compiler_params=pltpu.CompilerParams(dimension_semantics=("arbitrary",), vmem_limit_bytes=VMEM, flags=flags, **more),
        cost_estimate=pl.CostEstimate(flops=flops, transcendentals=0, bytes_accessed=0),
    )
    return lambda *given: run(*given, *parts)


def _rows(width=D):
    return pl.BlockSpec((BLOCK, width), lambda i: (i, 0))


def _whole(*shape):
    return pl.BlockSpec(shape, lambda i: (0,) * len(shape), pipeline_mode=pl.Buffered(1))


def _of(layer, *shape):
    return pl.BlockSpec((None, *shape), lambda i: (layer, *(0,) * len(shape)), pipeline_mode=pl.Buffered(1))


def _angle_specs():
    return [_whole(2, n, HEAD) for n in (FINE, T // FINE)]


def _units(layer, kind):
    return pl.BlockSpec((D // ROWS, 4, ROWS, D), lambda i: (0, layer * 4 + kind, 0, 0), pipeline_mode=pl.Buffered(1))


def _like(*shape, dtype=BF):
    return jax.ShapeDtypeStruct(shape, dtype)


def _ffn_back(dh_ref, mid_ref, gate_ref, up_ref, down_ref, dmid_ref, dgate_ref, dup_ref, ddown_ref, b_s, bt_s, dht_s, db_s, dg_s, du_s, hid_s, traffic=None):
    j = pl.program_id(0)

    @pl.when(j == 0)
    def _():
        for i in range(STEPS):
            here = pl.ds(i * BLOCK, BLOCK)
            b = _normed(mid_ref[here, :])[2]
            b_s[here, :] = b
            bt_s[:, here] = b.T
            dht_s[:, here] = dh_ref[here, :].T
            db_s[here, :] = jnp.zeros((BLOCK, D), F32)

    gate_w, up_w, down_w = _square(gate_ref[:, 0]), _square(up_ref[:, 0]), _square(down_ref[...])

    def rows(i, _):
        here = pl.ds(pl.multiple_of(i * BLOCK, BLOCK), BLOCK)
        b = b_s[here, :]
        gate, up = _dot(b, gate_w), _dot(b, up_w)
        dhid = _dot_t(dh_ref[here, :], down_w).astype(BF).astype(F32)
        half = 0.5 * jnp.tanh(0.5 * gate) + 0.5
        silu = gate * half
        hid_s[here, :] = (silu * up).astype(BF)
        du = (dhid * silu).astype(BF)
        dg = (dhid * up * (half + silu * (1.0 - half))).astype(BF)
        dg_s[here, :] = dg
        du_s[here, :] = du
        db_s[here, :] += _dot_t(dg, gate_w) + _dot_t(du, up_w)

    if traffic:
        traffic.tick(j, BEFORE)
    lax.fori_loop(0, STEPS, rows, None, unroll=True)
    if traffic:
        traffic.tick(j, AFTER)
    dgate_ref[:, 0] = _blocks(_dot(bt_s[...], dg_s[...]))
    dup_ref[:, 0] = _blocks(_dot(bt_s[...], du_s[...]))
    ddown_ref[...] = _dot(dht_s[...], hid_s[...]).astype(BF).T.reshape(8, 4, ROWS, D)

    @pl.when(j == pl.num_programs(0) - 1)
    def _():
        for i in range(STEPS):
            here = pl.ds(i * BLOCK, BLOCK)
            wide, scale, _ = _normed(mid_ref[here, :])
            dmid_ref[here, :] = dh_ref[here, :] + _norm_back(wide, scale, db_s[here, :].astype(BF).astype(F32)).astype(BF)
        if traffic:
            traffic.finish()


def ffn_back(dh, mid, w, layer, parts=()):
    n = D // ROWS
    one = lambda kind: pl.BlockSpec((n, 1, ROWS, D), lambda j: (0, layer * UNITS + 4 * kind + j, 0, 0))
    some = pl.BlockSpec((n // 4, 4, ROWS, D), lambda j: (j, layer * 4 + 3, 0, 0))
    big = lambda dtype=BF: pltpu.VMEM((T, D), dtype)
    return _call(_ffn_back, "ffn_back", [_like(T, D)] + [_like(n, 4, ROWS, D)] * 3,
                 ins=[_whole(T, D), _of(layer, T, D), one(1), one(2), some],
                 outs=[_whole(T, D)] + [pl.BlockSpec((n, 1, ROWS, D), lambda j: (0, j, 0, 0))] * 2 + [pl.BlockSpec((n // 4, 4, ROWS, D), lambda j: (j, 0, 0, 0))],
                 scratch=[big(), pltpu.VMEM((D, T), BF), pltpu.VMEM((D, T), BF), big(F32), big(), big(), big()],
                 flops=64 * T * D * D, parts=parts, lag=1, slots=[(0, BEFORE)] + [(j, place) for j in range(1, STEPS) for place in (BEFORE, AFTER)])(dh, mid, w, w, w)


def _attn_back(first, h_ref, q_ref, k_ref, v_ref, o_ref, lse_ref, dmid_ref, w_ref, fine_ref, coarse_ref, *refs):
    step = pl.program_id(0)
    iq = STEPS - 1 - step
    dh_ref, refs = (None, refs) if first else (refs[0], refs[1:])
    dw_ref, do_s, dot_s, qt_s, cols_s, dq_s, dkt_s, dvt_s, dw_s, *traffic = refs
    traffic = traffic[0] if traffic else None
    e = SCALE * LOG2E

    @pl.when(step == 0)
    def _():
        dw_s[...] = jnp.zeros_like(dw_s)

    dmid, o = dmid_ref[...], o_ref[...]
    do = _dot_t(dmid, _square(w_ref[:, 3])).astype(BF)
    do_s[...], dot_s[...], qt_s[...] = do, do.T, q_ref[...].T
    pick = (lax.broadcasted_iota(jnp.int32, (8, D), 1) // HEAD == lax.broadcasted_iota(jnp.int32, (8, D), 0)).astype(F32)
    both = do.astype(F32) * o.astype(F32)
    delta = lax.dot_general(pick, both, (((1,), (1,)), ((), ())), precision=lax.Precision.HIGHEST, preferred_element_type=F32)
    parts = []
    for n in range(HEADS):
        for left in (lse_ref[n : n + 1, :] * (-1 / SCALE), -delta[n : n + 1, :]):
            for _ in range(PARTS):
                parts.append(left.astype(BF).astype(F32))
                left = left - parts[-1]
    parts.append(jnp.zeros((HEAD - len(parts), BLOCK), F32))
    cols_s[...] = jnp.concatenate(parts, 0).T.astype(BF)
    dw_s[3] += _dot(o.T, dmid)
    dq_s[...] = jnp.zeros_like(dq_s)

    def block(j, masked):
        if traffic:
            traffic.tick(iq, DIAGONAL if masked else j)
        here = pl.ds(pl.multiple_of(j * BLOCK, BLOCK), BLOCK)
        lane = lax.broadcasted_iota(jnp.int32, (BLOCK, HEAD), 1) // PARTS

        def beside(a, b, n):
            return _dot_t(jnp.concatenate([a, cols_s[...]], 1), jnp.concatenate([b, (lane == n).astype(F32).astype(BF)], 1))

        scores = [beside(q_ref[:, _head(n)], k_ref[here, _head(n)], 2 * n) for n in range(HEADS)]
        dps = [beside(do_s[:, _head(n)], v_ref[here, _head(n)], 2 * n + 1) for n in range(HEADS)]
        if masked:
            ok = lax.broadcasted_iota(jnp.int32, (BLOCK, BLOCK), 0) >= lax.broadcasted_iota(jnp.int32, (BLOCK, BLOCK), 1)
        for n in range(HEADS):
            p = jnp.exp2(scores[n] * e)
            if masked:
                p = jnp.where(ok, p, 0.0)
            ds = (p * dps[n]).astype(BF)
            for total, more in ((dvt_s, _dot(dot_s[_head(n), :], p.astype(BF))), (dkt_s, _dot(qt_s[_head(n), :], ds))):
                total[_head(n), here] = jnp.where(step > 0, total[_head(n), here], 0.0) + more
            dq_s[:, _head(n)] += _dot(ds, k_ref[here, _head(n)])

    lax.fori_loop(0, iq, lambda j, _: block(j, False), None)
    block(iq, True)
    if traffic:
        traffic.tick(iq, AFTER)
    here = pl.ds(pl.multiple_of(iq * BLOCK, BLOCK), BLOCK)
    wide, scale, a = _normed(h_ref[...])
    cos, sin = _angles(fine_ref, coarse_ref, iq)
    at = a.T
    dq = (dq_s[...] * SCALE).astype(BF)
    dk = (dkt_s[:, here] * SCALE).T.astype(BF)
    da = None
    for n, t in enumerate((dq, dk, dvt_s[:, here].T.astype(BF))):
        if n < 2:
            t = _turned(t.astype(F32), cos, -sin)
        dw_s[n] += _dot(at, t)
        if not first:
            back = _dot_t(t, _square(w_ref[:, n])).astype(BF)
            da = back if n == 0 else da + back
    if not first:
        dh_ref[...] = dmid + _norm_back(wide, scale, da.astype(F32)).astype(BF)

    @pl.when(step == STEPS - 1)
    def _():
        for n in range(4):
            dw_ref[:, n] = _blocks(dw_s[n])
        if traffic:
            traffic.finish()


def attn_back(h, q, k, v, o, lse, dmid, w, layer, angles, parts=()):
    n, first = D // ROWS, layer == 0
    down = lambda width=D: pl.BlockSpec((BLOCK, width), lambda i: (STEPS - 1 - i, 0))
    ours = pl.BlockSpec((None, BLOCK, D), lambda i: (layer, STEPS - 1 - i, 0))
    every = _of(layer, T, D)
    flat, tall = (functools.partial(pltpu.VMEM, (D, size)) for size in (BLOCK, T))
    return _call(functools.partial(_attn_back, first), "attn_back", [_like(T, D)] * (not first) + [_like(n, 4, ROWS, D)],
                 ins=[down(), ours, every, every, ours, pl.BlockSpec((None, HEADS, BLOCK), lambda i: (layer, 0, STEPS - 1 - i)), down(), _units(layer, 0), *_angle_specs()],
                 outs=[down()] * (not first) + [_whole(n, 4, ROWS, D)],
                 scratch=[pltpu.VMEM((BLOCK, D), BF), flat(BF), flat(BF), pltpu.VMEM((BLOCK, HEAD), BF), pltpu.VMEM((BLOCK, D), F32), tall(F32), tall(F32), pltpu.VMEM((4, D, D), F32)],
                 flops=14 * T * T * D, parts=parts, slots=attention_slots([(i, i) for i in reversed(range(STEPS))]))(h, q, k, v, o, lse, dmid, w, *angles)


def angles_of():
    def table(places):
        angle = places[:, None] * 10000.0 ** (-np.arange(HEAD // 2) / (HEAD // 2))
        return jnp.asarray([np.concatenate([t, u], 1) for t, u in ((np.cos(angle),) * 2, (-np.sin(angle), np.sin(angle)))], F32)

    return table(np.arange(FINE)), table(np.arange(0, T, FINE))


def _angles(fine_ref, coarse_ref, i):
    some = pl.ds(pl.multiple_of(i * (BLOCK // FINE), BLOCK // FINE), BLOCK // FINE)
    (cos, sin), (cos_0, sin_0) = fine_ref[...], (coarse_ref[n, some, :][:, None] for n in range(2))
    return [t.reshape(BLOCK, HEAD) for t in (cos_0 * cos - sin_0 * sin, sin_0 * cos + cos_0 * sin)]


def place():
    me = lax.axis_index("dp")
    return me // 16, (me // 8) % 2, (me // 2) % 4, me % 2


def at(x, y, z, c):
    return {"dp": ((x * 2 + y) * 4 + z) * 2 + c}


def peers(x, y, z, c):
    return [at(x, y, (z + n) % 4, c) for n in (1, 2, 3)] + [at(1 - x, y, z, c), at(x, 1 - y, z, c), at(x, y, z, 1 - c)]


def greet(others):
    for other in others:
        pl.semaphore_signal(pltpu.get_barrier_semaphore(), inc=1, device_id=other, device_id_type=MESH)


def wait_for(others):
    pl.semaphore_wait(pltpu.get_barrier_semaphore(), len(others))


def remote(src, dst, send, recv, to):
    return pltpu.make_async_remote_copy(src_ref=src, dst_ref=dst, send_sem=send, recv_sem=recv, device_id=to, device_id_type=MESH)


def halves(span, n):
    a, b = span
    m = (a + b + n % 2) // 2
    return [(first, pl.ds(lo, hi - lo)) for first, lo, hi in ((True, a, m), (False, m, b)) if hi > lo]


def stretch(span):
    return pl.ds(span[0], span[1] - span[0])


def shard_pieces(refs, layer):
    wq, wk, wv, wo, gate, up, down = refs
    found = [(n, w.at[layer]) for n, w in enumerate((wq, wk, wv, wo))]
    for j in range(4):
        found.append((4 + j, gate.at[layer, :, pl.ds(j * D, D)]))
        found.append((8 + j, up.at[layer, :, pl.ds(j * D, D)]))
        found.append((12 + j, down.at[layer, pl.ds(j * ROWS, ROWS), :]))
    return [(unit + layer * UNITS, piece) for unit, piece in found]


class Fetch:
    def __init__(self, spans, shards, g, kept, own_sem, kept_sem, send_sem, recv_sem):
        self.spans, self.shards, self.g, self.kept = spans, shards, g, kept
        self.own_sem, self.kept_sem, self.send_sem, self.recv_sem = own_sem, kept_sem, send_sem, recv_sem
        self.place = place()

    def loads(self):
        pieces = [piece for layer in range(2) for piece in shard_pieces(self.shards, layer)]
        return [pltpu.make_async_copy(piece, self.g.at[(*self.place, unit)], self.own_sem.at[unit]) for unit, piece in pieces]

    def keep(self, n):
        u = stretch(self.spans[n])
        return pltpu.make_async_copy(self.g.at[:, :, :, :, u], self.kept.at[:, :, :, :, u], self.kept_sem.at[n])

    def copies(self, n, step, arriving=False):
        (x, y, z, c), g, span = self.place, self.g, self.spans[n]
        u, by_x, by_y = stretch(span), at(1 - x, y, z, c), at(x, 1 - y, z, c)
        xx, yy, cc = (1 - x, 1 - y, 1 - c) if arriving else (x, y, c)
        if step == 0:
            todo = [(g.at[x, y, (z + 4 - k) % 4 if arriving else z, c, u], at(x, y, (z + k) % 4, c)) for k in (1, 2, 3)]
        elif step == 1:
            todo = [(g.at[xx, y, :, c, u], by_x) if first else (g.at[x, yy, :, c, u], by_y) for first, u in halves(span, n)]
        elif step == 2:
            todo = [(g.at[:, yy, :, c, u], by_y) if first else (g.at[xx, :, :, c, u], by_x) for first, u in halves(span, n)]
        else:
            todo = [(g.at[:, :, :, cc, u], at(x, y, z, 1 - c))]
        return [remote(piece, piece, self.send_sem.at[n, step, i], self.recv_sem.at[n, step, i], to) for i, (piece, to) in enumerate(todo)]

    def start(self, n, step):
        for copy in self.copies(n, step):
            copy.start()

    def begin(self):
        for load in self.loads():
            load.start()
        greet(peers(*self.place))
        wait_for(peers(*self.place))
        for load in self.loads():
            load.wait()
    def turns(self):
        found = {}
        for step in (3, 2, 1, 0, -1):
            for n, (a, _) in enumerate(self.spans):
                turn = n + DELAY * (a >= UNITS) + (-AHEAD if step < 0 else step if n < FIRST else LAG * step)
                found.setdefault(max(turn, 0) - (turn < 0), []).append((n, step))

        def turn(now):
            for n, step in now:
                for copy in self.copies(n, step, True) if step >= 0 else ():
                    copy.wait_recv()
                if step < 3:
                    self.start(n, step + 1)
                else:
                    self.keep(n).start()

        done, named = 0, []
        for n in sorted(found):
            named.append((functools.partial(turn, found[n]), done))
            done = max([done] + [self.spans[m][1] for m, step in found[n] if step == 3])
        return named

    def finish(self):
        for n in range(len(self.spans)):
            self.keep(n).wait()
            for step in range(4):
                for copy in self.copies(n, step):
                    copy.wait_send()


BEFORE, DIAGONAL, AFTER = "before", "diagonal", "after"


def run_at(slots, turns, i, j):
    for n, turn in enumerate(turns):
        a, b = slots[n * len(slots) // len(turns)]
        if isinstance(b, str) or isinstance(j, str):
            if b == j:
                pl.when(i == a)(turn)
        else:
            pl.when(i * UNITS + j == a * UNITS + b)(turn)


def attention_slots(steps):
    return [(s, j) for s, n in steps for j in (*range(n), DIAGONAL, AFTER)]


def _add_into(total, more):
    lead = total.shape[:-4]

    def one(i, _):
        where = []
        for n in reversed(lead):
            where = [i % n] + where
            i = i // n
        where = tuple(where)
        total[where] = (total[where].astype(F32) + more[where].astype(F32)).astype(BF)

    lax.fori_loop(0, int(np.prod(lead, dtype=int)), one, None)


def sum_spans(parts, most):
    spans, units = [], 0
    for which, d in enumerate(parts):
        n = d.shape[1]
        spans += [(which, a, units + a, units + min(a + most, n)) for a in range(0, n, most)]
        units += n
    return spans, units


def sum_buffers(units, n):
    return [pltpu.VMEM((*lead, units, ROWS, D), BF) for lead in ((2, 2, 4), (2, 2, 4), (2, 4), (4,), (3,))] + [
        pltpu.SemaphoreType.DMA(shape) for shape in ((n,), (n, 4, 3), (n, 4, 3))]


class Sums:
    def __init__(self, lag, slots, spans, ds, g, *buffers):
        self.lag, self.slots, self.spans, self.ds, self.g = lag, slots, spans, ds, g
        self.s, self.r1, self.r2, self.r3, self.r4, self.local_sem, self.send_sem, self.recv_sem = buffers
        self.place = place()

    def own(self, n, core):
        which, first, a, b = self.spans[n]
        return self.ds[which].at[:, :, :, core, pl.ds(first, b - a)]

    def load(self, n):
        return pltpu.make_async_copy(self.own(n, self.place[3]), self.s.at[:, :, :, stretch(self.spans[n][2:])], self.local_sem.at[n])

    def copies(self, n, step):
        (x, y, z, c), s, span = self.place, self.s, self.spans[n][2:]
        u, by_x, by_y = stretch(span), at(1 - x, y, z, c), at(x, 1 - y, z, c)
        if step == 0:
            todo = [(self.own(n, 1 - c), self.r1.at[:, :, :, u], at(x, y, z, 1 - c))]
        elif step == 1:
            todo = [(s.at[1 - x, :, :, u] if first else s.at[:, 1 - y, :, u], self.r2.at[:, :, u], by_x if first else by_y) for first, u in halves(span, n)]
        elif step == 2:
            todo = [(s.at[x, 1 - y, :, u] if first else s.at[1 - x, y, :, u], self.r3.at[:, u], by_y if first else by_x) for first, u in halves(span, n)]
        else:
            todo = [(s.at[x, y, (z + k) % 4, u], self.r4.at[k - 1, u], at(x, y, (z + k) % 4, c)) for k in (1, 2, 3)]
        return [remote(a, b, self.send_sem.at[n, step, i], self.recv_sem.at[n, step, i], to) for i, (a, b, to) in enumerate(todo)]

    def add(self, n, step):
        (x, y, z, c), s, span = self.place, self.s, self.spans[n][2:]
        u = stretch(span)
        if step == 0:
            _add_into(s.at[:, :, :, u], self.r1.at[:, :, :, u])
        elif step == 1:
            for first, u in halves(span, n):
                _add_into(s.at[x, :, :, u] if first else s.at[:, y, :, u], self.r2.at[:, :, u])
        elif step == 2:
            _add_into(s.at[x, y, :, u], self.r3.at[:, u])
        else:
            out = s[x, y, z, u].astype(F32)
            for k in range(3):
                out = out + self.r4[k, u].astype(F32)
            self.g[u] = out.astype(BF)

    def begin(self):
        for n in range(len(self.spans)):
            self.load(n).start()
        greet(peers(*self.place))

    def send(self):
        wait_for(peers(*self.place))
        for n in range(len(self.spans)):
            self.start(n, 0)

    def start(self, n, step):
        for copy in self.copies(n, step):
            copy.start()

    def turns(self):
        found = [self.begin, self.send]
        for tick in range(len(self.spans) + 3 * self.lag):
            now = [(tick - self.lag * step, step) for step in range(4) if 0 <= tick - self.lag * step < len(self.spans)]

            def turn(now=now):
                for n, step in now:
                    if step == 0:
                        self.load(n).wait()
                    for copy in self.copies(n, step):
                        copy.wait_recv()
                    self.add(n, step)
                    if step < 3:
                        self.start(n, step + 1)

            found.append(turn)
        return found

    def tick(self, i, j):
        run_at(self.slots, self.turns(), i, j)

    def finish(self):
        for n in range(len(self.spans)):
            for step in range(4):
                for copy in self.copies(n, step):
                    copy.wait_send()


def _last_sums(spans, d, *refs):
    *done, g, squares, sq, sq_all, sq_send, sq_recv = refs[: -len(sum_buffers(1, 1))]
    traffic = Sums(1, (), spans, [d], g, *refs[-len(sum_buffers(1, 1)) :])
    me = lax.axis_index("dp")
    everyone = [{"dp": (me + k) % 32} for k in range(1, 32)]
    greet(everyone)
    for n in range(len(spans)):
        traffic.load(n).start()
    wait_for(everyone)
    for n in range(len(spans)):
        traffic.start(n, 0)
    sq[...] = jnp.zeros_like(sq)

    def squared(ref):
        def one(i, total):
            wide = ref[i].astype(F32)
            return total + (wide * wide).reshape(ROWS // 8, 8, D // HEAD, HEAD).sum((0, 2))

        sq[...] += lax.fori_loop(0, ref.shape[0], one, jnp.zeros((8, HEAD), F32))

    for ref in done:
        squared(ref)
    for turn in traffic.turns()[2:]:
        turn()
    squared(g)
    spread = [remote(sq, sq_all.at[k + 1], sq_send.at[k], sq_recv.at[k], to) for k, to in enumerate(everyone)]
    for copy in spread:
        copy.start()
    for copy in spread:
        copy.wait_recv()
    sq_all[0] = sq[...]
    squares[...] = jnp.full((8, HEAD), jnp.sum(sq_all[...]))
    for copy in spread:
        copy.wait_send()
    traffic.finish()


def last_sums(d, done):
    spans, units = sum_spans([d], LAST)
    return pl.pallas_call(
        functools.partial(_last_sums, spans),
        out_shape=[_like(units, ROWS, D), _like(8, HEAD, dtype=F32)],
        in_specs=[ANY] + [IN_VMEM] * len(done),
        out_specs=[IN_VMEM, IN_VMEM],
        scratch_shapes=[pltpu.VMEM((8, HEAD), F32), pltpu.VMEM((32, 8, HEAD), F32), pltpu.SemaphoreType.DMA((31,)), pltpu.SemaphoreType.DMA((31,)),
                        *sum_buffers(units, len(spans))],
        compiler_params=pltpu.CompilerParams(collective_id=1, has_side_effects=True, vmem_limit_bytes=VMEM),
        name="last_sums",
    )(d.reshape(2, 2, 4, 2, *d.shape[1:]), *done)


def _adamw(squares, *refs):
    g, (w, m, v, new_w, new_m, new_v) = refs[:4], (refs[i : i + 7] for i in range(4, 46, 7))
    count = 2 * UNITS * ROWS * D * 32
    factor = jnp.minimum(1.0, 0.5 * lax.rsqrt(squares[0:1, 0:1] / count + 1e-30))
    for layer in range(2):
        for i in range(7):
            for unit, piece in _pieces(i):
                where = (layer, *piece)
                sums, unit = (g[2 * layer], unit) if i < 4 else (g[2 * layer + 1], unit - 4)
                one = sums[unit].astype(F32) * factor
                mm = 0.9 * m[i][where] + 0.1 * one
                vv = 0.95 * v[i][where] + 0.05 * one * one
                old = w[i][where].astype(F32)
                new_w[i][where] = (old - 0.02 * (mm * lax.rsqrt(vv + 1e-8) + 0.1 * old)).astype(BF)
                new_m[i][where] = mm
                new_v[i][where] = vv


def _pieces(i):
    every = slice(None)
    if i < 4:
        return [(i, (every, every))]
    if i < 6:
        return [(4 * (i - 3) + j, (every, pl.ds(j * D, D))) for j in range(4)]
    return [(12 + j, (pl.ds(j * ROWS, ROWS), every)) for j in range(4)]


def adamw_all(weights, m, v, sums, squares):
    return pl.pallas_call(
        _adamw,
        out_shape=[_like(*w.shape) for w in weights] + [_like(*w.shape, dtype=F32) for w in weights] * 2,
        in_specs=[IN_VMEM] * 26,
        out_specs=[IN_VMEM] * 21,
        compiler_params=pltpu.CompilerParams(vmem_limit_bytes=VMEM),
        name="adamw_all",
    )(squares, *sums, *weights, *m, *v)


def _forward(spans, x_ref, fine_ref, coarse_ref, *refs):
    shards, (kept, q_ref, k_ref, v_ref, o_ref, lse_ref, mid_ref, h1_ref), refs = refs[:7], refs[7:15], refs[15:]
    g, h_s, k_s, vt_s, top_s, mix_s, *sems = refs
    fetch = Fetch(spans, shards, g, kept, *sems)
    s = pl.program_id(0)
    layer, i = s // (2 * STEPS), s % STEPS
    here = pl.ds(pl.multiple_of(i * BLOCK, BLOCK), BLOCK)
    unit = layer * UNITS
    phase = s // STEPS
    turns = fetch.turns()
    ready = [turn for turn, unit in turns if unit < 4]
    early = [turn for turn, unit in turns if 4 <= unit < UNITS]
    middle = [turn for turn, unit in turns if UNITS <= unit < UNITS + 4]
    late = [turn for turn, unit in turns if unit >= UNITS + 4]

    def tick(j):
        run_at(attention_slots([(n, n) for n in range(STEPS)]), early, s, j)
        run_at([(n, f"part {j}") for n in range(STEPS, 2 * STEPS) for j in range(STEPS)], middle, s, j)
        run_at(attention_slots([(n + 2 * STEPS, n) for n in range(STEPS)]), late, s, j)

    def weight(n):
        return g[:, :, :, :, unit + n].reshape(D, D)

    @pl.when(s == 0)
    def _():
        fetch.begin()
        for turn in ready:
            turn()

    @pl.when(phase == 0)
    def _():
        h_s[here, :] = x_ref[here, :]

    @pl.when(phase != 1)
    def _():
        a = _normed(h_s[here, :])[2]
        cos, sin = _angles(fine_ref, coarse_ref, i)
        for n, out in enumerate((q_ref, k_ref, v_ref)):
            t = _dot(a, weight(n)).astype(BF)
            t = t if n == 2 else _turned(t.astype(F32), cos, sin)
            out[...] = t
            if n == 1:
                k_s[here, :] = t
            if n == 2:
                vt_s[:, here] = t.T
        top_s[...] = jnp.full_like(top_s, NEG)
        mix_s[...] = jnp.zeros_like(mix_s)
        ones = jnp.ones((8, BLOCK), BF)
        e = SCALE * LOG2E

        def block(j, masked):
            tick(DIAGONAL if masked else j)
            keys = pl.ds(pl.multiple_of(j * BLOCK, BLOCK), BLOCK)
            scores = [_dot_t(k_s[keys, _head(n)], q_ref[:, _head(n)]) for n in range(HEADS)]
            if masked:
                ok = lax.broadcasted_iota(jnp.int32, (BLOCK, BLOCK), 1) >= lax.broadcasted_iota(jnp.int32, (BLOCK, BLOCK), 0)
            weights, keeps = [], []
            for n, x in enumerate(scores):
                if masked:
                    x = jnp.where(ok, x, HIDDEN)
                old = top_s[n : n + 1, :]
                top = jnp.maximum(old, x.max(axis=0, keepdims=True))
                top_s[n : n + 1, :] = top
                weights.append(jnp.exp2((x - top) * e).astype(BF))
                keeps.append(jnp.exp2((old - top) * e))
            for n in range(HEADS):
                values = jnp.concatenate([vt_s[_head(n), keys], ones], axis=0)
                mix_s[n] = mix_s[n] * keeps[n] + _dot(values, weights[n])

        lax.fori_loop(0, i, lambda j, _: block(j, False), None)
        block(i, True)
        tick(AFTER)
        for n in range(HEADS):
            total = mix_s[n, HEAD : HEAD + 1, :]
            o_ref[:, _head(n)] = (mix_s[n, :HEAD, :] * (1 / total)).T.astype(BF)
            lse_ref[n : n + 1, :] = top_s[n : n + 1, :] * SCALE + jnp.log(total)
        mid = h_s[here, :] + _dot(o_ref[...], weight(3)).astype(BF)
        mid_ref[...] = mid
        h_s[here, :] = mid

    @pl.when(phase == 1)
    def _():
        mid = h_s[here, :]
        b = _normed(mid)[2]
        total = None
        for j in range(FF // BLOCK):
            tick(f"part {j}")
            gate, up = _dot(b, weight(4 + j)), _dot(b, weight(8 + j))
            hid = (gate * (0.5 * jnp.tanh(0.5 * gate) + 0.5) * up).astype(BF)
            more = _dot(hid, g[j // 2, j % 2, :, :, 12:UNITS].reshape(D, D))
            total = more if j == 0 else total + more
        out = mid + total.astype(BF)
        h1_ref[...] = out
        h_s[here, :] = out

    @pl.when(s == pl.num_programs(0) - 1)
    def _():
        fetch.finish()


def forward(x, weights, angles):
    spans = [(n * 4 // FIRST, (n + 1) * 4 // FIRST) for n in range(FIRST)] + [(n, n + SPAN) for n in range(4, 2 * UNITS, SPAN)]
    n = len(spans)

    def place_of(s):
        t = s % (2 * STEPS)
        return s // (2 * STEPS), t - t // STEPS * (t - STEPS + 1)

    both = pl.BlockSpec((None, BLOCK, D), lambda s: (*place_of(s), 0))
    stats = pl.BlockSpec((None, HEADS, BLOCK), lambda s: (place_of(s)[0], 0, place_of(s)[1]))
    ffn_rows = pl.BlockSpec((BLOCK, D), lambda s: (s // STEPS % 2 * (s - STEPS) + s // STEPS // 2 * (STEPS - 1), 0))
    gathered = (2, 2, 4, 2, 2 * UNITS, ROWS, D)
    w, *rest = pl.pallas_call(
        functools.partial(_forward, spans),
        name="forward",
        grid=(3 * STEPS,),
        in_specs=[_whole(T, D), *_angle_specs()] + [ANY] * 7,
        out_specs=[ANY] + [both] * 4 + [stats, both, ffn_rows],
        out_shape=[_like(*gathered)] + [_like(2, T, D)] * 4 + [_like(2, HEADS, T, dtype=F32), _like(2, T, D), _like(T, D)],
        scratch_shapes=[pltpu.VMEM(gathered, BF), pltpu.VMEM((T, D), BF), pltpu.VMEM((T, D), BF), pltpu.VMEM((D, T), BF), pltpu.VMEM((HEADS, BLOCK), F32),
                        pltpu.VMEM((HEADS, HEAD + 8, BLOCK), F32)] + [pltpu.SemaphoreType.DMA(shape) for shape in ((2 * UNITS,), (n,), (n, 4, 3), (n, 4, 3))],
        compiler_params=pltpu.CompilerParams(dimension_semantics=("arbitrary",), vmem_limit_bytes=VMEM, collective_id=0, has_side_effects=True),
        cost_estimate=pl.CostEstimate(flops=50 * T * D * D, transcendentals=0, bytes_accessed=0),
    )(x, *angles, *weights)
    return w.reshape(D // ROWS, 2 * UNITS, ROWS, D), *rest


def solution(mesh):
    def step(x, dy, *arrays):
        weights, m, v = (arrays[i : i + 7] for i in (0, 7, 14))
        angles = angles_of()
        w, q, k, vv, o, lse, mid, h1 = forward(x[0], weights, angles)
        saved = (q, k, vv, o, lse)
        dmid, *ffn_1 = ffn_back(dy[0], mid, w, 1)
        dh, attn_1, ffn_1 = attn_back(h1, *saved, dmid, w, 1, angles, (2, *ffn_1))
        dmid, *ffn_0, attn_1 = ffn_back(dh, mid, w, 0, (3, attn_1))
        attn_0, ffn_0 = attn_back(x[0], *saved, dmid, w, 0, angles, (4, *ffn_0))
        attn_0, squares = last_sums(attn_0, (ffn_0, attn_1, ffn_1))
        return tuple(adamw_all(weights, m, v, (attn_0, ffn_0, attn_1, ffn_1), squares))

    states, cut = P(("rep", "dp"), None, None), P(None, "dp", None)
    return jax.shard_map(
        step,
        mesh=mesh,
        in_specs=(states, states) + (cut,) * 21,
        out_specs=(P("rep", "dp", None),) * 21,
        check_vma=False,
    )
```
